128 devices in a mesh: shell: 4 (over y_hi, core), img: 32 (over z, y_lo, x).
Axes of the slice: x: 4, y: 4 (y_hi: 2, y_lo: 2; y = y_hi * 2 + y_lo), z: 4, core: 2. Of those that a mesh axis runs over, the one named last changes fastest.
Arguments:
- images: bfloat16 [24576, 16384], P('img', 'shell'), may hold values from -12 to 12, as said below
- references: bfloat16 [1024, 16384], P('img', 'shell'), may hold values from -1 to 1, as said below
- shell_of_pixel: int32 [16384], P('shell'), may hold values from 0 to 63
- noise_power: float32 [64], replicated, may hold values from 0.1 to 10
- ref_class: int32 [1024], replicated, may hold values from 0 to 3
- ref_orient: int32 [1024], replicated, may hold values from 0 to 6143
- class_logw: float32 [4], replicated, may hold values from -4 to 4
- orient_logw: float32 [6144], replicated, may hold values from -4 to 4
Outputs:
- accumulators: float32 [1024, 16384], P('img', 'shell')
- evidence_logarithm: float32 [24576], P('img')
The draws below stay inside these ranges and needn't reach their ends.
Inputs may be any that keep to these rules, and one draw needn't show every extreme that they name: `images`: images are real-valued Fourier data. `references`: references are real-valued projections.
All inputs are finite; a program needn't handle non-finite values.
Results may differ from the reference program's by a relative error of at most 0.0077.
Values may be sent and summed in bfloat16 or wider, within the bound.
A program may use at most 128 MiB of HBM per device.

```python
import math
import jax
import jax.numpy as jnp
from jax import lax

PIX = 16384
NSHELL = 64
NCLASS = 4
NORIENT = 6144
NREF = 1024
NIMG = 24576


def joint_draw(key):
    folded = jax.random.fold_in(key, 7001)
    subkeys = jax.random.split(folded, 3)
    row_scale = jnp.exp(jax.random.uniform(subkeys[0], (NREF, 1), jnp.float32, jnp.log(0.5), jnp.log(2.5)))
    reference_pixels = jax.random.normal(subkeys[1], (NREF, PIX), jnp.float32) * row_scale / jnp.sqrt(jnp.float32(PIX))
    image_data = jax.random.normal(subkeys[2], (NIMG, PIX), jnp.float32)
    return (jnp.clip(image_data, -12.0, 12.0), jnp.clip(reference_pixels, -1.0, 1.0))


def draw_images(key, part):
    return joint_draw(key)[0].astype(jnp.bfloat16)


def draw_references(key, part):
    return joint_draw(key)[1].astype(jnp.bfloat16)


def with_ends(entries, own_key, low, top_value):
    place = [jax.random.randint(jax.random.fold_in(own_key, axis), (), 0, length) for axis, length in enumerate(entries.shape)]
    widest = entries.shape.index(max(entries.shape))
    beside = place[:widest] + [(place[widest] + 1) % entries.shape[widest]] + place[widest + 1:]
    return entries.at[tuple(place)].set(low).at[tuple(beside)].set(top_value)


def gaussian(key, dims, width, bound, held_as=jnp.bfloat16):
    array = jax.random.normal(key, dims, jnp.float32) * width
    return jnp.minimum(jnp.maximum(array, -bound), bound).astype(held_as)


def setup_inputs(seed: int = 0) -> dict:
    key_list = jax.random.split(jax.random.key(seed), 9)
    return {
        "images": draw_images(jax.random.fold_in(key_list[8], 71), 0),
        "references": draw_references(jax.random.fold_in(key_list[8], 71), 0),
        "shell_of_pixel": with_ends(jax.random.randint(key_list[2], (PIX,), 0, NSHELL), jax.random.fold_in(key_list[2], 1), 0, NSHELL - 1).astype(jnp.int32),
        "noise_power": jnp.clip(jnp.exp(jax.random.uniform(key_list[3], (NSHELL,), jnp.float32, math.log(0.1), math.log(10.0))), 0.1, 10.0),
        "ref_class": with_ends(jax.random.randint(key_list[4], (NREF,), 0, NCLASS), jax.random.fold_in(key_list[4], 1), 0, NCLASS - 1).astype(jnp.int32),
        "ref_orient": with_ends(jax.random.randint(key_list[5], (NREF,), 0, NORIENT), jax.random.fold_in(key_list[5], 1), 0, NORIENT - 1).astype(jnp.int32),
        "class_logw": gaussian(key_list[6], (NCLASS,), 1.0, 4.0, jnp.float32),
        "orient_logw": gaussian(key_list[7], (NORIENT,), 1.0, 4.0, jnp.float32),
    }


inverse_heat_factor = 0.5


def reference(images, references, shell_of_pixel, noise_power, ref_class, ref_orient, class_logw, orient_logw):
    inverse_noise = 1.0 / noise_power
    matches = shell_of_pixel[:, None] == jnp.arange(NSHELL, dtype=jnp.int32)[None, :]
    weights = jnp.sum(jnp.where(matches, inverse_noise[None, :], jnp.float32(0.0)), axis=1)
    weighted = (images.astype(jnp.float32) * weights[None, :]).astype(jnp.bfloat16)
    ref_float = references.astype(jnp.float32)
    ref_norm = jnp.dot(ref_float * ref_float, weights, precision=lax.Precision.HIGHEST)
    correlation = jnp.dot(weighted, references.T, preferred_element_type=jnp.float32)
    agreement_measures = correlation - 0.5 * ref_norm[None, :]
    class_agreement = ref_class[:, None] == jnp.arange(NCLASS, dtype=jnp.int32)[None, :]
    beforehand_logarithmic_share = jnp.sum(jnp.where(class_agreement, class_logw[None, :], jnp.float32(0.0)), axis=1) + orient_logw[ref_orient]
    raw_logarithmic_measures = inverse_heat_factor * agreement_measures + beforehand_logarithmic_share[None, :]
    highest = jnp.max(raw_logarithmic_measures, axis=1)
    evidence_logarithm = highest + jnp.log(jnp.sum(jnp.exp(raw_logarithmic_measures - highest[:, None]), axis=1))
    posterior = jnp.exp(raw_logarithmic_measures - evidence_logarithm[:, None]).astype(jnp.bfloat16)
    accumulators = jnp.dot(posterior.T, images, preferred_element_type=jnp.float32)
    return accumulators, evidence_logarithm
```

```python
import jax
import jax.numpy as jnp
from jax import lax
from jax.experimental import pallas as pl
from jax.experimental.pallas import tpu as pltpu
from jax.sharding import PartitionSpec as P

INVERSE_HEAT = 0.5
MESH = pl.DeviceIdType.MESH
F32 = jnp.float32
BF16 = jnp.bfloat16

NZ, NY, NX = 4, 2, 4
ROWS = 32
PIECE = 16
PIX = 4096
NIM = 768
HALF = NIM // 2
GROUP = 256
SIDE = GROUP // 2
NREF = 1024
TILE = 512
NT = PIX // TILE
PH = PIX // 2
NORIENT = 6144


def kernel(
    images_hbm,
    references_hbm,
    shell_ref,
    noise_ref,
    key_ref,
    orient_ref,
    class_ref,
    out_ref,
    evidence_ref,
    im,
    wim,
    refs,
    score,
    core_in,
    row_out,
    row_in,
    total,
    weight,
    keys,
    prior,
    stat_out,
    stat_in,
    post,
    s1,
    s2,
    s3,
    r_opp,
    r_plus,
    r_minus,
    acc,
    z1,
    z2,
    z3,
    zr_opp,
    zr_plus,
    zr_minus,
    y_out,
    y_in,
    load_sem,
    ag_s,
    ag_r,
    ex_s,
    ex_r,
    a_s,
    a_r,
    b_s,
    b_r,
    yy_s,
    yy_r,
):
    s = lax.axis_index("shell")
    i = lax.axis_index("img")
    core = lax.rem(s, 2)
    y_hi = s // 2
    z = i // (NY * NX)
    y = lax.rem(i // NX, NY)
    x = lax.rem(i, NX)

    def at(zz, yv, xx):
        return (zz * NY + yv) * NX + xx

    x_plus = (s, at(z, y, lax.rem(x + 1, NX)))
    x_minus = (s, at(z, y, lax.rem(x + NX - 1, NX)))
    z_plus = (s, at(lax.rem(z + 1, NZ), y, x))
    z_minus = (s, at(lax.rem(z + NZ - 1, NZ), y, x))
    y_pal = (s, at(z, 1 - y, x))
    core_pal = (y_hi * 2 + 1 - core, i)
    hi_pal = ((1 - y_hi) * 2 + core, i)
    a_plus, a_minus = (x_plus, z_plus), (x_minus, z_minus)
    b_plus, b_minus = (z_plus, x_plus), (z_minus, x_minus)

    def remote(src, dst, send_sem, recv_sem, peer):
        return pltpu.make_async_remote_copy(
            src_ref=src,
            dst_ref=dst,
            send_sem=send_sem,
            recv_sem=recv_sem,
            device_id=peer,
            device_id_type=MESH,
        )

    def landed(dst, send_sem, recv_sem):
        remote(dst, dst, send_sem, recv_sem, core_pal).wait_recv()

    own = []
    for t in range(2):
        c = pltpu.make_async_copy(
            references_hbm.at[pl.ds(t * PIECE, PIECE), :],
            refs.at[0, pl.ds(t * SIDE, PIECE), :],
            load_sem.at[t],
        )
        c.start()
        own.append(c)
    image_loads = []
    for n in range(3):
        c = pltpu.make_async_copy(
            images_hbm.at[pl.ds(n * 256, 256), :], im.at[pl.ds(n * 256, 256), :], load_sem.at[2 + n]
        )
        c.start()
        image_loads.append(c)

    barrier = pltpu.get_barrier_semaphore()
    for peer in (x_plus, x_minus, z_plus, z_minus, y_pal, core_pal, hi_pal):
        pl.semaphore_signal(barrier, inc=1, device_id=peer, device_id_type=MESH)
    pl.semaphore_wait(barrier, 7)

    index = {}
    ag_sends = []

    def slot(name):
        if name not in index:
            index[name] = len(index)
        return index[name]

    def piece(t, a, b, yr, part=None):
        rows = pl.ds(t * SIDE + b * 32 + yr * PIECE, PIECE)
        if part is None:
            return refs.at[a, rows, :]
        return refs.at[a, rows, pl.ds(part * PH, PH)]

    def ag_send(name, src, dst, peer):
        n = slot(name)
        c = remote(src, dst, ag_s.at[n], ag_r.at[n], peer)
        c.start()
        ag_sends.append(c)

    def ag_wait(name, dst):
        n = slot(name)
        landed(dst, ag_s.at[n], ag_r.at[n])

    def send_b(t, yr):
        ag_send(("b+", t, yr), piece(t, 0, 0, yr), piece(t, 0, 3, yr), b_plus[t])
        ag_send(("b-", t, yr), piece(t, 0, 0, yr), piece(t, 0, 1, yr), b_minus[t])

    def send_a(t, b, yr):
        ag_send(("a+", t, b, yr), piece(t, 0, b, yr), piece(t, 3, b, yr), a_plus[t])
        ag_send(("a-", t, b, yr), piece(t, 0, b, yr), piece(t, 1, b, yr), a_minus[t])

    for t in range(2):
        own[t].wait()
    for t in range(2):
        ag_send(("y", t), piece(t, 0, 0, 0), piece(t, 0, 0, 1), y_pal)
    for t in range(2):
        send_b(t, 0)
    for t in range(2):
        send_a(t, 0, 0)

    noise_row = 1.0 / noise_ref[...]
    r64 = lax.broadcasted_iota(jnp.int32, (64, 64), 0)
    c64 = lax.broadcasted_iota(jnp.int32, (64, 64), 1)
    noise_col = jnp.sum(
        jnp.where(r64 == c64, jnp.broadcast_to(noise_row, (64, 64)), 0.0), axis=1, keepdims=True
    )

    @pl.loop(0, PIX // 512)
    def _(n):
        cols = pl.ds(pl.multiple_of(n * 512, 512), 512)
        shell = jnp.broadcast_to(shell_ref[:, cols], (64, 512))
        hit = shell == lax.broadcasted_iota(jnp.int32, (64, 512), 0)
        weight[:, cols] = jnp.sum(
            jnp.where(hit, jnp.broadcast_to(noise_col, (64, 512)), 0.0), axis=0, keepdims=True
        )

    for t in range(2):
        ag_wait(("y", t), piece(t, 0, 0, 1))
        send_b(t, 1)
    for t in range(2):
        send_a(t, 0, 1)

    for n in range(3):
        image_loads[n].wait()

        @pl.loop(n * 16, n * 16 + 16)
        def _(k):
            rows = pl.ds(pl.multiple_of(k * 16, 16), 16)
            wim[rows, :] = (im[rows, :].astype(F32) * weight[...]).astype(BF16)

    for yr in range(2):
        for t in range(2):
            ag_wait(("b+", t, yr), piece(t, 0, 3, yr))
            ag_send(("bf+", t, yr), piece(t, 0, 3, yr, 0), piece(t, 0, 2, yr, 0), b_plus[t])
            ag_wait(("b-", t, yr), piece(t, 0, 1, yr))
            ag_send(("bf-", t, yr), piece(t, 0, 1, yr, 1), piece(t, 0, 2, yr, 1), b_minus[t])
        for t in range(2):
            send_a(t, 3, yr)
            send_a(t, 1, yr)
        if yr == 0:
            for a in range(4):
                for b in range(4):
                    for yr2 in range(2):
                        za = lax.rem(z + jnp.where(y_hi == 0, b, a), NZ)
                        xa = lax.rem(x + jnp.where(y_hi == 0, a, b), NX)
                        ya = y if yr2 == 0 else 1 - y
                        first = at(za, ya, xa) * ROWS + y_hi * PIECE
                        keys[pl.ds(a * SIDE + b * 32 + yr2 * PIECE, PIECE), :] = key_ref[
                            pl.ds(pl.multiple_of(first, PIECE), PIECE), :
                        ]

            @pl.loop(0, 4)
            def _(a):
                rows = pl.ds(pl.multiple_of(a * SIDE, SIDE), SIDE)
                key = keys[rows, :]
                orient = jnp.broadcast_to(lax.rem(key, 8192), (SIDE, 128))
                kind = key // 8192

                def add(n, sums):
                    cols = pl.ds(pl.multiple_of(n * 128, 128), 128)
                    ids = lax.broadcasted_iota(jnp.int32, (SIDE, 128), 1) + n * 128
                    logw = jnp.broadcast_to(orient_ref[:, cols], (SIDE, 128))
                    return sums + jnp.where(orient == ids, logw, 0.0)

                sums = lax.fori_loop(0, NORIENT // 128, add, jnp.zeros((SIDE, 128), F32))
                found = jnp.zeros((SIDE, 1), F32)
                for n in range(4):
                    found = found + jnp.where(kind == n, class_ref[n], 0.0)
                prior[rows, :] = found + jnp.sum(sums, axis=1, keepdims=True)

    for yr in range(2):
        for t in range(2):
            ag_wait(("bf+", t, yr), piece(t, 0, 2, yr, 0))
            ag_wait(("bf-", t, yr), piece(t, 0, 2, yr, 1))
            send_a(t, 2, yr)

    mine = pl.ds(pl.multiple_of(core * HALF, 128), HALF)
    theirs = pl.ds(pl.multiple_of((1 - core) * HALF, 128), HALF)
    keep = pl.ds(pl.multiple_of(y_hi * SIDE, SIDE), SIDE)
    give = pl.ds(pl.multiple_of((1 - y_hi) * SIDE, SIDE), SIDE)
    ex_sends = []

    def ex_send(n, src, dst, peer):
        c = remote(src, dst, ex_s.at[n], ex_r.at[n], peer)
        c.start()
        ex_sends.append(c)

    def ex_wait(n, dst):
        landed(dst, ex_s.at[n], ex_r.at[n])

    def do_scores(g):
        def add(n, sums):
            cols = pl.ds(pl.multiple_of(n * 128, 128), 128)
            r = refs[g, :, cols].astype(F32)
            return sums + r * r * weight[:, cols]

        sums = lax.fori_loop(0, PIX // 128, add, jnp.zeros((GROUP, 128), F32))
        norm = 0.5 * jnp.sum(sums, axis=1, keepdims=True)

        @pl.loop(0, 3)
        def _(n):
            rows = pl.ds(pl.multiple_of(n * 256, 256), 256)
            part = lax.dot_general(
                refs[g], wim[rows, :], (((1,), (1,)), ((), ())), preferred_element_type=F32
            )
            score[g, :, rows] = part - norm

        ex_send(g, score.at[g, :, theirs], core_in.at[g], core_pal)

    def do_rows(g):
        ex_wait(g, core_in.at[g])
        row_out[g] = score[g, give, mine] + core_in[g, give, :]
        ex_send(4 + g, row_out.at[g], row_in.at[g], hi_pal)
        total[g] = score[g, keep, mine] + core_in[g, keep, :]

    def do_logits(g):
        ex_wait(4 + g, row_in.at[g])
        rows = pl.ds(g * SIDE, SIDE)
        logits = INVERSE_HEAT * (total[g] + row_in[g]) + prior[rows, :]
        total[g] = logits
        return jnp.max(logits, axis=0, keepdims=True)

    do_scores(0)
    order = [(0, 0), (0, 1), (3, 0), (1, 0), (3, 1), (1, 1), (2, 0), (2, 1)]
    for n, (b, yr) in enumerate(order):
        for t in range(2):
            ag_wait(("a+", t, b, yr), piece(t, 3, b, yr))
            ag_send(("af+", t, b, yr), piece(t, 3, b, yr, 0), piece(t, 2, b, yr, 0), a_plus[t])
            ag_wait(("a-", t, b, yr), piece(t, 1, b, yr))
            ag_send(("af-", t, b, yr), piece(t, 1, b, yr, 1), piece(t, 2, b, yr, 1), a_minus[t])
        if n == 1:
            do_rows(0)
    do_scores(1)
    do_scores(3)
    do_rows(1)
    do_rows(3)
    for b, yr in order:
        for t in range(2):
            ag_wait(("af+", t, b, yr), piece(t, 2, b, yr, 0))
            ag_wait(("af-", t, b, yr), piece(t, 2, b, yr, 1))
    do_scores(2)
    top = do_logits(0)
    top = jnp.maximum(top, do_logits(1))
    do_rows(2)
    top = jnp.maximum(top, do_logits(3))
    top = jnp.maximum(top, do_logits(2))
    mass = jnp.zeros((1, HALF), F32)
    for g in range(4):
        mass = mass + jnp.sum(jnp.exp(total[g] - top), axis=0, keepdims=True)
    stat_out[0:8, :] = jnp.broadcast_to(top, (8, HALF))
    stat_out[8:16, :] = jnp.broadcast_to(mass, (8, HALF))
    ex_send(8, stat_out.at[0:16], stat_in.at[0:16], hi_pal)
    ex_wait(8, stat_in.at[0:16])
    other_top, other_mass = stat_in[0:1, :], stat_in[8:9, :]
    first = y_hi == 0
    top_a, top_b = jnp.where(first, top, other_top), jnp.where(first, other_top, top)
    mass_a, mass_b = jnp.where(first, mass, other_mass), jnp.where(first, other_mass, mass)
    best = jnp.maximum(top_a, top_b)
    evidence = best + jnp.log(mass_a * jnp.exp(top_a - best) + mass_b * jnp.exp(top_b - best))
    stat_out[16:24, :] = jnp.broadcast_to(evidence, (8, HALF))
    gs = (2, 1, 3, 0)
    for g in gs:
        post[g, keep, mine] = jnp.exp(total[g] - evidence).astype(BF16)
        ex_send(12 + g, post.at[g, keep, mine], post.at[g, keep, mine], hi_pal)
        ex_send(16 + g, post.at[g, keep, mine], post.at[g, keep, mine], core_pal)
    ex_send(9, stat_out.at[16:24], stat_in.at[16:24], core_pal)

    def do_relay(g):
        ex_wait(12 + g, post.at[g, give, mine])
        ex_send(20 + g, post.at[g, give, mine], post.at[g, give, mine], core_pal)

    def do_posterior(g):
        ex_wait(16 + g, post.at[g, keep, theirs])
        ex_wait(20 + g, post.at[g, give, theirs])

    def product(g, j):
        cols = pl.ds(pl.multiple_of(j * TILE, TILE), TILE)
        return jnp.dot(post[g], im[:, cols], preferred_element_type=F32)

    def half(t):
        return pl.ds(t * SIDE, SIDE)

    def a_copy(kind, j, t, src, dst, peer):
        return remote(
            src.at[j, half(t)], dst.at[j, half(t)], a_s.at[kind, j, t], a_r.at[kind, j, t], peer
        )

    def a_landed(kind, j, t, dst):
        landed(dst.at[j, half(t)], a_s.at[kind, j, t], a_r.at[kind, j, t])

    do_relay(2)
    do_posterior(2)
    do_relay(1)

    @pl.loop(0, 4)
    def _(k):
        s2[k] = product(2, k).astype(BF16)
        for t in range(2):
            a_copy(0, k, t, s2, r_opp, a_plus[t]).start()
        s2[k + 4] = product(2, k + 4).astype(BF16)
        for t in range(2):
            a_copy(0, k + 4, t, s2, r_opp, a_minus[t]).start()

    do_relay(3)
    do_posterior(1)
    do_posterior(3)
    do_relay(0)

    @pl.loop(0, 4)
    def _(k):
        s1[k + 4] = product(1, k + 4).astype(BF16)
        for t in range(2):
            a_copy(1, k + 4, t, s1, r_minus, a_plus[t]).start()
        s3[k] = product(3, k).astype(BF16)
        for t in range(2):
            a_copy(2, k, t, s3, r_plus, a_minus[t]).start()

    do_posterior(0)
    ex_wait(9, stat_in.at[16:24])
    evidence_ref[:, mine] = stat_out[16:17, :]
    evidence_ref[:, theirs] = stat_in[16:17, :]

    @pl.loop(0, 4)
    def _(k):
        p1 = product(1, k)
        for t in range(2):
            a_landed(0, k, t, r_opp)
        s1[k] = (p1 + r_opp[k].astype(F32)).astype(BF16)
        for t in range(2):
            a_copy(1, k, t, s1, r_minus, a_plus[t]).start()
        p3 = product(3, k + 4)
        for t in range(2):
            a_landed(0, k + 4, t, r_opp)
        s3[k + 4] = (p3 + r_opp[k + 4].astype(F32)).astype(BF16)
        for t in range(2):
            a_copy(2, k + 4, t, s3, r_plus, a_minus[t]).start()

    def b_copy(kind, j, t, src, dst, peer):
        return remote(src.at[j, t], dst.at[j, t], b_s.at[kind, j, t], b_r.at[kind, j, t], peer)

    def b_landed(kind, j, t, dst):
        landed(dst.at[j, t], b_s.at[kind, j, t], b_r.at[kind, j, t])

    def y_copy(j, t):
        return remote(y_out.at[j, t], y_in.at[j, t], yy_s.at[j, t], yy_r.at[j, t], y_pal)

    def step_a(k):
        for j, low in ((k, True), (k + 4, False)):
            p = product(0, j)
            for t in range(2):
                a_landed(1, j, t, r_minus)
                a_landed(2, j, t, r_plus)
            acc[j] = p + r_plus[j].astype(F32) + r_minus[j].astype(F32)
            for t in range(2):
                o = t * SIDE
                z2[j, t] = acc[j, o + 64 : o + 96, :].astype(BF16)
                b_copy(0, j, t, z2, zr_opp, b_plus[t] if low else b_minus[t]).start()
                if low:
                    z3[j, t] = acc[j, o + 96 : o + 128, :].astype(BF16)
                    b_copy(2, j, t, z3, zr_plus, b_minus[t]).start()
                else:
                    z1[j, t] = acc[j, o + 32 : o + 64, :].astype(BF16)
                    b_copy(1, j, t, z1, zr_minus, b_plus[t]).start()

    def step_b(k):
        for t in range(2):
            o = t * SIDE
            b_landed(0, k, t, zr_opp)
            z1[k, t] = (acc[k, o + 32 : o + 64, :] + zr_opp[k, t].astype(F32)).astype(BF16)
            b_copy(1, k, t, z1, zr_minus, b_plus[t]).start()
            j = k + 4
            b_landed(0, j, t, zr_opp)
            z3[j, t] = (acc[j, o + 96 : o + 128, :] + zr_opp[j, t].astype(F32)).astype(BF16)
            b_copy(2, j, t, z3, zr_plus, b_minus[t]).start()

    def step_c(k):
        for j in (k, k + 4):
            for t in range(2):
                o = t * SIDE
                b_landed(1, j, t, zr_minus)
                b_landed(2, j, t, zr_plus)
                v = acc[j, o : o + 32, :] + zr_plus[j, t].astype(F32) + zr_minus[j, t].astype(F32)
                y_out[j, t] = v[PIECE:, :].astype(BF16)
                y_copy(j, t).start()
                acc[j, o : o + PIECE, :] = v[:PIECE, :]

    def step_d(k):
        for j in (k, k + 4):
            for t in range(2):
                o = t * SIDE
                y_copy(j, t).wait_recv()
                cols = pl.ds(pl.multiple_of(j * TILE, TILE), TILE)
                out_ref[t * PIECE : (t + 1) * PIECE, cols] = acc[j, o : o + PIECE, :] + y_in[
                    j, t
                ].astype(F32)

    @pl.loop(0, 7)
    def _(k):
        @pl.when(k < 4)
        def _():
            step_a(k)

        @pl.when(jnp.logical_and(k >= 1, k < 5))
        def _():
            step_b(k - 1)

        @pl.when(jnp.logical_and(k >= 2, k < 6))
        def _():
            step_c(k - 2)

        @pl.when(k >= 3)
        def _():
            step_d(k - 3)

    for c in ag_sends:
        c.wait_send()
    for c in ex_sends:
        c.wait_send()

    @pl.loop(0, NT)
    def _(j):
        for t in range(2):
            a_copy(0, j, t, s2, r_opp, core_pal).wait_send()
            a_copy(1, j, t, s1, r_minus, core_pal).wait_send()
            a_copy(2, j, t, s3, r_plus, core_pal).wait_send()
            b_copy(0, j, t, z2, zr_opp, core_pal).wait_send()
            b_copy(1, j, t, z1, zr_minus, core_pal).wait_send()
            b_copy(2, j, t, z3, zr_plus, core_pal).wait_send()
            y_copy(j, t).wait_send()


def shards(
    images, references, shell_of_pixel, noise_power, ref_class, ref_orient, class_logw, orient_logw
):
    key = (ref_class * 8192 + ref_orient).reshape(NREF, 1)
    vmem = pl.BlockSpec(memory_space=pltpu.VMEM)
    hbm = pl.BlockSpec(memory_space=pl.ANY)
    smem = pl.BlockSpec(memory_space=pltpu.SMEM)
    dma = pltpu.SemaphoreType.DMA
    accumulators, evidence = pl.pallas_call(
        kernel,
        out_shape=(
            jax.ShapeDtypeStruct((ROWS, PIX), F32),
            jax.ShapeDtypeStruct((1, NIM), F32),
        ),
        in_specs=[hbm, hbm, vmem, vmem, vmem, vmem, smem],
        out_specs=(vmem, vmem),
        scratch_shapes=[
            pltpu.VMEM((NIM, PIX), BF16),
            pltpu.VMEM((NIM, PIX), BF16),
            pltpu.VMEM((4, GROUP, PIX), BF16),
            pltpu.VMEM((4, GROUP, NIM), F32),
            pltpu.VMEM((4, GROUP, HALF), F32),
            pltpu.VMEM((4, SIDE, HALF), F32),
            pltpu.VMEM((4, SIDE, HALF), F32),
            pltpu.VMEM((4, SIDE, HALF), F32),
            pltpu.VMEM((1, PIX), F32),
            pltpu.VMEM((4 * SIDE, 1), jnp.int32),
            pltpu.VMEM((4 * SIDE, 1), F32),
            pltpu.VMEM((24, HALF), F32),
            pltpu.VMEM((24, HALF), F32),
            pltpu.VMEM((4, GROUP, NIM), BF16),
            pltpu.VMEM((NT, GROUP, TILE), BF16),
            pltpu.VMEM((NT, GROUP, TILE), BF16),
            pltpu.VMEM((NT, GROUP, TILE), BF16),
            pltpu.VMEM((NT, GROUP, TILE), BF16),
            pltpu.VMEM((NT, GROUP, TILE), BF16),
            pltpu.VMEM((NT, GROUP, TILE), BF16),
            pltpu.VMEM((NT, GROUP, TILE), F32),
            pltpu.VMEM((NT, 2, 32, TILE), BF16),
            pltpu.VMEM((NT, 2, 32, TILE), BF16),
            pltpu.VMEM((NT, 2, 32, TILE), BF16),
            pltpu.VMEM((NT, 2, 32, TILE), BF16),
            pltpu.VMEM((NT, 2, 32, TILE), BF16),
            pltpu.VMEM((NT, 2, 32, TILE), BF16),
            pltpu.VMEM((NT, 2, PIECE, TILE), BF16),
            pltpu.VMEM((NT, 2, PIECE, TILE), BF16),
            dma((5,)),
            dma((84,)),
            dma((84,)),
            dma((24,)),
            dma((24,)),
            dma((3, NT, 2)),
            dma((3, NT, 2)),
            dma((3, NT, 2)),
            dma((3, NT, 2)),
            dma((NT, 2)),
            dma((NT, 2)),
        ],
        compiler_params=pltpu.CompilerParams(
            collective_id=0, has_side_effects=True, vmem_limit_bytes=67043328
        ),
    )(
        images,
        references,
        shell_of_pixel.reshape(1, PIX),
        noise_power.reshape(1, 64),
        key,
        orient_logw.reshape(1, NORIENT),
        class_logw,
    )
    return accumulators, evidence.reshape(NIM)


def solution(mesh):
    placed = (P("img", "shell"), P("img", "shell"), P("shell"), P(), P(), P(), P(), P())
    return jax.shard_map(
        shards, mesh=mesh, in_specs=placed, out_specs=(P("img", "shell"), P("img")), check_vma=False
    )
```

```python
import jax
import jax.numpy as jnp
from jax import lax
from jax.experimental import pallas as pl
from jax.experimental.pallas import tpu as pltpu
from jax.sharding import PartitionSpec as P

INVERSE_HEAT = 0.5
MESH = pl.DeviceIdType.MESH
F32 = jnp.float32
BF16 = jnp.bfloat16

NZ, NY, NX = 4, 2, 4
ROWS = 32
PIECE = 16
PIX = 4096
NIM = 768
HALF = NIM // 2
GROUP = 256
SIDE = GROUP // 2
NREF = 1024
TILE = 512
NT = PIX // TILE
PH = PIX // 2
NORIENT = 6144


def kernel(
    images_hbm,
    references_hbm,
    shell_ref,
    noise_ref,
    class_id_ref,
    orient_id_ref,
    orient_ref,
    class_ref,
    out_ref,
    evidence_ref,
    im,
    wim,
    refs,
    score,
    core_in,
    row_out,
    row_in,
    total,
    weight,
    square,
    columns,
    prior,
    evid,
    stat_out,
    stat_in,
    post,
    s1,
    s2,
    s3,
    r_opp,
    r_plus,
    r_minus,
    acc,
    z1,
    z2,
    z3,
    zr_opp,
    zr_plus,
    zr_minus,
    y_out,
    y_in,
    load_sem,
    ag_s,
    ag_r,
    ex_s,
    ex_r,
    a_s,
    a_r,
    b_s,
    b_r,
    yy_s,
    yy_r,
):
    s = lax.axis_index("shell")
    i = lax.axis_index("img")
    core = lax.rem(s, 2)
    y_hi = s // 2
    z = i // (NY * NX)
    y = lax.rem(i // NX, NY)
    x = lax.rem(i, NX)

    def at(zz, yv, xx):
        return (zz * NY + yv) * NX + xx

    x_plus = (s, at(z, y, lax.rem(x + 1, NX)))
    x_minus = (s, at(z, y, lax.rem(x + NX - 1, NX)))
    z_plus = (s, at(lax.rem(z + 1, NZ), y, x))
    z_minus = (s, at(lax.rem(z + NZ - 1, NZ), y, x))
    y_pal = (s, at(z, 1 - y, x))
    core_pal = (y_hi * 2 + 1 - core, i)
    hi_pal = ((1 - y_hi) * 2 + core, i)
    a_plus, a_minus = (x_plus, z_plus), (x_minus, z_minus)
    b_plus, b_minus = (z_plus, x_plus), (z_minus, x_minus)

    def remote(src, dst, send_sem, recv_sem, peer):
        return pltpu.make_async_remote_copy(
            src_ref=src,
            dst_ref=dst,
            send_sem=send_sem,
            recv_sem=recv_sem,
            device_id=peer,
            device_id_type=MESH,
        )

    def landed(dst, send_sem, recv_sem):
        remote(dst, dst, send_sem, recv_sem, core_pal).wait_recv()

    own = []
    for t in range(2):
        c = pltpu.make_async_copy(
            references_hbm.at[pl.ds(t * PIECE, PIECE), :],
            refs.at[0, pl.ds(t * SIDE, PIECE), :],
            load_sem.at[t],
        )
        c.start()
        own.append(c)
    image_loads = []
    for n in range(3):
        c = pltpu.make_async_copy(
            images_hbm.at[pl.ds(n * 256, 256), :], im.at[pl.ds(n * 256, 256), :], load_sem.at[2 + n]
        )
        c.start()
        image_loads.append(c)

    barrier = pltpu.get_barrier_semaphore()
    for peer in (x_plus, x_minus, z_plus, z_minus, y_pal, core_pal, hi_pal):
        pl.semaphore_signal(barrier, inc=1, device_id=peer, device_id_type=MESH)
    pl.semaphore_wait(barrier, 7)

    index = {}
    ag_sends = []

    def slot(name):
        if name not in index:
            index[name] = len(index)
        return index[name]

    def piece(t, a, b, yr, part=None):
        rows = pl.ds(t * SIDE + b * 32 + yr * PIECE, PIECE)
        if part is None:
            return refs.at[a, rows, :]
        return refs.at[a, rows, pl.ds(part * PH, PH)]

    def ag_send(name, src, dst, peer):
        n = slot(name)
        c = remote(src, dst, ag_s.at[n], ag_r.at[n], peer)
        c.start()
        ag_sends.append(c)

    def ag_wait(name, dst):
        n = slot(name)
        landed(dst, ag_s.at[n], ag_r.at[n])

    def send_b(t, yr):
        ag_send(("b+", t, yr), piece(t, 0, 0, yr), piece(t, 0, 3, yr), b_plus[t])
        ag_send(("b-", t, yr), piece(t, 0, 0, yr), piece(t, 0, 1, yr), b_minus[t])

    def send_a(t, b, yr):
        ag_send(("a+", t, b, yr), piece(t, 0, b, yr), piece(t, 3, b, yr), a_plus[t])
        ag_send(("a-", t, b, yr), piece(t, 0, b, yr), piece(t, 1, b, yr), a_minus[t])

    def log_prior():
        square[...] = jnp.zeros((128, 128), F32)
        for n, ids in enumerate((class_id_ref, orient_id_ref)):
            square[0:8, :] = ids[...].astype(F32)
            columns[n] = square[...].T

        def place(block, row, a, b, yr, kind):
            za = lax.rem(z + jnp.where(kind == 0, b, a), NZ)
            xa = lax.rem(x + jnp.where(kind == 0, a, b), NX)
            ya = y if yr == 0 else 1 - y
            first = at(za, ya, xa) * ROWS + kind * PIECE
            rows = pl.ds(pl.multiple_of(lax.rem(first, 128), PIECE), PIECE)
            pick = lax.broadcasted_iota(jnp.int32, (PIECE, 128), 1) == first // 128
            for n in range(2):
                found = jnp.sum(jnp.where(pick, columns[n, rows, :], 0.0), axis=1, keepdims=True)
                prior[n, pl.ds(block * SIDE + row, PIECE), :] = found

        for b in range(4):
            for yr in range(2):
                for g in (0, 1, 3):
                    place(g, b * 32 + yr * PIECE, g, b, yr, y_hi)
                for t in range(2):
                    row = t * 64 + (b % 2) * 32 + yr * PIECE
                    place(2 + 2 * (b // 2), row, 2, b, yr, t)

        @pl.loop(0, 5)
        def _(block):
            rows = pl.ds(pl.multiple_of(block * SIDE, SIDE), SIDE)
            kind = prior[0, rows, :]
            orient = jnp.broadcast_to(prior[1, rows, :], (SIDE, 128)).astype(jnp.int32)

            def add(n, sums):
                cols = pl.ds(pl.multiple_of(n * 128, 128), 128)
                ids = lax.broadcasted_iota(jnp.int32, (SIDE, 128), 1) + n * 128
                logw = jnp.broadcast_to(orient_ref[:, cols], (SIDE, 128))
                return sums + jnp.where(orient == ids, logw, 0.0)

            sums = lax.fori_loop(0, NORIENT // 128, add, jnp.zeros((SIDE, 128), F32))
            found = jnp.zeros((SIDE, 1), F32)
            for n in range(4):
                found = found + jnp.where(kind == float(n), class_ref[n], 0.0)
            prior[0, rows, :] = found + jnp.sum(sums, axis=1, keepdims=True)

    for t in range(2):
        own[t].wait()
    for t in range(2):
        ag_send(("y", t), piece(t, 0, 0, 0), piece(t, 0, 0, 1), y_pal)
    for t in range(2):
        send_b(t, 0)
    for t in range(2):
        send_a(t, 0, 0)

    noise_row = 1.0 / noise_ref[...]
    r64 = lax.broadcasted_iota(jnp.int32, (64, 64), 0)
    c64 = lax.broadcasted_iota(jnp.int32, (64, 64), 1)
    noise_col = jnp.sum(
        jnp.where(r64 == c64, jnp.broadcast_to(noise_row, (64, 64)), 0.0), axis=1, keepdims=True
    )

    @pl.loop(0, PIX // 512)
    def _(n):
        cols = pl.ds(pl.multiple_of(n * 512, 512), 512)
        shell = jnp.broadcast_to(shell_ref[:, cols], (64, 512))
        hit = shell == lax.broadcasted_iota(jnp.int32, (64, 512), 0)
        weight[:, cols] = jnp.sum(
            jnp.where(hit, jnp.broadcast_to(noise_col, (64, 512)), 0.0), axis=0, keepdims=True
        )

    for t in range(2):
        ag_wait(("y", t), piece(t, 0, 0, 1))
        send_b(t, 1)
    for t in range(2):
        send_a(t, 0, 1)

    for n in range(3):
        image_loads[n].wait()

        @pl.loop(n * 16, n * 16 + 16)
        def _(k):
            rows = pl.ds(pl.multiple_of(k * 16, 16), 16)
            wim[rows, :] = (im[rows, :].astype(F32) * weight[...]).astype(BF16)

    for yr in range(2):
        for t in range(2):
            ag_wait(("b+", t, yr), piece(t, 0, 3, yr))
            ag_send(("bf+", t, yr), piece(t, 0, 3, yr, 0), piece(t, 0, 2, yr, 0), b_plus[t])
            ag_wait(("b-", t, yr), piece(t, 0, 1, yr))
            ag_send(("bf-", t, yr), piece(t, 0, 1, yr, 1), piece(t, 0, 2, yr, 1), b_minus[t])
        for t in range(2):
            send_a(t, 3, yr)
            send_a(t, 1, yr)
        if yr == 0:
            log_prior()

    for yr in range(2):
        for t in range(2):
            ag_wait(("bf+", t, yr), piece(t, 0, 2, yr, 0))
            ag_wait(("bf-", t, yr), piece(t, 0, 2, yr, 1))
            send_a(t, 2, yr)

    mine = pl.ds(pl.multiple_of(core * HALF, 128), HALF)
    theirs = pl.ds(pl.multiple_of((1 - core) * HALF, 128), HALF)
    keep = pl.ds(pl.multiple_of(y_hi * SIDE, SIDE), SIDE)
    give = pl.ds(pl.multiple_of((1 - y_hi) * SIDE, SIDE), SIDE)
    ex_sends = []

    def ex_send(n, src, dst, peer):
        c = remote(src, dst, ex_s.at[n], ex_r.at[n], peer)
        c.start()
        ex_sends.append(c)

    def ex_wait(n, dst):
        landed(dst, ex_s.at[n], ex_r.at[n])

    def scores(r, out, n_rows):
        def add(n, sums):
            cols = pl.ds(pl.multiple_of(n * 128, 128), 128)
            part = r(cols).astype(F32)
            return sums + part * part * weight[:, cols]

        sums = lax.fori_loop(0, PIX // 128, add, jnp.zeros((n_rows, 128), F32))
        norm = 0.5 * jnp.sum(sums, axis=1, keepdims=True)

        @pl.loop(0, 3)
        def _(n):
            rows = pl.ds(pl.multiple_of(n * 256, 256), 256)
            part = lax.dot_general(
                r(slice(None)), wim[rows, :], (((1,), (1,)), ((), ())), preferred_element_type=F32
            )
            out[:, rows] = part - norm

    def do_scores(g):
        scores(lambda cols: refs[g, :, cols], score.at[g], GROUP)
        ex_send(g, score.at[g, :, theirs], core_in.at[g], core_pal)

    def do_rows(g):
        ex_wait(g, core_in.at[g])
        row_out[g] = score[g, give, mine] + core_in[g, give, :]
        ex_send(4 + g, row_out.at[g], row_in.at[g], hi_pal)
        total[g] = score[g, keep, mine] + core_in[g, keep, :]

    half_rows = (pl.ds(0, SIDE), pl.ds(SIDE, SIDE))

    def do_scores_2(h):
        def r(cols):
            low = refs[2, h * 64 : h * 64 + 64, cols]
            return jnp.concatenate([low, refs[2, SIDE + h * 64 : SIDE + h * 64 + 64, cols]], axis=0)

        scores(r, score.at[2, half_rows[h]], SIDE)
        n = (2, 10)[h]
        ex_send(n, score.at[2, half_rows[h], theirs], core_in.at[2, half_rows[h]], core_pal)

    def do_rows_2(h):
        ex_wait((2, 10)[h], core_in.at[2, half_rows[h]])
        block = 2 + 2 * h
        row_out[block] = score[2, half_rows[h], mine] + core_in[2, half_rows[h], :]
        ex_send((6, 11)[h], row_out.at[block], row_in.at[block], hi_pal)

    def do_logits(block):
        rows = pl.ds(block * SIDE, SIDE)
        if block in (2, 4):
            ex_wait({2: 6, 4: 11}[block], row_in.at[block])
            summed = row_out[block] + row_in[block]
        else:
            ex_wait(4 + block, row_in.at[block])
            summed = total[block] + row_in[block]
        logits = INVERSE_HEAT * summed + prior[0, rows, :]
        total[block] = logits
        return jnp.max(logits, axis=0, keepdims=True)

    def mass_of(blocks, top):
        mass = jnp.zeros((1, HALF), F32)
        for block in blocks:
            mass = mass + jnp.sum(jnp.exp(total[block] - top), axis=0, keepdims=True)
        return mass

    do_scores(0)
    order = [(0, 0), (0, 1), (3, 0), (1, 0), (3, 1), (1, 1), (2, 0), (2, 1)]
    forward = [(0, 0), (0, 1), (1, 0), (1, 1), (3, 0), (3, 1), (2, 0), (2, 1)]
    arrived = []
    passed = 0
    for n, (b, yr) in enumerate(order):
        for t in range(2):
            ag_wait(("a+", t, b, yr), piece(t, 3, b, yr))
            ag_wait(("a-", t, b, yr), piece(t, 1, b, yr))
        arrived.append((b, yr))
        while passed < 8 and forward[passed] in arrived:
            b, yr = forward[passed]
            for t in range(2):
                ag_send(("af+", t, b, yr), piece(t, 3, b, yr, 0), piece(t, 2, b, yr, 0), a_plus[t])
                ag_send(("af-", t, b, yr), piece(t, 1, b, yr, 1), piece(t, 2, b, yr, 1), a_minus[t])
            passed += 1
        if n == 1:
            do_rows(0)
    do_scores(1)
    do_scores(3)
    do_rows(1)
    do_rows(3)

    def opposite_landed(pieces):
        for b, yr in pieces:
            for t in range(2):
                ag_wait(("af+", t, b, yr), piece(t, 2, b, yr, 0))
                ag_wait(("af-", t, b, yr), piece(t, 2, b, yr, 1))

    opposite_landed(forward[:4])
    do_scores_2(0)
    top = do_logits(0)
    do_rows_2(0)
    opposite_landed(forward[4:])
    do_scores_2(1)
    top = jnp.maximum(top, do_logits(1))
    top = jnp.maximum(top, do_logits(3))
    mass = mass_of((0, 1, 3), top)
    stat_out[0:1, :] = top
    stat_out[1:2, :] = mass
    do_rows_2(1)
    ex_send(8, stat_out.at[0:8], stat_in.at[0:8], hi_pal)
    last_top = do_logits(2)
    ex_wait(8, stat_in.at[0:8])
    other_top, other_mass = stat_in[0:1, :], stat_in[1:2, :]
    first = y_hi == 0
    top_a, top_b = jnp.where(first, top, other_top), jnp.where(first, other_top, top)
    mass_a, mass_b = jnp.where(first, mass, other_mass), jnp.where(first, other_mass, mass)
    last_top = jnp.maximum(last_top, do_logits(4))
    best = jnp.maximum(jnp.maximum(top_a, top_b), last_top)
    evidence = best + jnp.log(
        mass_a * jnp.exp(top_a - best) + mass_b * jnp.exp(top_b - best) + mass_of((2, 4), best)
    )
    for h in range(2):
        p = jnp.exp(total[2 + 2 * h] - evidence).astype(BF16)
        for t in range(2):
            rows = pl.ds(t * SIDE + h * 64, 64)
            post[2, rows, mine] = p[t * 64 : t * 64 + 64, :]
    ex_send(18, post.at[2, :, mine], post.at[2, :, mine], core_pal)
    stat_out[8:16, :] = jnp.broadcast_to(evidence, (8, HALF))
    for g in (1, 3, 0):
        post[g, keep, mine] = jnp.exp(total[g] - evidence).astype(BF16)
        ex_send(12 + g, post.at[g, keep, mine], post.at[g, keep, mine], hi_pal)
        ex_send(16 + g, post.at[g, keep, mine], post.at[g, keep, mine], core_pal)
    ex_send(9, stat_out.at[8:16], stat_in.at[8:16], core_pal)

    def do_relay(g):
        ex_wait(12 + g, post.at[g, give, mine])
        ex_send(20 + g, post.at[g, give, mine], post.at[g, give, mine], core_pal)

    def do_posterior(g):
        ex_wait(16 + g, post.at[g, keep, theirs])
        ex_wait(20 + g, post.at[g, give, theirs])

    def product(g, j):
        cols = pl.ds(pl.multiple_of(j * TILE, TILE), TILE)
        return jnp.dot(post[g], im[:, cols], preferred_element_type=F32)

    def half(t):
        return pl.ds(t * SIDE, SIDE)

    def a_copy(kind, j, t, src, dst, peer):
        return remote(
            src.at[j, half(t)], dst.at[j, half(t)], a_s.at[kind, j, t], a_r.at[kind, j, t], peer
        )

    def a_landed(kind, j, t, dst):
        landed(dst.at[j, half(t)], a_s.at[kind, j, t], a_r.at[kind, j, t])

    ex_wait(18, post.at[2, :, theirs])

    @pl.loop(0, 4)
    def _(k):
        s2[k] = product(2, k).astype(BF16)
        for t in range(2):
            a_copy(0, k, t, s2, r_opp, a_plus[t]).start()
        s2[k + 4] = product(2, k + 4).astype(BF16)
        for t in range(2):
            a_copy(0, k + 4, t, s2, r_opp, a_minus[t]).start()

    do_relay(1)
    do_relay(3)
    do_posterior(1)
    do_posterior(3)
    do_relay(0)

    @pl.loop(0, 4)
    def _(k):
        s1[k + 4] = product(1, k + 4).astype(BF16)
        for t in range(2):
            a_copy(1, k + 4, t, s1, r_minus, a_plus[t]).start()
        s3[k] = product(3, k).astype(BF16)
        for t in range(2):
            a_copy(2, k, t, s3, r_plus, a_minus[t]).start()

    do_posterior(0)
    ex_wait(9, stat_in.at[8:16])
    evid[:, mine] = stat_out[8:9, :]
    evid[:, theirs] = stat_in[8:9, :]
    for n in range(NIM // 128):
        evidence_ref[n : n + 1, :] = evid[:, n * 128 : n * 128 + 128]

    @pl.loop(0, 4)
    def _(k):
        p1 = product(1, k)
        for t in range(2):
            a_landed(0, k, t, r_opp)
        s1[k] = (p1 + r_opp[k].astype(F32)).astype(BF16)
        for t in range(2):
            a_copy(1, k, t, s1, r_minus, a_plus[t]).start()
        p3 = product(3, k + 4)
        for t in range(2):
            a_landed(0, k + 4, t, r_opp)
        s3[k + 4] = (p3 + r_opp[k + 4].astype(F32)).astype(BF16)
        for t in range(2):
            a_copy(2, k + 4, t, s3, r_plus, a_minus[t]).start()

    def b_copy(kind, j, t, src, dst, peer):
        return remote(src.at[j, t], dst.at[j, t], b_s.at[kind, j, t], b_r.at[kind, j, t], peer)

    def b_landed(kind, j, t, dst):
        landed(dst.at[j, t], b_s.at[kind, j, t], b_r.at[kind, j, t])

    def y_copy(j, t):
        return remote(y_out.at[j, t], y_in.at[j, t], yy_s.at[j, t], yy_r.at[j, t], y_pal)

    def step_a(k):
        for j, low in ((k, True), (k + 4, False)):
            p = product(0, j)
            for t in range(2):
                a_landed(1, j, t, r_minus)
                a_landed(2, j, t, r_plus)
            acc[j] = p + r_plus[j].astype(F32) + r_minus[j].astype(F32)
            for t in range(2):
                o = t * SIDE
                z2[j, t] = acc[j, o + 64 : o + 96, :].astype(BF16)
                b_copy(0, j, t, z2, zr_opp, b_plus[t] if low else b_minus[t]).start()
                if low:
                    z3[j, t] = acc[j, o + 96 : o + 128, :].astype(BF16)
                    b_copy(2, j, t, z3, zr_plus, b_minus[t]).start()
                else:
                    z1[j, t] = acc[j, o + 32 : o + 64, :].astype(BF16)
                    b_copy(1, j, t, z1, zr_minus, b_plus[t]).start()

    def step_b(k):
        for t in range(2):
            o = t * SIDE
            b_landed(0, k, t, zr_opp)
            z1[k, t] = (acc[k, o + 32 : o + 64, :] + zr_opp[k, t].astype(F32)).astype(BF16)
            b_copy(1, k, t, z1, zr_minus, b_plus[t]).start()
            j = k + 4
            b_landed(0, j, t, zr_opp)
            z3[j, t] = (acc[j, o + 96 : o + 128, :] + zr_opp[j, t].astype(F32)).astype(BF16)
            b_copy(2, j, t, z3, zr_plus, b_minus[t]).start()

    def step_c(k):
        for j in (k, k + 4):
            for t in range(2):
                o = t * SIDE
                b_landed(1, j, t, zr_minus)
                b_landed(2, j, t, zr_plus)
                v = acc[j, o : o + 32, :] + zr_plus[j, t].astype(F32) + zr_minus[j, t].astype(F32)
                y_out[j, t] = v[PIECE:, :].astype(BF16)
                y_copy(j, t).start()
                acc[j, o : o + PIECE, :] = v[:PIECE, :]

    def step_d(k):
        for j in (k, k + 4):
            for t in range(2):
                o = t * SIDE
                y_copy(j, t).wait_recv()
                cols = pl.ds(pl.multiple_of(j * TILE, TILE), TILE)
                out_ref[t * PIECE : (t + 1) * PIECE, cols] = acc[j, o : o + PIECE, :] + y_in[
                    j, t
                ].astype(F32)

    @pl.loop(0, 7)
    def _(k):
        @pl.when(k < 4)
        def _():
            step_a(k)

        @pl.when(jnp.logical_and(k >= 1, k < 5))
        def _():
            step_b(k - 1)

        @pl.when(jnp.logical_and(k >= 2, k < 6))
        def _():
            step_c(k - 2)

        @pl.when(k >= 3)
        def _():
            step_d(k - 3)

    for c in ag_sends:
        c.wait_send()
    for c in ex_sends:
        c.wait_send()

    @pl.loop(0, NT)
    def _(j):
        for t in range(2):
            a_copy(0, j, t, s2, r_opp, core_pal).wait_send()
            a_copy(1, j, t, s1, r_minus, core_pal).wait_send()
            a_copy(2, j, t, s3, r_plus, core_pal).wait_send()
            b_copy(0, j, t, z2, zr_opp, core_pal).wait_send()
            b_copy(1, j, t, z1, zr_minus, core_pal).wait_send()
            b_copy(2, j, t, z3, zr_plus, core_pal).wait_send()
            y_copy(j, t).wait_send()


def shards(
    images, references, shell_of_pixel, noise_power, ref_class, ref_orient, class_logw, orient_logw
):
    vmem = pl.BlockSpec(memory_space=pltpu.VMEM)
    hbm = pl.BlockSpec(memory_space=pl.ANY)
    smem = pl.BlockSpec(memory_space=pltpu.SMEM)
    dma = pltpu.SemaphoreType.DMA
    accumulators, evidence = pl.pallas_call(
        kernel,
        out_shape=(
            jax.ShapeDtypeStruct((ROWS, PIX), F32),
            jax.ShapeDtypeStruct((NIM // 128, 128), F32),
        ),
        in_specs=[hbm, hbm, vmem, vmem, vmem, vmem, vmem, smem],
        out_specs=(vmem, vmem),
        scratch_shapes=[
            pltpu.VMEM((NIM, PIX), BF16),
            pltpu.VMEM((NIM, PIX), BF16),
            pltpu.VMEM((4, GROUP, PIX), BF16),
            pltpu.VMEM((4, GROUP, NIM), F32),
            pltpu.VMEM((4, GROUP, HALF), F32),
            pltpu.VMEM((5, SIDE, HALF), F32),
            pltpu.VMEM((5, SIDE, HALF), F32),
            pltpu.VMEM((5, SIDE, HALF), F32),
            pltpu.VMEM((1, PIX), F32),
            pltpu.VMEM((128, 128), F32),
            pltpu.VMEM((2, 128, 128), F32),
            pltpu.VMEM((2, 5 * SIDE, 1), F32),
            pltpu.VMEM((1, NIM), F32),
            pltpu.VMEM((16, HALF), F32),
            pltpu.VMEM((16, HALF), F32),
            pltpu.VMEM((4, GROUP, NIM), BF16),
            pltpu.VMEM((NT, GROUP, TILE), BF16),
            pltpu.VMEM((NT, GROUP, TILE), BF16),
            pltpu.VMEM((NT, GROUP, TILE), BF16),
            pltpu.VMEM((NT, GROUP, TILE), BF16),
            pltpu.VMEM((NT, GROUP, TILE), BF16),
            pltpu.VMEM((NT, GROUP, TILE), BF16),
            pltpu.VMEM((NT, GROUP, TILE), F32),
            pltpu.VMEM((NT, 2, 32, TILE), BF16),
            pltpu.VMEM((NT, 2, 32, TILE), BF16),
            pltpu.VMEM((NT, 2, 32, TILE), BF16),
            pltpu.VMEM((NT, 2, 32, TILE), BF16),
            pltpu.VMEM((NT, 2, 32, TILE), BF16),
            pltpu.VMEM((NT, 2, 32, TILE), BF16),
            pltpu.VMEM((NT, 2, PIECE, TILE), BF16),
            pltpu.VMEM((NT, 2, PIECE, TILE), BF16),
            dma((5,)),
            dma((84,)),
            dma((84,)),
            dma((24,)),
            dma((24,)),
            dma((3, NT, 2)),
            dma((3, NT, 2)),
            dma((3, NT, 2)),
            dma((3, NT, 2)),
            dma((NT, 2)),
            dma((NT, 2)),
        ],
        compiler_params=pltpu.CompilerParams(
            collective_id=0, has_side_effects=True, vmem_limit_bytes=67043328
        ),
    )(
        images,
        references,
        shell_of_pixel.reshape(1, PIX),
        noise_power.reshape(1, 64),
        ref_class.reshape(NREF // 128, 128),
        ref_orient.reshape(NREF // 128, 128),
        orient_logw.reshape(1, NORIENT),
        class_logw,
    )
    return accumulators, evidence.reshape(NIM)


def solution(mesh):
    placed = (P("img", "shell"), P("img", "shell"), P("shell"), P(), P(), P(), P(), P())
    return jax.shard_map(
        shards, mesh=mesh, in_specs=placed, out_specs=(P("img", "shell"), P("img")), check_vma=False
    )
```

```python
import jax
import jax.numpy as jnp
from jax import lax
from jax.experimental import pallas as pl
from jax.experimental.pallas import tpu as pltpu
from jax.sharding import PartitionSpec as P

INVERSE_HEAT = 0.5
MESH = pl.DeviceIdType.MESH
F32 = jnp.float32
BF16 = jnp.bfloat16

NZ, NY, NX = 4, 2, 4
ROWS = 32
PIECE = 16
PIX = 4096
NIM = 768
HALF = NIM // 2
GROUP = 256
SIDE = GROUP // 2
NREF = 1024
TILE = 512
NT = PIX // TILE
PH = PIX // 2
NORIENT = 6144


def kernel(
    images_hbm,
    references_hbm,
    shell_ref,
    noise_ref,
    class_id_ref,
    orient_id_ref,
    orient_ref,
    class_ref,
    out_ref,
    evidence_ref,
    im,
    wim,
    refs,
    score,
    core_in,
    row_out,
    row_in,
    total,
    weight,
    square,
    columns,
    prior,
    evid,
    stat_out,
    stat_in,
    post,
    s1,
    s2,
    s3,
    r_opp,
    r_plus,
    r_minus,
    acc,
    z1,
    z2,
    z3,
    zr_opp,
    zr_plus,
    zr_minus,
    y_out,
    y_in,
    kept,
    f_out,
    f_in,
    load_sem,
    ag_s,
    ag_r,
    ex_s,
    ex_r,
    a_s,
    a_r,
    b_s,
    b_r,
    yy_s,
    yy_r,
    f_s,
    f_r,
):
    s = lax.axis_index("shell")
    i = lax.axis_index("img")
    core = lax.rem(s, 2)
    y_hi = s // 2
    z = i // (NY * NX)
    y = lax.rem(i // NX, NY)
    x = lax.rem(i, NX)

    def at(zz, yv, xx):
        return (zz * NY + yv) * NX + xx

    x_plus = (s, at(z, y, lax.rem(x + 1, NX)))
    x_minus = (s, at(z, y, lax.rem(x + NX - 1, NX)))
    z_plus = (s, at(lax.rem(z + 1, NZ), y, x))
    z_minus = (s, at(lax.rem(z + NZ - 1, NZ), y, x))
    y_pal = (s, at(z, 1 - y, x))
    core_pal = (y_hi * 2 + 1 - core, i)
    hi_pal = ((1 - y_hi) * 2 + core, i)
    a_plus, a_minus = (x_plus, z_plus), (x_minus, z_minus)
    b_plus, b_minus = (z_plus, x_plus), (z_minus, x_minus)

    def remote(src, dst, send_sem, recv_sem, peer):
        return pltpu.make_async_remote_copy(
            src_ref=src,
            dst_ref=dst,
            send_sem=send_sem,
            recv_sem=recv_sem,
            device_id=peer,
            device_id_type=MESH,
        )

    def landed(dst, send_sem, recv_sem):
        remote(dst, dst, send_sem, recv_sem, core_pal).wait_recv()

    own = []
    for t in range(2):
        c = pltpu.make_async_copy(
            references_hbm.at[pl.ds(t * PIECE, PIECE), :],
            refs.at[0, pl.ds(t * SIDE, PIECE), :],
            load_sem.at[t],
        )
        c.start()
        own.append(c)
    image_loads = []
    for n in range(3):
        c = pltpu.make_async_copy(
            images_hbm.at[pl.ds(n * 256, 256), :], im.at[pl.ds(n * 256, 256), :], load_sem.at[2 + n]
        )
        c.start()
        image_loads.append(c)

    barrier = pltpu.get_barrier_semaphore()
    for peer in (x_plus, x_minus, z_plus, z_minus, y_pal, core_pal, hi_pal):
        pl.semaphore_signal(barrier, inc=1, device_id=peer, device_id_type=MESH)
    pl.semaphore_wait(barrier, 7)

    index = {}
    ag_sends = []

    def slot(name):
        if name not in index:
            index[name] = len(index)
        return index[name]

    def piece(t, a, b, yr, part=None):
        rows = pl.ds(t * SIDE + b * 32 + yr * PIECE, PIECE)
        if part is None:
            return refs.at[a, rows, :]
        return refs.at[a, rows, pl.ds(part * PH, PH)]

    def ag_send(name, src, dst, peer):
        n = slot(name)
        c = remote(src, dst, ag_s.at[n], ag_r.at[n], peer)
        c.start()
        ag_sends.append(c)

    def ag_wait(name, dst):
        n = slot(name)
        landed(dst, ag_s.at[n], ag_r.at[n])

    def send_b(t, yr):
        ag_send(("b+", t, yr), piece(t, 0, 0, yr), piece(t, 0, 3, yr), b_plus[t])
        ag_send(("b-", t, yr), piece(t, 0, 0, yr), piece(t, 0, 1, yr), b_minus[t])

    def send_a(t, b, yr):
        ag_send(("a+", t, b, yr), piece(t, 0, b, yr), piece(t, 3, b, yr), a_plus[t])
        ag_send(("a-", t, b, yr), piece(t, 0, b, yr), piece(t, 1, b, yr), a_minus[t])

    def log_prior():
        square[...] = jnp.zeros((128, 128), F32)
        for n, ids in enumerate((class_id_ref, orient_id_ref)):
            square[0:8, :] = ids[...].astype(F32)
            columns[n] = square[...].T

        def place(block, row, a, b, yr, kind):
            za = lax.rem(z + jnp.where(kind == 0, b, a), NZ)
            xa = lax.rem(x + jnp.where(kind == 0, a, b), NX)
            ya = y if yr == 0 else 1 - y
            first = at(za, ya, xa) * ROWS + kind * PIECE
            rows = pl.ds(pl.multiple_of(lax.rem(first, 128), PIECE), PIECE)
            pick = lax.broadcasted_iota(jnp.int32, (PIECE, 128), 1) == first // 128
            for n in range(2):
                found = jnp.sum(jnp.where(pick, columns[n, rows, :], 0.0), axis=1, keepdims=True)
                prior[n, pl.ds(block * SIDE + row, PIECE), :] = found

        for b in range(4):
            for yr in range(2):
                for g in (0, 1, 3):
                    place(g, b * 32 + yr * PIECE, g, b, yr, y_hi)
                for t in range(2):
                    row = t * 64 + (b % 2) * 32 + yr * PIECE
                    place(2 + 2 * (b // 2), row, 2, b, yr, t)

        @pl.loop(0, 5)
        def _(block):
            rows = pl.ds(pl.multiple_of(block * SIDE, SIDE), SIDE)
            kind = prior[0, rows, :]
            orient = jnp.broadcast_to(prior[1, rows, :], (SIDE, 128)).astype(jnp.int32)

            def add(n, sums):
                cols = pl.ds(pl.multiple_of(n * 128, 128), 128)
                ids = lax.broadcasted_iota(jnp.int32, (SIDE, 128), 1) + n * 128
                logw = jnp.broadcast_to(orient_ref[:, cols], (SIDE, 128))
                return sums + jnp.where(orient == ids, logw, 0.0)

            sums = lax.fori_loop(0, NORIENT // 128, add, jnp.zeros((SIDE, 128), F32))
            found = jnp.zeros((SIDE, 1), F32)
            for n in range(4):
                found = found + jnp.where(kind == float(n), class_ref[n], 0.0)
            prior[0, rows, :] = found + jnp.sum(sums, axis=1, keepdims=True)

    for t in range(2):
        own[t].wait()
    for t in range(2):
        ag_send(("y", t), piece(t, 0, 0, 0), piece(t, 0, 0, 1), y_pal)
    for t in range(2):
        send_b(t, 0)
    for t in range(2):
        send_a(t, 0, 0)

    noise_row = 1.0 / noise_ref[...]
    r64 = lax.broadcasted_iota(jnp.int32, (64, 64), 0)
    c64 = lax.broadcasted_iota(jnp.int32, (64, 64), 1)
    noise_col = jnp.sum(
        jnp.where(r64 == c64, jnp.broadcast_to(noise_row, (64, 64)), 0.0), axis=1, keepdims=True
    )

    @pl.loop(0, PIX // 512)
    def _(n):
        cols = pl.ds(pl.multiple_of(n * 512, 512), 512)
        shell = jnp.broadcast_to(shell_ref[:, cols], (64, 512))
        hit = shell == lax.broadcasted_iota(jnp.int32, (64, 512), 0)
        weight[:, cols] = jnp.sum(
            jnp.where(hit, jnp.broadcast_to(noise_col, (64, 512)), 0.0), axis=0, keepdims=True
        )

    for t in range(2):
        ag_wait(("y", t), piece(t, 0, 0, 1))
        send_b(t, 1)
    for t in range(2):
        send_a(t, 0, 1)

    for n in range(3):
        image_loads[n].wait()

        @pl.loop(n * 16, n * 16 + 16)
        def _(k):
            rows = pl.ds(pl.multiple_of(k * 16, 16), 16)
            wim[rows, :] = (im[rows, :].astype(F32) * weight[...]).astype(BF16)

    for yr in range(2):
        for t in range(2):
            ag_wait(("b+", t, yr), piece(t, 0, 3, yr))
            ag_send(("bf+", t, yr), piece(t, 0, 3, yr, 0), piece(t, 0, 2, yr, 0), b_plus[t])
            ag_wait(("b-", t, yr), piece(t, 0, 1, yr))
            ag_send(("bf-", t, yr), piece(t, 0, 1, yr, 1), piece(t, 0, 2, yr, 1), b_minus[t])
        for t in range(2):
            send_a(t, 3, yr)
            send_a(t, 1, yr)
        if yr == 0:
            log_prior()

    for yr in range(2):
        for t in range(2):
            ag_wait(("bf+", t, yr), piece(t, 0, 2, yr, 0))
            ag_wait(("bf-", t, yr), piece(t, 0, 2, yr, 1))
            send_a(t, 2, yr)

    mine = pl.ds(pl.multiple_of(core * HALF, 128), HALF)
    theirs = pl.ds(pl.multiple_of((1 - core) * HALF, 128), HALF)
    keep = pl.ds(pl.multiple_of(y_hi * SIDE, SIDE), SIDE)
    give = pl.ds(pl.multiple_of((1 - y_hi) * SIDE, SIDE), SIDE)
    ex_sends = []

    def ex_send(n, src, dst, peer):
        c = remote(src, dst, ex_s.at[n], ex_r.at[n], peer)
        c.start()
        ex_sends.append(c)

    def ex_wait(n, dst):
        landed(dst, ex_s.at[n], ex_r.at[n])

    def scores(r, out, n_rows):
        def add(n, sums):
            cols = pl.ds(pl.multiple_of(n * 128, 128), 128)
            part = r(cols).astype(F32)
            return sums + part * part * weight[:, cols]

        sums = lax.fori_loop(0, PIX // 128, add, jnp.zeros((n_rows, 128), F32))
        norm = 0.5 * jnp.sum(sums, axis=1, keepdims=True)

        @pl.loop(0, 3)
        def _(n):
            rows = pl.ds(pl.multiple_of(n * 256, 256), 256)
            part = lax.dot_general(
                r(slice(None)), wim[rows, :], (((1,), (1,)), ((), ())), preferred_element_type=F32
            )
            out[:, rows] = part - norm

    def do_scores(g):
        scores(lambda cols: refs[g, :, cols], score.at[g], GROUP)
        ex_send(g, score.at[g, :, theirs], core_in.at[g], core_pal)

    def do_rows(g):
        ex_wait(g, core_in.at[g])
        row_out[g] = score[g, give, mine] + core_in[g, give, :]
        ex_send(4 + g, row_out.at[g], row_in.at[g], hi_pal)
        total[g] = score[g, keep, mine] + core_in[g, keep, :]

    half_rows = (pl.ds(0, SIDE), pl.ds(SIDE, SIDE))

    def do_scores_2(h):
        def r(cols):
            low = refs[2, h * 64 : h * 64 + 64, cols]
            return jnp.concatenate([low, refs[2, SIDE + h * 64 : SIDE + h * 64 + 64, cols]], axis=0)

        scores(r, score.at[2, half_rows[h]], SIDE)
        n = (2, 10)[h]
        ex_send(n, score.at[2, half_rows[h], theirs], core_in.at[2, half_rows[h]], core_pal)

    def do_rows_2(h):
        ex_wait((2, 10)[h], core_in.at[2, half_rows[h]])
        block = 2 + 2 * h
        row_out[block] = score[2, half_rows[h], mine] + core_in[2, half_rows[h], :]
        ex_send((6, 11)[h], row_out.at[block], row_in.at[block], hi_pal)

    def do_logits(block):
        rows = pl.ds(block * SIDE, SIDE)
        if block in (2, 4):
            ex_wait({2: 6, 4: 11}[block], row_in.at[block])
            summed = row_out[block] + row_in[block]
        else:
            ex_wait(4 + block, row_in.at[block])
            summed = total[block] + row_in[block]
        logits = INVERSE_HEAT * summed + prior[0, rows, :]
        total[block] = logits
        return jnp.max(logits, axis=0, keepdims=True)

    def mass_of(blocks, top):
        mass = jnp.zeros((1, HALF), F32)
        for block in blocks:
            mass = mass + jnp.sum(jnp.exp(total[block] - top), axis=0, keepdims=True)
        return mass

    do_scores(0)
    order = [(0, 0), (0, 1), (3, 0), (1, 0), (3, 1), (1, 1), (2, 0), (2, 1)]
    forward = [(0, 0), (0, 1), (1, 0), (1, 1), (3, 0), (3, 1), (2, 0), (2, 1)]
    arrived = []
    passed = 0
    for n, (b, yr) in enumerate(order):
        for t in range(2):
            ag_wait(("a+", t, b, yr), piece(t, 3, b, yr))
            ag_wait(("a-", t, b, yr), piece(t, 1, b, yr))
        arrived.append((b, yr))
        while passed < 8 and forward[passed] in arrived:
            b, yr = forward[passed]
            for t in range(2):
                ag_send(("af+", t, b, yr), piece(t, 3, b, yr, 0), piece(t, 2, b, yr, 0), a_plus[t])
                ag_send(("af-", t, b, yr), piece(t, 1, b, yr, 1), piece(t, 2, b, yr, 1), a_minus[t])
            passed += 1
        if n == 1:
            do_rows(0)
    do_scores(1)
    do_scores(3)
    do_rows(1)
    do_rows(3)

    def opposite_landed(pieces):
        for b, yr in pieces:
            for t in range(2):
                ag_wait(("af+", t, b, yr), piece(t, 2, b, yr, 0))
                ag_wait(("af-", t, b, yr), piece(t, 2, b, yr, 1))

    opposite_landed(forward[:4])
    do_scores_2(0)
    top = do_logits(0)
    do_rows_2(0)
    opposite_landed(forward[4:])
    do_scores_2(1)
    top = jnp.maximum(top, do_logits(1))
    top = jnp.maximum(top, do_logits(3))
    mass = mass_of((0, 1, 3), top)
    stat_out[0:1, :] = top
    stat_out[1:2, :] = mass
    do_rows_2(1)
    ex_send(8, stat_out.at[0:8], stat_in.at[0:8], hi_pal)
    last_top = do_logits(2)
    ex_wait(8, stat_in.at[0:8])
    other_top, other_mass = stat_in[0:1, :], stat_in[1:2, :]
    first = y_hi == 0
    top_a, top_b = jnp.where(first, top, other_top), jnp.where(first, other_top, top)
    mass_a, mass_b = jnp.where(first, mass, other_mass), jnp.where(first, other_mass, mass)
    last_top = jnp.maximum(last_top, do_logits(4))
    best = jnp.maximum(jnp.maximum(top_a, top_b), last_top)
    evidence = best + jnp.log(
        mass_a * jnp.exp(top_a - best) + mass_b * jnp.exp(top_b - best) + mass_of((2, 4), best)
    )
    for h in range(2):
        p = jnp.exp(total[2 + 2 * h] - evidence).astype(BF16)
        for t in range(2):
            rows = pl.ds(t * SIDE + h * 64, 64)
            post[2, rows, mine] = p[t * 64 : t * 64 + 64, :]
    ex_send(18, post.at[2, :, mine], post.at[2, :, mine], core_pal)
    stat_out[8:16, :] = jnp.broadcast_to(evidence, (8, HALF))
    for g in (1, 3, 0):
        post[g, keep, mine] = jnp.exp(total[g] - evidence).astype(BF16)
        ex_send(12 + g, post.at[g, keep, mine], post.at[g, keep, mine], hi_pal)
        ex_send(16 + g, post.at[g, keep, mine], post.at[g, keep, mine], core_pal)
    ex_send(9, stat_out.at[8:16], stat_in.at[8:16], core_pal)

    def do_relay(g):
        ex_wait(12 + g, post.at[g, give, mine])
        ex_send(20 + g, post.at[g, give, mine], post.at[g, give, mine], core_pal)

    def do_posterior(g):
        ex_wait(16 + g, post.at[g, keep, theirs])
        ex_wait(20 + g, post.at[g, give, theirs])

    def product(g, j):
        cols = pl.ds(pl.multiple_of(j * TILE, TILE), TILE)
        return jnp.dot(post[g], im[:, cols], preferred_element_type=F32)

    def a_rows(j, t):
        return pl.ds(t * SIDE, 64 if isinstance(j, int) and j % 4 == 3 else SIDE)

    def a_copy(kind, j, t, src, dst, peer):
        rows = a_rows(j, t)
        return remote(
            src.at[j, rows], dst.at[j, rows], a_s.at[kind, j, t], a_r.at[kind, j, t], peer
        )

    def a_landed(kind, j, t, dst):
        landed(dst.at[j, a_rows(j, t)], a_s.at[kind, j, t], a_r.at[kind, j, t])

    def f_copy(g, n):
        return remote(f_out.at[n, g], f_in.at[n, g], f_s.at[n, g], f_r.at[n, g], y_pal)

    def first_product(g, n):
        p = product(g, 3 + 4 * n).reshape(8, 2, PIECE, TILE)
        f_out[n, g] = p[:, 1].reshape(SIDE, TILE).astype(BF16)
        f_copy(g, n).start()
        kept[n, g] = p[:, 0].reshape(SIDE, TILE)

    def first_sum(g, n):
        f_copy(g, n).wait_recv()
        return kept[n, g] + f_in[n, g].astype(F32)

    def put(dst, j, rows):
        for t in range(2):
            dst[j, a_rows(j, t)] = rows[t * 64 : t * 64 + 64, :].astype(BF16)

    def get(src, j):
        return jnp.concatenate([src[j, a_rows(j, t)] for t in range(2)], axis=0).astype(F32)

    ex_wait(18, post.at[2, :, theirs])

    @pl.loop(0, 3)
    def _(k):
        s2[k] = product(2, k).astype(BF16)
        for t in range(2):
            a_copy(0, k, t, s2, r_opp, a_plus[t]).start()
        s2[k + 4] = product(2, k + 4).astype(BF16)
        for t in range(2):
            a_copy(0, k + 4, t, s2, r_opp, a_minus[t]).start()

    for n in range(2):
        first_product(2, n)
    do_relay(1)
    do_relay(3)
    do_posterior(1)
    do_posterior(3)

    @pl.loop(0, 3)
    def _(k):
        s1[k + 4] = product(1, k + 4).astype(BF16)
        for t in range(2):
            a_copy(1, k + 4, t, s1, r_minus, a_plus[t]).start()
        s3[k] = product(3, k).astype(BF16)
        for t in range(2):
            a_copy(2, k, t, s3, r_plus, a_minus[t]).start()

    first_product(1, 1)
    first_product(3, 0)
    first_product(1, 0)
    first_product(3, 1)
    do_relay(0)
    do_posterior(0)
    for n in range(2):
        first_product(0, n)

    @pl.loop(0, 3)
    def _(k):
        p1 = product(1, k)
        for t in range(2):
            a_landed(0, k, t, r_opp)
        s1[k] = (p1 + r_opp[k].astype(F32)).astype(BF16)
        for t in range(2):
            a_copy(1, k, t, s1, r_minus, a_plus[t]).start()
        p3 = product(3, k + 4)
        for t in range(2):
            a_landed(0, k + 4, t, r_opp)
        s3[k + 4] = (p3 + r_opp[k + 4].astype(F32)).astype(BF16)
        for t in range(2):
            a_copy(2, k + 4, t, s3, r_plus, a_minus[t]).start()

    ex_wait(9, stat_in.at[8:16])
    evid[:, mine] = stat_out[8:9, :]
    evid[:, theirs] = stat_in[8:9, :]
    for n in range(NIM // 128):
        evidence_ref[n : n + 1, :] = evid[:, n * 128 : n * 128 + 128]

    def b_copy(kind, j, t, src, dst, peer):
        rows = pl.ds(0, PIECE if j % 4 == 3 else 32)
        return remote(
            src.at[j, t, rows], dst.at[j, t, rows], b_s.at[kind, j, t], b_r.at[kind, j, t], peer
        )

    def b_landed(kind, j, t, dst):
        b_copy(kind, j, t, dst, dst, core_pal).wait_recv()

    def y_copy(j, t):
        return remote(y_out.at[j, t], y_in.at[j, t], yy_s.at[j, t], yy_r.at[j, t], y_pal)

    def first_opposite():
        for n, j in enumerate((3, 7)):
            put(s2, j, first_sum(2, n))
            for t in range(2):
                a_copy(0, j, t, s2, r_opp, (a_plus, a_minus)[n][t]).start()

    def first_free():
        put(s1, 7, first_sum(1, 1))
        for t in range(2):
            a_copy(1, 7, t, s1, r_minus, a_plus[t]).start()
        put(s3, 3, first_sum(3, 0))
        for t in range(2):
            a_copy(2, 3, t, s3, r_plus, a_minus[t]).start()

    def first_bound():
        for t in range(2):
            a_landed(0, 3, t, r_opp)
        put(s1, 3, first_sum(1, 0) + get(r_opp, 3))
        for t in range(2):
            a_copy(1, 3, t, s1, r_minus, a_plus[t]).start()
        for t in range(2):
            a_landed(0, 7, t, r_opp)
        put(s3, 7, first_sum(3, 1) + get(r_opp, 7))
        for t in range(2):
            a_copy(2, 7, t, s3, r_plus, a_minus[t]).start()

    def rows_of(j, t, b):
        n = PIECE if j % 4 == 3 else 32
        return pl.ds(t * SIDE + b * n, n)

    def step_a(k):
        for j, low in ((k, True), (k + 4, False)):
            p = None if k == 3 else product(0, j)
            for t in range(2):
                a_landed(1, j, t, r_minus)
                a_landed(2, j, t, r_plus)
            if k == 3:
                total_j = first_sum(0, j // 4) + get(r_plus, j) + get(r_minus, j)
                for t in range(2):
                    acc[j, a_rows(j, t)] = total_j[t * 64 : t * 64 + 64, :]
            else:
                acc[j] = p + r_plus[j].astype(F32) + r_minus[j].astype(F32)
            n = PIECE if k == 3 else 32
            for t in range(2):
                z2[j, t, 0:n] = acc[j, rows_of(j, t, 2), :].astype(BF16)
                b_copy(0, j, t, z2, zr_opp, b_plus[t] if low else b_minus[t]).start()
                if low:
                    z3[j, t, 0:n] = acc[j, rows_of(j, t, 3), :].astype(BF16)
                    b_copy(2, j, t, z3, zr_plus, b_minus[t]).start()
                else:
                    z1[j, t, 0:n] = acc[j, rows_of(j, t, 1), :].astype(BF16)
                    b_copy(1, j, t, z1, zr_minus, b_plus[t]).start()

    def step_b(k):
        n = PIECE if k == 3 else 32
        for t in range(2):
            b_landed(0, k, t, zr_opp)
            v = acc[k, rows_of(k, t, 1), :] + zr_opp[k, t, 0:n].astype(F32)
            z1[k, t, 0:n] = v.astype(BF16)
            b_copy(1, k, t, z1, zr_minus, b_plus[t]).start()
            j = k + 4
            b_landed(0, j, t, zr_opp)
            v = acc[j, rows_of(j, t, 3), :] + zr_opp[j, t, 0:n].astype(F32)
            z3[j, t, 0:n] = v.astype(BF16)
            b_copy(2, j, t, z3, zr_plus, b_minus[t]).start()

    def step_c(k):
        n = PIECE if k == 3 else 32
        for j in (k, k + 4):
            cols = pl.ds(j * TILE, TILE)
            for t in range(2):
                b_landed(1, j, t, zr_minus)
                b_landed(2, j, t, zr_plus)
                v = acc[j, rows_of(j, t, 0), :] + zr_plus[j, t, 0:n].astype(F32)
                v = v + zr_minus[j, t, 0:n].astype(F32)
                out_ref[t * PIECE : (t + 1) * PIECE, cols] = v[:PIECE, :]
                if k < 3:
                    y_out[j, t] = v[PIECE:, :].astype(BF16)
                    y_copy(j, t).start()

    def step_d(k):
        for j in (k, k + 4):
            cols = pl.ds(j * TILE, TILE)
            for t in range(2):
                y_copy(j, t).wait_recv()
                rows = slice(t * PIECE, (t + 1) * PIECE)
                out_ref[rows, cols] = out_ref[rows, cols] + y_in[j, t].astype(F32)

    first_opposite()
    step_a(0)
    first_free()
    step_a(1)
    step_b(0)
    first_bound()
    step_a(2)
    step_b(1)
    step_a(3)
    step_b(2)
    step_c(0)
    step_b(3)
    step_c(1)
    step_c(2)
    step_c(3)
    for k in range(3):
        step_d(k)

    for c in ag_sends:
        c.wait_send()
    for c in ex_sends:
        c.wait_send()

    for j in range(NT):
        for t in range(2):
            a_copy(0, j, t, s2, r_opp, core_pal).wait_send()
            a_copy(1, j, t, s1, r_minus, core_pal).wait_send()
            a_copy(2, j, t, s3, r_plus, core_pal).wait_send()
            b_copy(0, j, t, z2, zr_opp, core_pal).wait_send()
            b_copy(1, j, t, z1, zr_minus, core_pal).wait_send()
            b_copy(2, j, t, z3, zr_plus, core_pal).wait_send()
            if j % 4 < 3:
                y_copy(j, t).wait_send()
    for n in range(2):
        for g in range(4):
            f_copy(g, n).wait_send()


def shards(
    images, references, shell_of_pixel, noise_power, ref_class, ref_orient, class_logw, orient_logw
):
    vmem = pl.BlockSpec(memory_space=pltpu.VMEM)
    hbm = pl.BlockSpec(memory_space=pl.ANY)
    smem = pl.BlockSpec(memory_space=pltpu.SMEM)
    dma = pltpu.SemaphoreType.DMA
    accumulators, evidence = pl.pallas_call(
        kernel,
        out_shape=(
            jax.ShapeDtypeStruct((ROWS, PIX), F32),
            jax.ShapeDtypeStruct((NIM // 128, 128), F32),
        ),
        in_specs=[hbm, hbm, vmem, vmem, vmem, vmem, vmem, smem],
        out_specs=(vmem, vmem),
        scratch_shapes=[
            pltpu.VMEM((NIM, PIX), BF16),
            pltpu.VMEM((NIM, PIX), BF16),
            pltpu.VMEM((4, GROUP, PIX), BF16),
            pltpu.VMEM((4, GROUP, NIM), F32),
            pltpu.VMEM((4, GROUP, HALF), F32),
            pltpu.VMEM((5, SIDE, HALF), F32),
            pltpu.VMEM((5, SIDE, HALF), F32),
            pltpu.VMEM((5, SIDE, HALF), F32),
            pltpu.VMEM((1, PIX), F32),
            pltpu.VMEM((128, 128), F32),
            pltpu.VMEM((2, 128, 128), F32),
            pltpu.VMEM((2, 5 * SIDE, 1), F32),
            pltpu.VMEM((1, NIM), F32),
            pltpu.VMEM((16, HALF), F32),
            pltpu.VMEM((16, HALF), F32),
            pltpu.VMEM((4, GROUP, NIM), BF16),
            pltpu.VMEM((NT, GROUP, TILE), BF16),
            pltpu.VMEM((NT, GROUP, TILE), BF16),
            pltpu.VMEM((NT, GROUP, TILE), BF16),
            pltpu.VMEM((NT, GROUP, TILE), BF16),
            pltpu.VMEM((NT, GROUP, TILE), BF16),
            pltpu.VMEM((NT, GROUP, TILE), BF16),
            pltpu.VMEM((NT, GROUP, TILE), F32),
            pltpu.VMEM((NT, 2, 32, TILE), BF16),
            pltpu.VMEM((NT, 2, 32, TILE), BF16),
            pltpu.VMEM((NT, 2, 32, TILE), BF16),
            pltpu.VMEM((NT, 2, 32, TILE), BF16),
            pltpu.VMEM((NT, 2, 32, TILE), BF16),
            pltpu.VMEM((NT, 2, 32, TILE), BF16),
            pltpu.VMEM((NT, 2, PIECE, TILE), BF16),
            pltpu.VMEM((NT, 2, PIECE, TILE), BF16),
            pltpu.VMEM((2, 4, SIDE, TILE), F32),
            pltpu.VMEM((2, 4, SIDE, TILE), BF16),
            pltpu.VMEM((2, 4, SIDE, TILE), BF16),
            dma((5,)),
            dma((84,)),
            dma((84,)),
            dma((24,)),
            dma((24,)),
            dma((3, NT, 2)),
            dma((3, NT, 2)),
            dma((3, NT, 2)),
            dma((3, NT, 2)),
            dma((NT, 2)),
            dma((NT, 2)),
            dma((2, 4)),
            dma((2, 4)),
        ],
        compiler_params=pltpu.CompilerParams(
            collective_id=0, has_side_effects=True, vmem_limit_bytes=67043328
        ),
    )(
        images,
        references,
        shell_of_pixel.reshape(1, PIX),
        noise_power.reshape(1, 64),
        ref_class.reshape(NREF // 128, 128),
        ref_orient.reshape(NREF // 128, 128),
        orient_logw.reshape(1, NORIENT),
        class_logw,
    )
    return accumulators, evidence.reshape(NIM)


def solution(mesh):
    placed = (P("img", "shell"), P("img", "shell"), P("shell"), P(), P(), P(), P(), P())
    return jax.shard_map(
        shards, mesh=mesh, in_specs=placed, out_specs=(P("img", "shell"), P("img")), check_vma=False
    )
```

```python
import jax
import jax.numpy as jnp
from jax import lax
from jax.experimental import pallas as pl
from jax.experimental.pallas import tpu as pltpu
from jax.sharding import PartitionSpec as P

INVERSE_HEAT = 0.5
MESH = pl.DeviceIdType.MESH
F32 = jnp.float32
BF16 = jnp.bfloat16

NZ, NY, NX = 4, 2, 4
ROWS = 32
PIECE = 16
PIX = 4096
NIM = 768
HALF = NIM // 2
GROUP = 256
SIDE = GROUP // 2
NREF = 1024
TILE = 512
NT = PIX // TILE
PH = PIX // 2
NORIENT = 6144

FORWARD = [(0, 0), (0, 1), (3, 0), (1, 0), (3, 1), (1, 1), (2, 0), (2, 1)]
BATCHES = [
    [(0, b, yr) for b, yr in FORWARD],
    [(g, b, yr) for g in (1, 3) for b, yr in FORWARD[:4]],
    [(g, b, yr) for g in (1, 3) for b, yr in FORWARD[4:]],
    [(2, b, yr) for b, yr in FORWARD[:4]],
    [(2, b, yr) for b, yr in FORWARD[4:6]],
    [(2, b, yr) for b, yr in FORWARD[6:]],
]
FIRST = [0, SIDE, 2 * SIDE, 3 * SIDE, 4 * SIDE, 4 * SIDE + 64]


def kernel(
    images_hbm,
    references_hbm,
    shell_ref,
    noise_ref,
    class_id_ref,
    orient_id_ref,
    orient_ref,
    class_ref,
    out_ref,
    evidence_ref,
    im,
    wim,
    refs,
    score,
    core_in,
    row_out,
    row_in,
    total,
    weight,
    square,
    columns,
    prior,
    evid,
    stat_out,
    stat_in,
    post,
    s1,
    s2,
    s3,
    r_opp,
    r_plus,
    r_minus,
    acc,
    z1,
    z2,
    z3,
    zr_opp,
    zr_plus,
    zr_minus,
    y_out,
    y_in,
    kept,
    f_out,
    f_in,
    load_sem,
    ag_s,
    ag_r,
    ex_s,
    ex_r,
    a_s,
    a_r,
    b_s,
    b_r,
    yy_s,
    yy_r,
    f_s,
    f_r,
):
    s = lax.axis_index("shell")
    i = lax.axis_index("img")
    core = lax.rem(s, 2)
    y_hi = s // 2
    z = i // (NY * NX)
    y = lax.rem(i // NX, NY)
    x = lax.rem(i, NX)

    def at(zz, yv, xx):
        return (zz * NY + yv) * NX + xx

    x_plus = (s, at(z, y, lax.rem(x + 1, NX)))
    x_minus = (s, at(z, y, lax.rem(x + NX - 1, NX)))
    z_plus = (s, at(lax.rem(z + 1, NZ), y, x))
    z_minus = (s, at(lax.rem(z + NZ - 1, NZ), y, x))
    y_pal = (s, at(z, 1 - y, x))
    core_pal = (y_hi * 2 + 1 - core, i)
    hi_pal = ((1 - y_hi) * 2 + core, i)
    a_plus, a_minus = (x_plus, z_plus), (x_minus, z_minus)
    b_plus, b_minus = (z_plus, x_plus), (z_minus, x_minus)

    def remote(src, dst, send_sem, recv_sem, peer):
        return pltpu.make_async_remote_copy(
            src_ref=src,
            dst_ref=dst,
            send_sem=send_sem,
            recv_sem=recv_sem,
            device_id=peer,
            device_id_type=MESH,
        )

    def landed(dst, send_sem, recv_sem):
        remote(dst, dst, send_sem, recv_sem, core_pal).wait_recv()

    own = []
    for t in range(2):
        c = pltpu.make_async_copy(
            references_hbm.at[pl.ds(t * PIECE, PIECE), :],
            refs.at[0, pl.ds(t * SIDE, PIECE), :],
            load_sem.at[t],
        )
        c.start()
        own.append(c)
    image_loads = []
    for n in range(3):
        c = pltpu.make_async_copy(
            images_hbm.at[pl.ds(n * 256, 256), :], im.at[pl.ds(n * 256, 256), :], load_sem.at[2 + n]
        )
        c.start()
        image_loads.append(c)

    barrier = pltpu.get_barrier_semaphore()
    for peer in (x_plus, x_minus, z_plus, z_minus, y_pal, core_pal, hi_pal):
        pl.semaphore_signal(barrier, inc=1, device_id=peer, device_id_type=MESH)
    pl.semaphore_wait(barrier, 7)

    index = {}
    ag_sends = []

    def slot(name):
        if name not in index:
            index[name] = len(index)
        return index[name]

    def piece(t, a, b, yr, part=None):
        rows = pl.ds(t * SIDE + b * 32 + yr * PIECE, PIECE)
        if part is None:
            return refs.at[a, rows, :]
        return refs.at[a, rows, pl.ds(part * PH, PH)]

    def ag_send(name, src, dst, peer):
        n = slot(name)
        c = remote(src, dst, ag_s.at[n], ag_r.at[n], peer)
        c.start()
        ag_sends.append(c)

    def ag_wait(name, dst):
        n = slot(name)
        landed(dst, ag_s.at[n], ag_r.at[n])

    def send_b(t, yr):
        ag_send(("b+", t, yr), piece(t, 0, 0, yr), piece(t, 0, 3, yr), b_plus[t])
        ag_send(("b-", t, yr), piece(t, 0, 0, yr), piece(t, 0, 1, yr), b_minus[t])

    def send_a(t, b, yr):
        ag_send(("a+", t, b, yr), piece(t, 0, b, yr), piece(t, 3, b, yr), a_plus[t])
        ag_send(("a-", t, b, yr), piece(t, 0, b, yr), piece(t, 1, b, yr), a_minus[t])

    def log_prior():
        square[...] = jnp.zeros((128, 128), F32)
        for n, ids in enumerate((class_id_ref, orient_id_ref)):
            square[0:8, :] = ids[...].astype(F32)
            columns[n] = square[...].T

        def place(row, a, b, yr, kind):
            za = lax.rem(z + jnp.where(kind == 0, b, a), NZ)
            xa = lax.rem(x + jnp.where(kind == 0, a, b), NX)
            ya = y if yr == 0 else 1 - y
            first = at(za, ya, xa) * ROWS + kind * PIECE
            rows = pl.ds(pl.multiple_of(lax.rem(first, 128), PIECE), PIECE)
            pick = lax.broadcasted_iota(jnp.int32, (PIECE, 128), 1) == first // 128
            for n in range(2):
                found = jnp.sum(jnp.where(pick, columns[n, rows, :], 0.0), axis=1, keepdims=True)
                prior[n, pl.ds(row, PIECE), :] = found

        for n, batch in enumerate(BATCHES):
            for k, (g, b, yr) in enumerate(batch):
                if n < 3:
                    place(FIRST[n] + k * PIECE, g, b, yr, y_hi)
                else:
                    for t in range(2):
                        place(FIRST[n] + (t * len(batch) + k) * PIECE, g, b, yr, t)

        @pl.loop(0, 5)
        def _(block):
            rows = pl.ds(pl.multiple_of(block * SIDE, SIDE), SIDE)
            kind = prior[0, rows, :]
            orient = jnp.broadcast_to(prior[1, rows, :], (SIDE, 128)).astype(jnp.int32)

            def add(n, sums):
                cols = pl.ds(pl.multiple_of(n * 128, 128), 128)
                ids = lax.broadcasted_iota(jnp.int32, (SIDE, 128), 1) + n * 128
                logw = jnp.broadcast_to(orient_ref[:, cols], (SIDE, 128))
                return sums + jnp.where(orient == ids, logw, 0.0)

            sums = lax.fori_loop(0, NORIENT // 128, add, jnp.zeros((SIDE, 128), F32))
            found = jnp.zeros((SIDE, 1), F32)
            for n in range(4):
                found = found + jnp.where(kind == float(n), class_ref[n], 0.0)
            prior[0, rows, :] = found + jnp.sum(sums, axis=1, keepdims=True)

    for t in range(2):
        own[t].wait()
    for t in range(2):
        ag_send(("y", t), piece(t, 0, 0, 0), piece(t, 0, 0, 1), y_pal)
    for t in range(2):
        send_b(t, 0)
    for t in range(2):
        send_a(t, 0, 0)

    noise_row = 1.0 / noise_ref[...]
    r64 = lax.broadcasted_iota(jnp.int32, (64, 64), 0)
    c64 = lax.broadcasted_iota(jnp.int32, (64, 64), 1)
    noise_col = jnp.sum(
        jnp.where(r64 == c64, jnp.broadcast_to(noise_row, (64, 64)), 0.0), axis=1, keepdims=True
    )

    @pl.loop(0, PIX // 512)
    def _(n):
        cols = pl.ds(pl.multiple_of(n * 512, 512), 512)
        shell = jnp.broadcast_to(shell_ref[:, cols], (64, 512))
        hit = shell == lax.broadcasted_iota(jnp.int32, (64, 512), 0)
        weight[:, cols] = jnp.sum(
            jnp.where(hit, jnp.broadcast_to(noise_col, (64, 512)), 0.0), axis=0, keepdims=True
        )

    for t in range(2):
        ag_wait(("y", t), piece(t, 0, 0, 1))
        send_b(t, 1)
    for t in range(2):
        send_a(t, 0, 1)

    for n in range(3):
        image_loads[n].wait()

        @pl.loop(n * 16, n * 16 + 16)
        def _(k):
            rows = pl.ds(pl.multiple_of(k * 16, 16), 16)
            wim[rows, :] = (im[rows, :].astype(F32) * weight[...]).astype(BF16)

    def pass_b(yr):
        for t in range(2):
            ag_wait(("b+", t, yr), piece(t, 0, 3, yr))
            ag_send(("bf+", t, yr), piece(t, 0, 3, yr, 0), piece(t, 0, 2, yr, 0), b_plus[t])
            ag_wait(("b-", t, yr), piece(t, 0, 1, yr))
            ag_send(("bf-", t, yr), piece(t, 0, 1, yr, 1), piece(t, 0, 2, yr, 1), b_minus[t])
        for t in range(2):
            send_a(t, 3, yr)
            send_a(t, 1, yr)

    def pass_a(b, yr):
        for t in range(2):
            ag_wait(("a+", t, b, yr), piece(t, 3, b, yr))
            ag_send(("af+", t, b, yr), piece(t, 3, b, yr, 0), piece(t, 2, b, yr, 0), a_plus[t])
            ag_wait(("a-", t, b, yr), piece(t, 1, b, yr))
            ag_send(("af-", t, b, yr), piece(t, 1, b, yr, 1), piece(t, 2, b, yr, 1), a_minus[t])

    def opposite_landed(pieces):
        for b, yr in pieces:
            for t in range(2):
                ag_wait(("af+", t, b, yr), piece(t, 2, b, yr, 0))
                ag_wait(("af-", t, b, yr), piece(t, 2, b, yr, 1))

    pass_b(0)
    log_prior()
    pass_a(0, 0)
    pass_a(0, 1)
    pass_b(1)
    pass_a(3, 0)
    pass_a(1, 0)
    for yr in range(2):
        for t in range(2):
            ag_wait(("bf+", t, yr), piece(t, 0, 2, yr, 0))
            ag_wait(("bf-", t, yr), piece(t, 0, 2, yr, 1))
            send_a(t, 2, yr)

    mine = pl.ds(pl.multiple_of(core * HALF, 128), HALF)
    theirs = pl.ds(pl.multiple_of((1 - core) * HALF, 128), HALF)
    keep = pl.ds(pl.multiple_of(y_hi * SIDE, SIDE), SIDE)
    give = pl.ds(pl.multiple_of((1 - y_hi) * SIDE, SIDE), SIDE)
    ex_sends = []

    def ex_send(n, src, dst, peer):
        c = remote(src, dst, ex_s.at[n], ex_r.at[n], peer)
        c.start()
        ex_sends.append(c)

    def ex_wait(n, dst):
        landed(dst, ex_s.at[n], ex_r.at[n])

    def places(n):
        rows = 2 * PIECE * len(BATCHES[n])
        return (n, pl.ds(0, rows)) if n < 3 else (3, pl.ds(FIRST[n] - FIRST[3], rows))

    def sums_place(n):
        rows = SIDE if n < 3 else 2 * PIECE * len(BATCHES[n])
        return (FIRST[n] // SIDE, pl.ds(FIRST[n] % SIDE, rows))

    def do_scores(n):
        batch = BATCHES[n]
        n_rows = 2 * PIECE * len(batch)
        slot_n, rows = places(n)

        def of(cols):
            return jnp.concatenate(
                [
                    refs[g, t * SIDE + b * 32 + yr * PIECE : t * SIDE + b * 32 + (yr + 1) * PIECE, cols]
                    for t in range(2)
                    for g, b, yr in batch
                ],
                axis=0,
            )

        def add(k, sums):
            for u in range(4):
                cols = pl.ds(pl.multiple_of(k * 512 + u * 128, 128), 128)
                part = of(cols).astype(F32)
                sums = sums + part * part * weight[:, cols]
            return sums

        sums = lax.fori_loop(0, PIX // 512, add, jnp.zeros((n_rows, 128), F32))
        norm = 0.5 * jnp.sum(sums, axis=1, keepdims=True)
        part = lax.dot_general(
            of(slice(None)), wim[...], (((1,), (1,)), ((), ())), preferred_element_type=F32
        )
        score[slot_n, rows, :] = part - norm
        ex_send(n, score.at[slot_n, rows, theirs], core_in.at[slot_n, rows], core_pal)

    def do_rows(n):
        slot_n, rows = places(n)
        block, sums = sums_place(n)
        ex_wait(n, core_in.at[slot_n, rows])
        if n < 3:
            row_out[block] = score[n, give, mine] + core_in[n, give, :]
            total[block] = score[n, keep, mine] + core_in[n, keep, :]
        else:
            row_out[block, sums] = score[3, rows, mine] + core_in[3, rows, :]
        ex_send(6 + n, row_out.at[block, sums], row_in.at[block, sums], hi_pal)

    def do_logits(n):
        block, sums = sums_place(n)
        ex_wait(6 + n, row_in.at[block, sums])
        near = total if n < 3 else row_out
        first_row = FIRST[n]
        size = SIDE if n < 3 else 2 * PIECE * len(BATCHES[n])
        logits = INVERSE_HEAT * (near[block, sums] + row_in[block, sums])
        logits = logits + prior[0, pl.ds(first_row, size), :]
        total[block, sums] = logits
        return jnp.max(logits, axis=0, keepdims=True)

    def mass_of(blocks, top):
        mass = jnp.zeros((1, HALF), F32)
        for block in blocks:
            mass = mass + jnp.sum(jnp.exp(total[block] - top), axis=0, keepdims=True)
        return mass

    do_scores(0)
    do_scores(1)
    pass_a(3, 1)
    pass_a(1, 1)
    do_rows(0)
    do_rows(1)
    opposite_landed(FORWARD[:4])
    do_scores(3)
    pass_a(2, 0)
    pass_a(2, 1)
    do_rows(3)
    do_scores(2)
    opposite_landed(FORWARD[4:6])
    do_rows(2)
    do_scores(4)
    top = do_logits(0)
    top = jnp.maximum(top, do_logits(1))
    do_rows(4)
    opposite_landed(FORWARD[6:])
    do_scores(5)
    top = jnp.maximum(top, do_logits(2))
    mass = mass_of((0, 1, 2), top)
    stat_out[0:1, :] = top
    stat_out[1:2, :] = mass
    ex_send(12, stat_out.at[0:8], stat_in.at[0:8], hi_pal)
    do_rows(5)
    last_top = jnp.maximum(do_logits(3), do_logits(4))
    ex_wait(12, stat_in.at[0:8])
    other_top, other_mass = stat_in[0:1, :], stat_in[1:2, :]
    first = y_hi == 0
    top_a, top_b = jnp.where(first, top, other_top), jnp.where(first, other_top, top)
    mass_a, mass_b = jnp.where(first, mass, other_mass), jnp.where(first, other_mass, mass)
    last_top = jnp.maximum(last_top, do_logits(5))
    best = jnp.maximum(jnp.maximum(top_a, top_b), last_top)
    evidence = best + jnp.log(
        mass_a * jnp.exp(top_a - best) + mass_b * jnp.exp(top_b - best) + mass_of((3, 4), best)
    )
    for n in (3, 4, 5):
        block, sums = sums_place(n)
        p = jnp.exp(total[block, sums] - evidence).astype(BF16)
        for t in range(2):
            for k, (g, b, yr) in enumerate(BATCHES[n]):
                o = (t * len(BATCHES[n]) + k) * PIECE
                rows = pl.ds(t * SIDE + b * 32 + yr * PIECE, PIECE)
                post[g, rows, mine] = p[o : o + PIECE, :]
    ex_send(20, post.at[2, :, mine], post.at[2, :, mine], core_pal)
    stat_out[8:16, :] = jnp.broadcast_to(evidence, (8, HALF))
    for n in (1, 2, 0):
        p = jnp.exp(total[n] - evidence).astype(BF16)
        for k, (g, b, yr) in enumerate(BATCHES[n]):
            first_row = pl.multiple_of(y_hi * SIDE + b * 32 + yr * PIECE, PIECE)
            post[g, pl.ds(first_row, PIECE), mine] = p[k * PIECE : (k + 1) * PIECE, :]
        for g in {1: (), 2: (1, 3), 0: (0,)}[n]:
            ex_send(14 + g, post.at[g, keep, mine], post.at[g, keep, mine], hi_pal)
            ex_send(18 + g, post.at[g, keep, mine], post.at[g, keep, mine], core_pal)
    ex_send(13, stat_out.at[8:16], stat_in.at[8:16], core_pal)

    def do_relay(g):
        ex_wait(14 + g, post.at[g, give, mine])
        ex_send(22 + g, post.at[g, give, mine], post.at[g, give, mine], core_pal)

    def do_posterior(g):
        ex_wait(18 + g, post.at[g, keep, theirs])
        ex_wait(22 + g, post.at[g, give, theirs])

    def product(g, j):
        cols = pl.ds(pl.multiple_of(j * TILE, TILE), TILE)
        return jnp.dot(post[g], im[:, cols], preferred_element_type=F32)

    def a_rows(j, t):
        return pl.ds(t * SIDE, 64 if isinstance(j, int) and j % 4 == 3 else SIDE)

    def a_copy(kind, j, t, src, dst, peer):
        rows = a_rows(j, t)
        return remote(
            src.at[j, rows], dst.at[j, rows], a_s.at[kind, j, t], a_r.at[kind, j, t], peer
        )

    def a_landed(kind, j, t, dst):
        landed(dst.at[j, a_rows(j, t)], a_s.at[kind, j, t], a_r.at[kind, j, t])

    def f_copy(g, n):
        return remote(f_out.at[n, g], f_in.at[n, g], f_s.at[n, g], f_r.at[n, g], y_pal)

    def first_product(g, n):
        p = product(g, 3 + 4 * n).reshape(8, 2, PIECE, TILE)
        f_out[n, g] = p[:, 1].reshape(SIDE, TILE).astype(BF16)
        f_copy(g, n).start()
        kept[n, g] = p[:, 0].reshape(SIDE, TILE)

    def first_sum(g, n):
        f_copy(g, n).wait_recv()
        return kept[n, g] + f_in[n, g].astype(F32)

    def put(dst, j, rows):
        for t in range(2):
            dst[j, a_rows(j, t)] = rows[t * 64 : t * 64 + 64, :].astype(BF16)

    def get(src, j):
        return jnp.concatenate([src[j, a_rows(j, t)] for t in range(2)], axis=0).astype(F32)

    ex_wait(20, post.at[2, :, theirs])

    @pl.loop(0, 3)
    def _(k):
        s2[k] = product(2, k).astype(BF16)
        for t in range(2):
            a_copy(0, k, t, s2, r_opp, a_plus[t]).start()
        s2[k + 4] = product(2, k + 4).astype(BF16)
        for t in range(2):
            a_copy(0, k + 4, t, s2, r_opp, a_minus[t]).start()

    for n in range(2):
        first_product(2, n)
    do_relay(1)
    do_relay(3)
    do_posterior(1)
    do_posterior(3)

    @pl.loop(0, 3)
    def _(k):
        s1[k + 4] = product(1, k + 4).astype(BF16)
        for t in range(2):
            a_copy(1, k + 4, t, s1, r_minus, a_plus[t]).start()
        s3[k] = product(3, k).astype(BF16)
        for t in range(2):
            a_copy(2, k, t, s3, r_plus, a_minus[t]).start()

    first_product(1, 1)
    first_product(3, 0)
    first_product(1, 0)
    first_product(3, 1)
    do_relay(0)
    do_posterior(0)
    for n in range(2):
        first_product(0, n)

    @pl.loop(0, 3)
    def _(k):
        p1 = product(1, k)
        for t in range(2):
            a_landed(0, k, t, r_opp)
        s1[k] = (p1 + r_opp[k].astype(F32)).astype(BF16)
        for t in range(2):
            a_copy(1, k, t, s1, r_minus, a_plus[t]).start()
        p3 = product(3, k + 4)
        for t in range(2):
            a_landed(0, k + 4, t, r_opp)
        s3[k + 4] = (p3 + r_opp[k + 4].astype(F32)).astype(BF16)
        for t in range(2):
            a_copy(2, k + 4, t, s3, r_plus, a_minus[t]).start()

    ex_wait(13, stat_in.at[8:16])
    evid[:, mine] = stat_out[8:9, :]
    evid[:, theirs] = stat_in[8:9, :]
    for n in range(NIM // 128):
        evidence_ref[n : n + 1, :] = evid[:, n * 128 : n * 128 + 128]

    def b_copy(kind, j, t, src, dst, peer):
        rows = pl.ds(0, PIECE if j % 4 == 3 else 32)
        return remote(
            src.at[j, t, rows], dst.at[j, t, rows], b_s.at[kind, j, t], b_r.at[kind, j, t], peer
        )

    def b_landed(kind, j, t, dst):
        b_copy(kind, j, t, dst, dst, core_pal).wait_recv()

    def y_copy(j, t):
        return remote(y_out.at[j, t], y_in.at[j, t], yy_s.at[j, t], yy_r.at[j, t], y_pal)

    def first_opposite():
        for n, j in enumerate((3, 7)):
            put(s2, j, first_sum(2, n))
            for t in range(2):
                a_copy(0, j, t, s2, r_opp, (a_plus, a_minus)[n][t]).start()

    def first_free():
        put(s1, 7, first_sum(1, 1))
        for t in range(2):
            a_copy(1, 7, t, s1, r_minus, a_plus[t]).start()
        put(s3, 3, first_sum(3, 0))
        for t in range(2):
            a_copy(2, 3, t, s3, r_plus, a_minus[t]).start()

    def first_bound():
        for t in range(2):
            a_landed(0, 3, t, r_opp)
        put(s1, 3, first_sum(1, 0) + get(r_opp, 3))
        for t in range(2):
            a_copy(1, 3, t, s1, r_minus, a_plus[t]).start()
        for t in range(2):
            a_landed(0, 7, t, r_opp)
        put(s3, 7, first_sum(3, 1) + get(r_opp, 7))
        for t in range(2):
            a_copy(2, 7, t, s3, r_plus, a_minus[t]).start()

    def rows_of(j, t, b):
        n = PIECE if j % 4 == 3 else 32
        return pl.ds(t * SIDE + b * n, n)

    def step_a(k):
        for j, low in ((k, True), (k + 4, False)):
            p = None if k == 3 else product(0, j)
            for t in range(2):
                a_landed(1, j, t, r_minus)
                a_landed(2, j, t, r_plus)
            if k == 3:
                total_j = first_sum(0, j // 4) + get(r_plus, j) + get(r_minus, j)
                for t in range(2):
                    acc[j, a_rows(j, t)] = total_j[t * 64 : t * 64 + 64, :]
            else:
                acc[j] = p + r_plus[j].astype(F32) + r_minus[j].astype(F32)
            n = PIECE if k == 3 else 32
            for t in range(2):
                z2[j, t, 0:n] = acc[j, rows_of(j, t, 2), :].astype(BF16)
                b_copy(0, j, t, z2, zr_opp, b_plus[t] if low else b_minus[t]).start()
                if low:
                    z3[j, t, 0:n] = acc[j, rows_of(j, t, 3), :].astype(BF16)
                    b_copy(2, j, t, z3, zr_plus, b_minus[t]).start()
                else:
                    z1[j, t, 0:n] = acc[j, rows_of(j, t, 1), :].astype(BF16)
                    b_copy(1, j, t, z1, zr_minus, b_plus[t]).start()

    def step_b(k):
        n = PIECE if k == 3 else 32
        for t in range(2):
            b_landed(0, k, t, zr_opp)
            v = acc[k, rows_of(k, t, 1), :] + zr_opp[k, t, 0:n].astype(F32)
            z1[k, t, 0:n] = v.astype(BF16)
            b_copy(1, k, t, z1, zr_minus, b_plus[t]).start()
            j = k + 4
            b_landed(0, j, t, zr_opp)
            v = acc[j, rows_of(j, t, 3), :] + zr_opp[j, t, 0:n].astype(F32)
            z3[j, t, 0:n] = v.astype(BF16)
            b_copy(2, j, t, z3, zr_plus, b_minus[t]).start()

    def step_c(k):
        n = PIECE if k == 3 else 32
        for j in (k, k + 4):
            cols = pl.ds(j * TILE, TILE)
            for t in range(2):
                b_landed(1, j, t, zr_minus)
                b_landed(2, j, t, zr_plus)
                v = acc[j, rows_of(j, t, 0), :] + zr_plus[j, t, 0:n].astype(F32)
                v = v + zr_minus[j, t, 0:n].astype(F32)
                out_ref[t * PIECE : (t + 1) * PIECE, cols] = v[:PIECE, :]
                if k < 3:
                    y_out[j, t] = v[PIECE:, :].astype(BF16)
                    y_copy(j, t).start()

    def step_d(k):
        for j in (k, k + 4):
            cols = pl.ds(j * TILE, TILE)
            for t in range(2):
                y_copy(j, t).wait_recv()
                rows = slice(t * PIECE, (t + 1) * PIECE)
                out_ref[rows, cols] = out_ref[rows, cols] + y_in[j, t].astype(F32)

    first_opposite()
    step_a(0)
    first_free()
    step_a(1)
    step_b(0)
    first_bound()
    step_a(2)
    step_b(1)
    step_a(3)
    step_b(2)
    step_c(0)
    step_b(3)
    step_c(1)
    step_c(2)
    step_c(3)
    for k in range(3):
        step_d(k)

    for c in ag_sends:
        c.wait_send()
    for c in ex_sends:
        c.wait_send()

    for j in range(NT):
        for t in range(2):
            a_copy(0, j, t, s2, r_opp, core_pal).wait_send()
            a_copy(1, j, t, s1, r_minus, core_pal).wait_send()
            a_copy(2, j, t, s3, r_plus, core_pal).wait_send()
            b_copy(0, j, t, z2, zr_opp, core_pal).wait_send()
            b_copy(1, j, t, z1, zr_minus, core_pal).wait_send()
            b_copy(2, j, t, z3, zr_plus, core_pal).wait_send()
            if j % 4 < 3:
                y_copy(j, t).wait_send()
    for n in range(2):
        for g in range(4):
            f_copy(g, n).wait_send()


def shards(
    images, references, shell_of_pixel, noise_power, ref_class, ref_orient, class_logw, orient_logw
):
    vmem = pl.BlockSpec(memory_space=pltpu.VMEM)
    hbm = pl.BlockSpec(memory_space=pl.ANY)
    smem = pl.BlockSpec(memory_space=pltpu.SMEM)
    dma = pltpu.SemaphoreType.DMA
    accumulators, evidence = pl.pallas_call(
        kernel,
        out_shape=(
            jax.ShapeDtypeStruct((ROWS, PIX), F32),
            jax.ShapeDtypeStruct((NIM // 128, 128), F32),
        ),
        in_specs=[hbm, hbm, vmem, vmem, vmem, vmem, vmem, smem],
        out_specs=(vmem, vmem),
        scratch_shapes=[
            pltpu.VMEM((NIM, PIX), BF16),
            pltpu.VMEM((NIM, PIX), BF16),
            pltpu.VMEM((4, GROUP, PIX), BF16),
            pltpu.VMEM((4, GROUP, NIM), F32),
            pltpu.VMEM((4, GROUP, HALF), F32),
            pltpu.VMEM((5, SIDE, HALF), F32),
            pltpu.VMEM((5, SIDE, HALF), F32),
            pltpu.VMEM((5, SIDE, HALF), F32),
            pltpu.VMEM((1, PIX), F32),
            pltpu.VMEM((128, 128), F32),
            pltpu.VMEM((2, 128, 128), F32),
            pltpu.VMEM((2, 5 * SIDE, 1), F32),
            pltpu.VMEM((1, NIM), F32),
            pltpu.VMEM((16, HALF), F32),
            pltpu.VMEM((16, HALF), F32),
            pltpu.VMEM((4, GROUP, NIM), BF16),
            pltpu.VMEM((NT, GROUP, TILE), BF16),
            pltpu.VMEM((NT, GROUP, TILE), BF16),
            pltpu.VMEM((NT, GROUP, TILE), BF16),
            pltpu.VMEM((NT, GROUP, TILE), BF16),
            pltpu.VMEM((NT, GROUP, TILE), BF16),
            pltpu.VMEM((NT, GROUP, TILE), BF16),
            pltpu.VMEM((NT, GROUP, TILE), F32),
            pltpu.VMEM((NT, 2, 32, TILE), BF16),
            pltpu.VMEM((NT, 2, 32, TILE), BF16),
            pltpu.VMEM((NT, 2, 32, TILE), BF16),
            pltpu.VMEM((NT, 2, 32, TILE), BF16),
            pltpu.VMEM((NT, 2, 32, TILE), BF16),
            pltpu.VMEM((NT, 2, 32, TILE), BF16),
            pltpu.VMEM((NT, 2, PIECE, TILE), BF16),
            pltpu.VMEM((NT, 2, PIECE, TILE), BF16),
            pltpu.VMEM((2, 4, SIDE, TILE), F32),
            pltpu.VMEM((2, 4, SIDE, TILE), BF16),
            pltpu.VMEM((2, 4, SIDE, TILE), BF16),
            dma((5,)),
            dma((84,)),
            dma((84,)),
            dma((26,)),
            dma((26,)),
            dma((3, NT, 2)),
            dma((3, NT, 2)),
            dma((3, NT, 2)),
            dma((3, NT, 2)),
            dma((NT, 2)),
            dma((NT, 2)),
            dma((2, 4)),
            dma((2, 4)),
        ],
        compiler_params=pltpu.CompilerParams(
            collective_id=0, has_side_effects=True, vmem_limit_bytes=67043328
        ),
    )(
        images,
        references,
        shell_of_pixel.reshape(1, PIX),
        noise_power.reshape(1, 64),
        ref_class.reshape(NREF // 128, 128),
        ref_orient.reshape(NREF // 128, 128),
        orient_logw.reshape(1, NORIENT),
        class_logw,
    )
    return accumulators, evidence.reshape(NIM)


def solution(mesh):
    placed = (P("img", "shell"), P("img", "shell"), P("shell"), P(), P(), P(), P(), P())
    return jax.shard_map(
        shards, mesh=mesh, in_specs=placed, out_specs=(P("img", "shell"), P("img")), check_vma=False
    )
```

```python
import jax
import jax.numpy as jnp
from jax import lax
from jax.experimental import pallas as pl
from jax.experimental.pallas import tpu as pltpu
from jax.sharding import PartitionSpec as P

INVERSE_HEAT = 0.5
MESH = pl.DeviceIdType.MESH
F32 = jnp.float32
BF16 = jnp.bfloat16

NZ, NY, NX = 4, 2, 4
ROWS = 32
PIECE = 16
PIX = 4096
NIM = 768
HALF = NIM // 2
GROUP = 256
SIDE = GROUP // 2
NREF = 1024
TILE = 512
NT = PIX // TILE
PH = PIX // 2
NORIENT = 6144

FORWARD = [(0, 0), (0, 1), (3, 0), (1, 0), (3, 1), (1, 1), (2, 0), (2, 1)]
BATCHES = [
    [(0, b, yr) for b, yr in FORWARD],
    [(g, b, yr) for g in (1, 3) for b, yr in FORWARD[:4]],
    [(g, b, yr) for g in (1, 3) for b, yr in FORWARD[4:6]],
    [(g, b, yr) for g in (1, 3) for b, yr in FORWARD[6:]],
    [(2, b, yr) for b, yr in FORWARD[:4]],
    [(2, b, yr) for b, yr in FORWARD[4:6]],
    [(2, b, yr) for b, yr in FORWARD[6:]],
]
SHARED = 4
SCORE_ROW = [0, 256, 512, 640, 768, 896, 960]
SUM_ROW = [0, 128, 256, 320, 384, 512, 576]


def kernel(
    images_hbm,
    references_hbm,
    shell_ref,
    noise_ref,
    class_id_ref,
    orient_id_ref,
    orient_ref,
    class_ref,
    out_ref,
    evidence_ref,
    im,
    wim,
    refs,
    score,
    core_in,
    row_out,
    row_in,
    total,
    weight,
    square,
    columns,
    prior,
    evid,
    stat_out,
    stat_in,
    post,
    s1,
    s2,
    s3,
    r_opp,
    r_plus,
    r_minus,
    acc,
    z1,
    z2,
    z3,
    zr_opp,
    zr_plus,
    zr_minus,
    y_out,
    y_in,
    kept,
    f_out,
    f_in,
    load_sem,
    ag_s,
    ag_r,
    ex_s,
    ex_r,
    a_s,
    a_r,
    b_s,
    b_r,
    yy_s,
    yy_r,
    f_s,
    f_r,
):
    s = lax.axis_index("shell")
    i = lax.axis_index("img")
    core = lax.rem(s, 2)
    y_hi = s // 2
    z = i // (NY * NX)
    y = lax.rem(i // NX, NY)
    x = lax.rem(i, NX)

    def at(zz, yv, xx):
        return (zz * NY + yv) * NX + xx

    x_plus = (s, at(z, y, lax.rem(x + 1, NX)))
    x_minus = (s, at(z, y, lax.rem(x + NX - 1, NX)))
    z_plus = (s, at(lax.rem(z + 1, NZ), y, x))
    z_minus = (s, at(lax.rem(z + NZ - 1, NZ), y, x))
    y_pal = (s, at(z, 1 - y, x))
    core_pal = (y_hi * 2 + 1 - core, i)
    hi_pal = ((1 - y_hi) * 2 + core, i)
    a_plus, a_minus = (x_plus, z_plus), (x_minus, z_minus)
    b_plus, b_minus = (z_plus, x_plus), (z_minus, x_minus)

    def remote(src, dst, send_sem, recv_sem, peer):
        return pltpu.make_async_remote_copy(
            src_ref=src,
            dst_ref=dst,
            send_sem=send_sem,
            recv_sem=recv_sem,
            device_id=peer,
            device_id_type=MESH,
        )

    def landed(dst, send_sem, recv_sem):
        remote(dst, dst, send_sem, recv_sem, core_pal).wait_recv()

    own = []
    for t in range(2):
        c = pltpu.make_async_copy(
            references_hbm.at[pl.ds(t * PIECE, PIECE), :],
            refs.at[0, pl.ds(t * SIDE, PIECE), :],
            load_sem.at[t],
        )
        c.start()
        own.append(c)
    image_loads = []
    for n in range(3):
        c = pltpu.make_async_copy(
            images_hbm.at[pl.ds(n * 256, 256), :], im.at[pl.ds(n * 256, 256), :], load_sem.at[2 + n]
        )
        c.start()
        image_loads.append(c)

    barrier = pltpu.get_barrier_semaphore()
    for peer in (x_plus, x_minus, z_plus, z_minus, y_pal, core_pal, hi_pal):
        pl.semaphore_signal(barrier, inc=1, device_id=peer, device_id_type=MESH)
    pl.semaphore_wait(barrier, 7)

    index = {}
    ag_sends = []

    def slot(name):
        if name not in index:
            index[name] = len(index)
        return index[name]

    def piece(t, a, b, yr, part=None):
        rows = pl.ds(t * SIDE + b * 32 + yr * PIECE, PIECE)
        if part is None:
            return refs.at[a, rows, :]
        return refs.at[a, rows, pl.ds(part * PH, PH)]

    def ag_send(name, src, dst, peer):
        n = slot(name)
        c = remote(src, dst, ag_s.at[n], ag_r.at[n], peer)
        c.start()
        ag_sends.append(c)

    def ag_wait(name, dst):
        n = slot(name)
        landed(dst, ag_s.at[n], ag_r.at[n])

    def send_b(t, yr):
        ag_send(("b+", t, yr), piece(t, 0, 0, yr), piece(t, 0, 3, yr), b_plus[t])
        ag_send(("b-", t, yr), piece(t, 0, 0, yr), piece(t, 0, 1, yr), b_minus[t])

    def send_a(t, b, yr):
        ag_send(("a+", t, b, yr), piece(t, 0, b, yr), piece(t, 3, b, yr), a_plus[t])
        ag_send(("a-", t, b, yr), piece(t, 0, b, yr), piece(t, 1, b, yr), a_minus[t])

    def log_prior():
        square[...] = jnp.zeros((128, 128), F32)
        for n, ids in enumerate((class_id_ref, orient_id_ref)):
            square[0:8, :] = ids[...].astype(F32)
            columns[n] = square[...].T

        def place(row, a, b, yr, kind):
            za = lax.rem(z + jnp.where(kind == 0, b, a), NZ)
            xa = lax.rem(x + jnp.where(kind == 0, a, b), NX)
            ya = y if yr == 0 else 1 - y
            first = at(za, ya, xa) * ROWS + kind * PIECE
            rows = pl.ds(pl.multiple_of(lax.rem(first, 128), PIECE), PIECE)
            pick = lax.broadcasted_iota(jnp.int32, (PIECE, 128), 1) == first // 128
            for n in range(2):
                found = jnp.sum(jnp.where(pick, columns[n, rows, :], 0.0), axis=1, keepdims=True)
                prior[n, pl.ds(row, PIECE), :] = found

        for n, batch in enumerate(BATCHES):
            for k, (g, b, yr) in enumerate(batch):
                if n < SHARED:
                    place(SUM_ROW[n] + k * PIECE, g, b, yr, y_hi)
                else:
                    for t in range(2):
                        place(SUM_ROW[n] + (t * len(batch) + k) * PIECE, g, b, yr, t)

        @pl.loop(0, 5)
        def _(block):
            rows = pl.ds(pl.multiple_of(block * SIDE, SIDE), SIDE)
            kind = prior[0, rows, :]
            orient = jnp.broadcast_to(prior[1, rows, :], (SIDE, 128)).astype(jnp.int32)

            def add(n, sums):
                cols = pl.ds(pl.multiple_of(n * 128, 128), 128)
                ids = lax.broadcasted_iota(jnp.int32, (SIDE, 128), 1) + n * 128
                logw = jnp.broadcast_to(orient_ref[:, cols], (SIDE, 128))
                return sums + jnp.where(orient == ids, logw, 0.0)

            sums = lax.fori_loop(0, NORIENT // 128, add, jnp.zeros((SIDE, 128), F32))
            found = jnp.zeros((SIDE, 1), F32)
            for n in range(4):
                found = found + jnp.where(kind == float(n), class_ref[n], 0.0)
            prior[0, rows, :] = found + jnp.sum(sums, axis=1, keepdims=True)

    for t in range(2):
        own[t].wait()
    for t in range(2):
        ag_send(("y", t), piece(t, 0, 0, 0), piece(t, 0, 0, 1), y_pal)
    for t in range(2):
        send_b(t, 0)
    for t in range(2):
        send_a(t, 0, 0)

    noise_row = 1.0 / noise_ref[...]
    r64 = lax.broadcasted_iota(jnp.int32, (64, 64), 0)
    c64 = lax.broadcasted_iota(jnp.int32, (64, 64), 1)
    noise_col = jnp.sum(
        jnp.where(r64 == c64, jnp.broadcast_to(noise_row, (64, 64)), 0.0), axis=1, keepdims=True
    )

    @pl.loop(0, PIX // 512)
    def _(n):
        cols = pl.ds(pl.multiple_of(n * 512, 512), 512)
        shell = jnp.broadcast_to(shell_ref[:, cols], (64, 512))
        hit = shell == lax.broadcasted_iota(jnp.int32, (64, 512), 0)
        weight[:, cols] = jnp.sum(
            jnp.where(hit, jnp.broadcast_to(noise_col, (64, 512)), 0.0), axis=0, keepdims=True
        )

    for t in range(2):
        ag_wait(("y", t), piece(t, 0, 0, 1))
        send_b(t, 1)
    for t in range(2):
        send_a(t, 0, 1)

    for n in range(3):
        image_loads[n].wait()

        @pl.loop(0, PIX // 256)
        def _(k):
            cols = pl.ds(pl.multiple_of(k * 256, 256), 256)
            rows = pl.ds(n * 256, 256)
            wim[cols, rows] = (im[rows, cols].astype(F32) * weight[:, cols]).astype(BF16).T

    def pass_b(yr):
        for t in range(2):
            ag_wait(("b+", t, yr), piece(t, 0, 3, yr))
            ag_send(("bf+", t, yr), piece(t, 0, 3, yr, 0), piece(t, 0, 2, yr, 0), b_plus[t])
            ag_wait(("b-", t, yr), piece(t, 0, 1, yr))
            ag_send(("bf-", t, yr), piece(t, 0, 1, yr, 1), piece(t, 0, 2, yr, 1), b_minus[t])
        for t in range(2):
            send_a(t, 3, yr)
            send_a(t, 1, yr)

    def pass_a(b, yr):
        for t in range(2):
            ag_wait(("a+", t, b, yr), piece(t, 3, b, yr))
            ag_send(("af+", t, b, yr), piece(t, 3, b, yr, 0), piece(t, 2, b, yr, 0), a_plus[t])
            ag_wait(("a-", t, b, yr), piece(t, 1, b, yr))
            ag_send(("af-", t, b, yr), piece(t, 1, b, yr, 1), piece(t, 2, b, yr, 1), a_minus[t])

    def opposite_landed(pieces):
        for b, yr in pieces:
            for t in range(2):
                ag_wait(("af+", t, b, yr), piece(t, 2, b, yr, 0))
                ag_wait(("af-", t, b, yr), piece(t, 2, b, yr, 1))

    pass_b(0)
    log_prior()
    pass_a(0, 0)
    pass_a(0, 1)
    pass_b(1)
    pass_a(3, 0)
    pass_a(1, 0)
    for yr in range(2):
        for t in range(2):
            ag_wait(("bf+", t, yr), piece(t, 0, 2, yr, 0))
            ag_wait(("bf-", t, yr), piece(t, 0, 2, yr, 1))
            send_a(t, 2, yr)

    mine = pl.ds(pl.multiple_of(core * HALF, 128), HALF)
    theirs = pl.ds(pl.multiple_of((1 - core) * HALF, 128), HALF)
    keep = pl.ds(pl.multiple_of(y_hi * SIDE, SIDE), SIDE)
    give = pl.ds(pl.multiple_of((1 - y_hi) * SIDE, SIDE), SIDE)
    ex_sends = []

    def ex_send(n, src, dst, peer):
        c = remote(src, dst, ex_s.at[n], ex_r.at[n], peer)
        c.start()
        ex_sends.append(c)

    def ex_wait(n, dst):
        landed(dst, ex_s.at[n], ex_r.at[n])

    def size(n):
        return 2 * PIECE * len(BATCHES[n])

    def score_rows(n):
        return pl.ds(SCORE_ROW[n], size(n))

    def sum_rows(n):
        return pl.ds(SUM_ROW[n], size(n) // 2 if n < SHARED else size(n))

    def kind_rows(n, kind):
        return pl.ds(pl.multiple_of(SCORE_ROW[n] + kind * (size(n) // 2), 16), size(n) // 2)

    def do_scores(n):
        batch = BATCHES[n]
        n_rows = size(n)
        rows = score_rows(n)

        def of(cols):
            return jnp.concatenate(
                [
                    refs[g, t * SIDE + b * 32 + yr * PIECE : t * SIDE + b * 32 + (yr + 1) * PIECE, cols]
                    for t in range(2)
                    for g, b, yr in batch
                ],
                axis=0,
            )

        def add(k, sums, chunks):
            for u in range(chunks):
                cols = pl.ds(pl.multiple_of((k * chunks + u) * 128, 128), 128)
                part = of(cols).astype(F32)
                sums = sums + part * part * weight[:, cols]
            return sums

        zero = jnp.zeros((n_rows, 128), F32)
        if n_rows > 128:
            sums = lax.fori_loop(0, PIX // 512, lambda k, v: add(k, v, 4), zero)
        else:
            sums = add(0, zero, PIX // 256) + add(1, zero, PIX // 256)
        norm = 0.5 * jnp.sum(sums, axis=1, keepdims=True)
        part = jnp.dot(of(slice(None)), wim[...], preferred_element_type=F32)
        score[rows, :] = part - norm
        ex_send(n, score.at[rows, theirs], core_in.at[rows], core_pal)

    def do_rows(n):
        rows, sums = score_rows(n), sum_rows(n)
        ex_wait(n, core_in.at[rows])
        if n < SHARED:
            away, home = kind_rows(n, 1 - y_hi), kind_rows(n, y_hi)
            row_out[sums] = score[away, mine] + core_in[away, :]
            ex_send(7 + n, row_out.at[sums], row_in.at[sums], hi_pal)
            total[sums] = score[home, mine] + core_in[home, :]
        else:
            row_out[sums] = score[rows, mine] + core_in[rows, :]
            ex_send(7 + n, row_out.at[sums], row_in.at[sums], hi_pal)

    def do_logits(n):
        sums = sum_rows(n)
        ex_wait(7 + n, row_in.at[sums])
        near = total if n < SHARED else row_out
        logits = INVERSE_HEAT * (near[sums] + row_in[sums]) + prior[0, sums, :]
        total[sums] = logits
        return jnp.max(logits, axis=0, keepdims=True)

    def mass_of(rows, top):
        return jnp.sum(jnp.exp(total[rows] - top), axis=0, keepdims=True)

    shared_rows = pl.ds(0, 3 * SIDE)
    do_scores(0)
    do_scores(1)
    do_rows(0)
    do_rows(1)
    pass_a(3, 1)
    pass_a(1, 1)
    do_scores(2)
    opposite_landed(FORWARD[:4])
    do_scores(4)
    do_rows(2)
    do_rows(4)
    pass_a(2, 0)
    pass_a(2, 1)
    do_scores(3)
    opposite_landed(FORWARD[4:6])
    do_rows(3)
    do_scores(5)
    top = jnp.maximum(do_logits(0), do_logits(1))
    opposite_landed(FORWARD[6:])
    do_rows(5)
    do_scores(6)
    top = jnp.maximum(top, do_logits(2))
    top = jnp.maximum(top, do_logits(3))
    mass = mass_of(shared_rows, top)
    stat_out[0:1, :] = top
    stat_out[1:2, :] = mass
    ex_send(14, stat_out.at[0:8], stat_in.at[0:8], hi_pal)
    do_rows(6)
    last_top = jnp.maximum(do_logits(4), do_logits(5))
    ex_wait(14, stat_in.at[0:8])
    other_top, other_mass = stat_in[0:1, :], stat_in[1:2, :]
    first = y_hi == 0
    top_a, top_b = jnp.where(first, top, other_top), jnp.where(first, other_top, top)
    mass_a, mass_b = jnp.where(first, mass, other_mass), jnp.where(first, other_mass, mass)
    last_top = jnp.maximum(last_top, do_logits(6))
    best = jnp.maximum(jnp.maximum(top_a, top_b), last_top)
    evidence = best + jnp.log(
        mass_a * jnp.exp(top_a - best) + mass_b * jnp.exp(top_b - best) + mass_of(pl.ds(3 * SIDE, 2 * SIDE), best)
    )
    for n in range(SHARED, len(BATCHES)):
        p = jnp.exp(total[sum_rows(n)] - evidence).astype(BF16)
        for t in range(2):
            for k, (g, b, yr) in enumerate(BATCHES[n]):
                o = (t * len(BATCHES[n]) + k) * PIECE
                rows = pl.ds(t * SIDE + b * 32 + yr * PIECE, PIECE)
                post[g, rows, mine] = p[o : o + PIECE, :]
    ex_send(22, post.at[2, :, mine], post.at[2, :, mine], core_pal)
    stat_out[8:16, :] = jnp.broadcast_to(evidence, (8, HALF))
    for n in (1, 2, 3, 0):
        p = jnp.exp(total[sum_rows(n)] - evidence).astype(BF16)
        for k, (g, b, yr) in enumerate(BATCHES[n]):
            first_row = pl.multiple_of(y_hi * SIDE + b * 32 + yr * PIECE, PIECE)
            post[g, pl.ds(first_row, PIECE), mine] = p[k * PIECE : (k + 1) * PIECE, :]
        for g in {3: (1, 3), 0: (0,)}.get(n, ()):
            ex_send(16 + g, post.at[g, keep, mine], post.at[g, keep, mine], hi_pal)
            ex_send(20 + g, post.at[g, keep, mine], post.at[g, keep, mine], core_pal)
    ex_send(15, stat_out.at[8:16], stat_in.at[8:16], core_pal)

    def do_relay(g):
        ex_wait(16 + g, post.at[g, give, mine])
        ex_send(24 + g, post.at[g, give, mine], post.at[g, give, mine], core_pal)

    def do_posterior(g):
        ex_wait(20 + g, post.at[g, keep, theirs])
        ex_wait(24 + g, post.at[g, give, theirs])

    def product(g, j):
        cols = pl.ds(pl.multiple_of(j * TILE, TILE), TILE)
        return jnp.dot(post[g], im[:, cols], preferred_element_type=F32)

    def a_rows(j, t):
        return pl.ds(t * SIDE, 64 if isinstance(j, int) and j % 4 == 3 else SIDE)

    def a_copy(kind, j, t, src, dst, peer):
        rows = a_rows(j, t)
        return remote(
            src.at[j, rows], dst.at[j, rows], a_s.at[kind, j, t], a_r.at[kind, j, t], peer
        )

    def a_landed(kind, j, t, dst):
        landed(dst.at[j, a_rows(j, t)], a_s.at[kind, j, t], a_r.at[kind, j, t])

    def f_copy(g, n):
        return remote(f_out.at[n, g], f_in.at[n, g], f_s.at[n, g], f_r.at[n, g], y_pal)

    def first_product(g, n):
        p = product(g, 3 + 4 * n).reshape(8, 2, PIECE, TILE)
        f_out[n, g] = p[:, 1].reshape(SIDE, TILE).astype(BF16)
        f_copy(g, n).start()
        kept[n, g] = p[:, 0].reshape(SIDE, TILE)

    def first_sum(g, n):
        f_copy(g, n).wait_recv()
        return kept[n, g] + f_in[n, g].astype(F32)

    def put(dst, j, rows):
        for t in range(2):
            dst[j, a_rows(j, t)] = rows[t * 64 : t * 64 + 64, :].astype(BF16)

    def get(src, j):
        return jnp.concatenate([src[j, a_rows(j, t)] for t in range(2)], axis=0).astype(F32)

    ex_wait(22, post.at[2, :, theirs])

    @pl.loop(0, 3)
    def _(k):
        s2[k] = product(2, k).astype(BF16)
        for t in range(2):
            a_copy(0, k, t, s2, r_opp, a_plus[t]).start()
        s2[k + 4] = product(2, k + 4).astype(BF16)
        for t in range(2):
            a_copy(0, k + 4, t, s2, r_opp, a_minus[t]).start()

    for n in range(2):
        first_product(2, n)
    def free(k):
        s1[k + 4] = product(1, k + 4).astype(BF16)
        for t in range(2):
            a_copy(1, k + 4, t, s1, r_minus, a_plus[t]).start()
        s3[k] = product(3, k).astype(BF16)
        for t in range(2):
            a_copy(2, k, t, s3, r_plus, a_minus[t]).start()

    def bound(k):
        p1 = product(1, k)
        for t in range(2):
            a_landed(0, k, t, r_opp)
        s1[k] = (p1 + r_opp[k].astype(F32)).astype(BF16)
        for t in range(2):
            a_copy(1, k, t, s1, r_minus, a_plus[t]).start()
        p3 = product(3, k + 4)
        for t in range(2):
            a_landed(0, k + 4, t, r_opp)
        s3[k + 4] = (p3 + r_opp[k + 4].astype(F32)).astype(BF16)
        for t in range(2):
            a_copy(2, k + 4, t, s3, r_plus, a_minus[t]).start()

    do_relay(1)
    do_relay(3)
    do_posterior(1)
    do_posterior(3)
    first_product(1, 1)
    first_product(3, 0)
    first_product(1, 0)
    first_product(3, 1)
    free(0)

    @pl.loop(0, 2)
    def _(k):
        bound(k)

    do_relay(0)
    do_posterior(0)
    for n in range(2):
        first_product(0, n)

    ex_wait(15, stat_in.at[8:16])
    evid[:, mine] = stat_out[8:9, :]
    evid[:, theirs] = stat_in[8:9, :]
    for n in range(NIM // 128):
        evidence_ref[n : n + 1, :] = evid[:, n * 128 : n * 128 + 128]

    def b_copy(kind, j, t, src, dst, peer):
        rows = pl.ds(0, PIECE if j % 4 == 3 else 32)
        return remote(
            src.at[j, t, rows], dst.at[j, t, rows], b_s.at[kind, j, t], b_r.at[kind, j, t], peer
        )

    def b_landed(kind, j, t, dst):
        b_copy(kind, j, t, dst, dst, core_pal).wait_recv()

    def y_copy(j, t):
        return remote(y_out.at[j, t], y_in.at[j, t], yy_s.at[j, t], yy_r.at[j, t], y_pal)

    def first_opposite():
        for n, j in enumerate((3, 7)):
            put(s2, j, first_sum(2, n))
            for t in range(2):
                a_copy(0, j, t, s2, r_opp, (a_plus, a_minus)[n][t]).start()

    def first_free():
        put(s1, 7, first_sum(1, 1))
        for t in range(2):
            a_copy(1, 7, t, s1, r_minus, a_plus[t]).start()
        put(s3, 3, first_sum(3, 0))
        for t in range(2):
            a_copy(2, 3, t, s3, r_plus, a_minus[t]).start()

    def first_bound():
        for t in range(2):
            a_landed(0, 3, t, r_opp)
        put(s1, 3, first_sum(1, 0) + get(r_opp, 3))
        for t in range(2):
            a_copy(1, 3, t, s1, r_minus, a_plus[t]).start()
        for t in range(2):
            a_landed(0, 7, t, r_opp)
        put(s3, 7, first_sum(3, 1) + get(r_opp, 7))
        for t in range(2):
            a_copy(2, 7, t, s3, r_plus, a_minus[t]).start()

    def rows_of(j, t, b):
        n = PIECE if j % 4 == 3 else 32
        return pl.ds(t * SIDE + b * n, n)

    def step_a(k):
        for j, low in ((k, True), (k + 4, False)):
            p = None if k == 3 else product(0, j)
            for t in range(2):
                a_landed(1, j, t, r_minus)
                a_landed(2, j, t, r_plus)
            if k == 3:
                total_j = first_sum(0, j // 4) + get(r_plus, j) + get(r_minus, j)
                for t in range(2):
                    acc[j, a_rows(j, t)] = total_j[t * 64 : t * 64 + 64, :]
            else:
                acc[j] = p + r_plus[j].astype(F32) + r_minus[j].astype(F32)
            n = PIECE if k == 3 else 32
            for t in range(2):
                z2[j, t, 0:n] = acc[j, rows_of(j, t, 2), :].astype(BF16)
                b_copy(0, j, t, z2, zr_opp, b_plus[t] if low else b_minus[t]).start()
                if low:
                    z3[j, t, 0:n] = acc[j, rows_of(j, t, 3), :].astype(BF16)
                    b_copy(2, j, t, z3, zr_plus, b_minus[t]).start()
                else:
                    z1[j, t, 0:n] = acc[j, rows_of(j, t, 1), :].astype(BF16)
                    b_copy(1, j, t, z1, zr_minus, b_plus[t]).start()

    def step_b(k):
        n = PIECE if k == 3 else 32
        for t in range(2):
            b_landed(0, k, t, zr_opp)
            v = acc[k, rows_of(k, t, 1), :] + zr_opp[k, t, 0:n].astype(F32)
            z1[k, t, 0:n] = v.astype(BF16)
            b_copy(1, k, t, z1, zr_minus, b_plus[t]).start()
            j = k + 4
            b_landed(0, j, t, zr_opp)
            v = acc[j, rows_of(j, t, 3), :] + zr_opp[j, t, 0:n].astype(F32)
            z3[j, t, 0:n] = v.astype(BF16)
            b_copy(2, j, t, z3, zr_plus, b_minus[t]).start()

    def step_c(k):
        n = PIECE if k == 3 else 32
        for j in (k, k + 4):
            cols = pl.ds(j * TILE, TILE)
            for t in range(2):
                b_landed(1, j, t, zr_minus)
                b_landed(2, j, t, zr_plus)
                v = acc[j, rows_of(j, t, 0), :] + zr_plus[j, t, 0:n].astype(F32)
                v = v + zr_minus[j, t, 0:n].astype(F32)
                out_ref[t * PIECE : (t + 1) * PIECE, cols] = v[:PIECE, :]
                if k < 3:
                    y_out[j, t] = v[PIECE:, :].astype(BF16)
                    y_copy(j, t).start()

    def step_d(k):
        for j in (k, k + 4):
            cols = pl.ds(j * TILE, TILE)
            for t in range(2):
                y_copy(j, t).wait_recv()
                rows = slice(t * PIECE, (t + 1) * PIECE)
                out_ref[rows, cols] = out_ref[rows, cols] + y_in[j, t].astype(F32)

    step_a(0)
    first_opposite()

    @pl.loop(1, 3)
    def _(k):
        free(k)

    bound(2)
    first_free()
    step_a(1)
    step_b(0)
    step_a(2)
    first_bound()
    step_c(0)
    step_b(1)
    step_b(2)
    step_a(3)
    step_c(1)
    step_c(2)
    step_b(3)
    step_d(0)
    step_d(1)
    step_c(3)
    step_d(2)

    for c in ag_sends:
        c.wait_send()
    for c in ex_sends:
        c.wait_send()

    for j in range(NT):
        for t in range(2):
            a_copy(0, j, t, s2, r_opp, core_pal).wait_send()
            a_copy(1, j, t, s1, r_minus, core_pal).wait_send()
            a_copy(2, j, t, s3, r_plus, core_pal).wait_send()
            b_copy(0, j, t, z2, zr_opp, core_pal).wait_send()
            b_copy(1, j, t, z1, zr_minus, core_pal).wait_send()
            b_copy(2, j, t, z3, zr_plus, core_pal).wait_send()
            if j % 4 < 3:
                y_copy(j, t).wait_send()
    for n in range(2):
        for g in range(4):
            f_copy(g, n).wait_send()


def hand_over(sums_hbm, evidence_hbm, sums_out, evidence_out, sums, evidence, sems):
    sources, held = (sums_hbm, evidence_hbm), (sums, evidence)
    for n, out in enumerate((sums_out, evidence_out)):
        pltpu.make_async_copy(sources[n], held[n], sems.at[0, n]).start()
    for n, out in enumerate((sums_out, evidence_out)):
        pltpu.make_async_copy(sources[n], held[n], sems.at[0, n]).wait()
        pltpu.make_async_copy(held[n], out, sems.at[1, n]).start()
    for n, out in enumerate((sums_out, evidence_out)):
        pltpu.make_async_copy(held[n], out, sems.at[1, n]).wait()


def shards(
    images, references, shell_of_pixel, noise_power, ref_class, ref_orient, class_logw, orient_logw
):
    vmem = pl.BlockSpec(memory_space=pltpu.VMEM)
    hbm = pl.BlockSpec(memory_space=pl.ANY)
    smem = pl.BlockSpec(memory_space=pltpu.SMEM)
    dma = pltpu.SemaphoreType.DMA
    accumulators, evidence = pl.pallas_call(
        kernel,
        out_shape=(
            jax.ShapeDtypeStruct((ROWS, PIX), F32),
            jax.ShapeDtypeStruct((NIM // 128, 128), F32),
        ),
        in_specs=[hbm, hbm, vmem, vmem, vmem, vmem, vmem, smem],
        out_specs=(vmem, vmem),
        scratch_shapes=[
            pltpu.VMEM((NIM, PIX), BF16),
            pltpu.VMEM((PIX, NIM), BF16),
            pltpu.VMEM((4, GROUP, PIX), BF16),
            pltpu.VMEM((NREF, NIM), F32),
            pltpu.VMEM((NREF, HALF), F32),
            pltpu.VMEM((5 * SIDE, HALF), F32),
            pltpu.VMEM((5 * SIDE, HALF), F32),
            pltpu.VMEM((5 * SIDE, HALF), F32),
            pltpu.VMEM((1, PIX), F32),
            pltpu.VMEM((128, 128), F32),
            pltpu.VMEM((2, 128, 128), F32),
            pltpu.VMEM((2, 5 * SIDE, 1), F32),
            pltpu.VMEM((1, NIM), F32),
            pltpu.VMEM((16, HALF), F32),
            pltpu.VMEM((16, HALF), F32),
            pltpu.VMEM((4, GROUP, NIM), BF16),
            pltpu.VMEM((NT, GROUP, TILE), BF16),
            pltpu.VMEM((NT, GROUP, TILE), BF16),
            pltpu.VMEM((NT, GROUP, TILE), BF16),
            pltpu.VMEM((NT, GROUP, TILE), BF16),
            pltpu.VMEM((NT, GROUP, TILE), BF16),
            pltpu.VMEM((NT, GROUP, TILE), BF16),
            pltpu.VMEM((NT, GROUP, TILE), F32),
            pltpu.VMEM((NT, 2, 32, TILE), BF16),
            pltpu.VMEM((NT, 2, 32, TILE), BF16),
            pltpu.VMEM((NT, 2, 32, TILE), BF16),
            pltpu.VMEM((NT, 2, 32, TILE), BF16),
            pltpu.VMEM((NT, 2, 32, TILE), BF16),
            pltpu.VMEM((NT, 2, 32, TILE), BF16),
            pltpu.VMEM((NT, 2, PIECE, TILE), BF16),
            pltpu.VMEM((NT, 2, PIECE, TILE), BF16),
            pltpu.VMEM((2, 4, SIDE, TILE), F32),
            pltpu.VMEM((2, 4, SIDE, TILE), BF16),
            pltpu.VMEM((2, 4, SIDE, TILE), BF16),
            dma((5,)),
            dma((84,)),
            dma((84,)),
            dma((28,)),
            dma((28,)),
            dma((3, NT, 2)),
            dma((3, NT, 2)),
            dma((3, NT, 2)),
            dma((3, NT, 2)),
            dma((NT, 2)),
            dma((NT, 2)),
            dma((2, 4)),
            dma((2, 4)),
        ],
        compiler_params=pltpu.CompilerParams(
            collective_id=0, has_side_effects=True, vmem_limit_bytes=58 << 20
        ),
    )(
        images,
        references,
        shell_of_pixel.reshape(1, PIX),
        noise_power.reshape(1, 64),
        ref_class.reshape(NREF // 128, 128),
        ref_orient.reshape(NREF // 128, 128),
        orient_logw.reshape(1, NORIENT),
        class_logw,
    )
    accumulators, evidence = pl.pallas_call(
        hand_over,
        out_shape=(
            jax.ShapeDtypeStruct((ROWS, PIX), F32),
            jax.ShapeDtypeStruct((NIM // 128, 128), F32),
        ),
        in_specs=[pl.BlockSpec(memory_space=pltpu.HBM)] * 2,
        out_specs=(pl.BlockSpec(memory_space=pltpu.HBM),) * 2,
        scratch_shapes=[
            pltpu.VMEM((ROWS, PIX), F32),
            pltpu.VMEM((NIM // 128, 128), F32),
            dma((2, 2)),
        ],
    )(accumulators, evidence)
    return accumulators, evidence.reshape(NIM)


def solution(mesh):
    placed = (P("img", "shell"), P("img", "shell"), P("shell"), P(), P(), P(), P(), P())
    return jax.shard_map(
        shards, mesh=mesh, in_specs=placed, out_specs=(P("img", "shell"), P("img")), check_vma=False
    )
```

```python
import jax
import jax.numpy as jnp
from jax import lax
from jax.experimental import pallas as pl
from jax.experimental.pallas import tpu as pltpu
from jax.sharding import PartitionSpec as P

INVERSE_HEAT = 0.5
MESH = pl.DeviceIdType.MESH
F32 = jnp.float32
BF16 = jnp.bfloat16

NZ, NY, NX = 4, 2, 4
ROWS = 32
PIECE = 16
PIX = 4096
NIM = 768
HALF = NIM // 2
GROUP = 256
SIDE = GROUP // 2
NREF = 1024
TILE = 512
NT = PIX // TILE
PH = PIX // 2
NORIENT = 6144

FORWARD = [(0, 0), (0, 1), (3, 0), (1, 0), (3, 1), (1, 1), (2, 0), (2, 1)]
BATCHES = [
    [(0, b, yr) for b, yr in FORWARD],
    [(g, b, yr) for g in (1, 3) for b, yr in FORWARD[:4]],
    [(g, b, yr) for g in (1, 3) for b, yr in FORWARD[4:6]],
    [(g, b, yr) for g in (1, 3) for b, yr in FORWARD[6:]],
    [(2, b, yr) for b, yr in FORWARD[:4]],
    [(2, b, yr) for b, yr in FORWARD[4:6]],
    [(2, b, yr) for b, yr in FORWARD[6:]],
]
SHARED = 4
SCORE_ROW = [0, 256, 512, 640, 768, 896, 960]
SUM_ROW = [0, 128, 256, 320, 384, 512, 576]


def kernel(
    images_hbm,
    references_hbm,
    shell_ref,
    noise_ref,
    class_id_ref,
    orient_id_ref,
    orient_ref,
    class_ref,
    out_ref,
    evidence_ref,
    im,
    wim,
    refs,
    score,
    core_in,
    row_out,
    row_in,
    total,
    weight,
    square,
    columns,
    prior,
    evid,
    stat_out,
    stat_in,
    post,
    s1,
    s2,
    s3,
    r_opp,
    r_plus,
    r_minus,
    acc,
    z1,
    z2,
    z3,
    zr_opp,
    zr_plus,
    zr_minus,
    y_out,
    y_in,
    kept,
    f_out,
    f_in,
    load_sem,
    ag_s,
    ag_r,
    ex_s,
    ex_r,
    a_s,
    a_r,
    b_s,
    b_r,
    yy_s,
    yy_r,
    f_s,
    f_r,
):
    s = lax.axis_index("shell")
    i = lax.axis_index("img")
    core = lax.rem(s, 2)
    y_hi = s // 2
    z = i // (NY * NX)
    y = lax.rem(i // NX, NY)
    x = lax.rem(i, NX)

    def at(zz, yv, xx):
        return (zz * NY + yv) * NX + xx

    x_plus = (s, at(z, y, lax.rem(x + 1, NX)))
    x_minus = (s, at(z, y, lax.rem(x + NX - 1, NX)))
    z_plus = (s, at(lax.rem(z + 1, NZ), y, x))
    z_minus = (s, at(lax.rem(z + NZ - 1, NZ), y, x))
    y_pal = (s, at(z, 1 - y, x))
    core_pal = (y_hi * 2 + 1 - core, i)
    hi_pal = ((1 - y_hi) * 2 + core, i)
    a_plus, a_minus = (x_plus, z_plus), (x_minus, z_minus)
    b_plus, b_minus = (z_plus, x_plus), (z_minus, x_minus)

    def remote(src, dst, send_sem, recv_sem, peer):
        return pltpu.make_async_remote_copy(
            src_ref=src,
            dst_ref=dst,
            send_sem=send_sem,
            recv_sem=recv_sem,
            device_id=peer,
            device_id_type=MESH,
        )

    def landed(dst, send_sem, recv_sem):
        remote(dst, dst, send_sem, recv_sem, core_pal).wait_recv()

    own = []
    for t in range(2):
        c = pltpu.make_async_copy(
            references_hbm.at[pl.ds(t * PIECE, PIECE), :],
            refs.at[0, pl.ds(t * SIDE, PIECE), :],
            load_sem.at[t],
        )
        c.start()
        own.append(c)
    image_loads = []
    for n in range(3):
        c = pltpu.make_async_copy(
            images_hbm.at[pl.ds(n * 256, 256), :], im.at[pl.ds(n * 256, 256), :], load_sem.at[2 + n]
        )
        c.start()
        image_loads.append(c)

    barrier = pltpu.get_barrier_semaphore()
    for peer in (x_plus, x_minus, z_plus, z_minus, y_pal, core_pal, hi_pal):
        pl.semaphore_signal(barrier, inc=1, device_id=peer, device_id_type=MESH)
    pl.semaphore_wait(barrier, 7)

    index = {}
    ag_sends = []

    def slot(name):
        if name not in index:
            index[name] = len(index)
        return index[name]

    def piece(t, a, b, yr, part=None):
        rows = pl.ds(t * SIDE + b * 32 + yr * PIECE, PIECE)
        if part is None:
            return refs.at[a, rows, :]
        return refs.at[a, rows, pl.ds(part * PH, PH)]

    def ag_send(name, src, dst, peer):
        n = slot(name)
        c = remote(src, dst, ag_s.at[n], ag_r.at[n], peer)
        c.start()
        ag_sends.append(c)

    def ag_wait(name, dst):
        n = slot(name)
        landed(dst, ag_s.at[n], ag_r.at[n])

    def send_b(t, yr):
        ag_send(("b+", t, yr), piece(t, 0, 0, yr), piece(t, 0, 3, yr), b_plus[t])
        ag_send(("b-", t, yr), piece(t, 0, 0, yr), piece(t, 0, 1, yr), b_minus[t])

    def send_a(t, b, yr):
        ag_send(("a+", t, b, yr), piece(t, 0, b, yr), piece(t, 3, b, yr), a_plus[t])
        ag_send(("a-", t, b, yr), piece(t, 0, b, yr), piece(t, 1, b, yr), a_minus[t])

    def log_prior():
        square[...] = jnp.zeros((128, 128), F32)
        for n, ids in enumerate((class_id_ref, orient_id_ref)):
            square[0:8, :] = ids[...].astype(F32)
            columns[n] = square[...].T

        def place(row, a, b, yr, kind):
            za = lax.rem(z + jnp.where(kind == 0, b, a), NZ)
            xa = lax.rem(x + jnp.where(kind == 0, a, b), NX)
            ya = y if yr == 0 else 1 - y
            first = at(za, ya, xa) * ROWS + kind * PIECE
            rows = pl.ds(pl.multiple_of(lax.rem(first, 128), PIECE), PIECE)
            pick = lax.broadcasted_iota(jnp.int32, (PIECE, 128), 1) == first // 128
            for n in range(2):
                found = jnp.sum(jnp.where(pick, columns[n, rows, :], 0.0), axis=1, keepdims=True)
                prior[n, pl.ds(row, PIECE), :] = found

        for n, batch in enumerate(BATCHES):
            for k, (g, b, yr) in enumerate(batch):
                if n < SHARED:
                    place(SUM_ROW[n] + k * PIECE, g, b, yr, y_hi)
                else:
                    for t in range(2):
                        place(SUM_ROW[n] + (t * len(batch) + k) * PIECE, g, b, yr, t)

        @pl.loop(0, 5)
        def _(block):
            rows = pl.ds(pl.multiple_of(block * SIDE, SIDE), SIDE)
            kind = prior[0, rows, :]
            orient = jnp.broadcast_to(prior[1, rows, :], (SIDE, 128)).astype(jnp.int32)

            def add(n, sums):
                cols = pl.ds(pl.multiple_of(n * 128, 128), 128)
                ids = lax.broadcasted_iota(jnp.int32, (SIDE, 128), 1) + n * 128
                logw = jnp.broadcast_to(orient_ref[:, cols], (SIDE, 128))
                return sums + jnp.where(orient == ids, logw, 0.0)

            sums = lax.fori_loop(0, NORIENT // 128, add, jnp.zeros((SIDE, 128), F32))
            found = jnp.zeros((SIDE, 1), F32)
            for n in range(4):
                found = found + jnp.where(kind == float(n), class_ref[n], 0.0)
            prior[0, rows, :] = found + jnp.sum(sums, axis=1, keepdims=True)

    for t in range(2):
        own[t].wait()
    for t in range(2):
        ag_send(("y", t), piece(t, 0, 0, 0), piece(t, 0, 0, 1), y_pal)
    for t in range(2):
        send_b(t, 0)
    for t in range(2):
        send_a(t, 0, 0)

    noise_row = 1.0 / noise_ref[...]
    r64 = lax.broadcasted_iota(jnp.int32, (64, 64), 0)
    c64 = lax.broadcasted_iota(jnp.int32, (64, 64), 1)
    noise_col = jnp.sum(
        jnp.where(r64 == c64, jnp.broadcast_to(noise_row, (64, 64)), 0.0), axis=1, keepdims=True
    )

    @pl.loop(0, PIX // 512)
    def _(n):
        cols = pl.ds(pl.multiple_of(n * 512, 512), 512)
        shell = jnp.broadcast_to(shell_ref[:, cols], (64, 512))
        hit = shell == lax.broadcasted_iota(jnp.int32, (64, 512), 0)
        weight[:, cols] = jnp.sum(
            jnp.where(hit, jnp.broadcast_to(noise_col, (64, 512)), 0.0), axis=0, keepdims=True
        )

    for t in range(2):
        ag_wait(("y", t), piece(t, 0, 0, 1))
        send_b(t, 1)
        send_a(t, 0, 1)

    for n in range(3):
        image_loads[n].wait()

        @pl.loop(0, PIX // 256)
        def _(k):
            cols = pl.ds(pl.multiple_of(k * 256, 256), 256)
            rows = pl.ds(n * 256, 256)
            wim[cols, rows] = (im[rows, cols].astype(F32) * weight[:, cols]).astype(BF16).T

    def pass_b(yr):
        for t in range(2):
            ag_wait(("b+", t, yr), piece(t, 0, 3, yr))
            ag_send(("bf+", t, yr), piece(t, 0, 3, yr, 0), piece(t, 0, 2, yr, 0), b_plus[t])
            ag_wait(("b-", t, yr), piece(t, 0, 1, yr))
            ag_send(("bf-", t, yr), piece(t, 0, 1, yr, 1), piece(t, 0, 2, yr, 1), b_minus[t])
        for t in range(2):
            send_a(t, 3, yr)
            send_a(t, 1, yr)

    def pass_a(b, yr):
        for t in range(2):
            ag_wait(("a+", t, b, yr), piece(t, 3, b, yr))
            ag_send(("af+", t, b, yr), piece(t, 3, b, yr, 0), piece(t, 2, b, yr, 0), a_plus[t])
            ag_wait(("a-", t, b, yr), piece(t, 1, b, yr))
            ag_send(("af-", t, b, yr), piece(t, 1, b, yr, 1), piece(t, 2, b, yr, 1), a_minus[t])

    def opposite_landed(pieces):
        for b, yr in pieces:
            for t in range(2):
                ag_wait(("af+", t, b, yr), piece(t, 2, b, yr, 0))
                ag_wait(("af-", t, b, yr), piece(t, 2, b, yr, 1))

    pass_b(0)
    pass_a(0, 0)
    pass_a(0, 1)
    pass_b(1)
    log_prior()
    pass_a(3, 0)
    pass_a(1, 0)
    for yr in range(2):
        for t in range(2):
            ag_wait(("bf+", t, yr), piece(t, 0, 2, yr, 0))
            ag_wait(("bf-", t, yr), piece(t, 0, 2, yr, 1))
            send_a(t, 2, yr)

    mine = pl.ds(pl.multiple_of(core * HALF, 128), HALF)
    theirs = pl.ds(pl.multiple_of((1 - core) * HALF, 128), HALF)
    keep = pl.ds(pl.multiple_of(y_hi * SIDE, SIDE), SIDE)
    give = pl.ds(pl.multiple_of((1 - y_hi) * SIDE, SIDE), SIDE)
    ex_sends = []

    def ex_send(n, src, dst, peer):
        c = remote(src, dst, ex_s.at[n], ex_r.at[n], peer)
        c.start()
        ex_sends.append(c)

    def ex_wait(n, dst):
        landed(dst, ex_s.at[n], ex_r.at[n])

    def size(n):
        return 2 * PIECE * len(BATCHES[n])

    def score_rows(n):
        return pl.ds(SCORE_ROW[n], size(n))

    def sum_rows(n):
        return pl.ds(SUM_ROW[n], size(n) // 2 if n < SHARED else size(n))

    def kind_rows(n, kind):
        return pl.ds(pl.multiple_of(SCORE_ROW[n] + kind * (size(n) // 2), 16), size(n) // 2)

    def do_scores(n):
        batch = BATCHES[n]
        n_rows = size(n)
        rows = score_rows(n)

        def of(cols):
            return jnp.concatenate(
                [
                    refs[g, t * SIDE + b * 32 + yr * PIECE : t * SIDE + b * 32 + (yr + 1) * PIECE, cols]
                    for t in range(2)
                    for g, b, yr in batch
                ],
                axis=0,
            )

        def add(k, sums, chunks):
            for u in range(chunks):
                cols = pl.ds(pl.multiple_of((k * chunks + u) * 128, 128), 128)
                part = of(cols).astype(F32)
                sums = sums + part * part * weight[:, cols]
            return sums

        zero = jnp.zeros((n_rows, 128), F32)
        if n_rows > 128:
            sums = lax.fori_loop(0, PIX // 512, lambda k, v: add(k, v, 4), zero)
        else:
            sums = add(0, zero, PIX // 256) + add(1, zero, PIX // 256)
        norm = 0.5 * jnp.sum(sums, axis=1, keepdims=True)
        part = jnp.dot(of(slice(None)), wim[...], preferred_element_type=F32)
        score[rows, :] = part - norm
        ex_send(n, score.at[rows, theirs], core_in.at[rows], core_pal)

    def do_rows(n):
        rows, sums = score_rows(n), sum_rows(n)
        ex_wait(n, core_in.at[rows])
        if n < SHARED:
            away, home = kind_rows(n, 1 - y_hi), kind_rows(n, y_hi)
            row_out[sums] = score[away, mine] + core_in[away, :]
            ex_send(7 + n, row_out.at[sums], row_in.at[sums], hi_pal)
            total[sums] = score[home, mine] + core_in[home, :]
        else:
            row_out[sums] = score[rows, mine] + core_in[rows, :]
            ex_send(7 + n, row_out.at[sums], row_in.at[sums], hi_pal)

    def do_logits(n):
        sums = sum_rows(n)
        ex_wait(7 + n, row_in.at[sums])
        near = total if n < SHARED else row_out
        logits = INVERSE_HEAT * (near[sums] + row_in[sums]) + prior[0, sums, :]
        total[sums] = logits
        return jnp.max(logits, axis=0, keepdims=True)

    def mass_of(rows, top):
        return jnp.sum(jnp.exp(total[rows] - top), axis=0, keepdims=True)

    shared_rows = pl.ds(0, 3 * SIDE)
    do_scores(0)
    do_scores(1)
    do_rows(0)
    do_rows(1)
    pass_a(3, 1)
    pass_a(1, 1)
    do_scores(2)
    opposite_landed(FORWARD[:4])
    do_scores(4)
    do_rows(2)
    do_rows(4)
    pass_a(2, 0)
    pass_a(2, 1)
    do_scores(3)
    opposite_landed(FORWARD[4:6])
    do_rows(3)
    do_scores(5)
    top = jnp.maximum(do_logits(0), do_logits(1))
    opposite_landed(FORWARD[6:])
    do_rows(5)
    do_scores(6)
    top = jnp.maximum(top, do_logits(2))
    top = jnp.maximum(top, do_logits(3))
    mass = mass_of(shared_rows, top)
    stat_out[0:1, :] = top
    stat_out[1:2, :] = mass
    ex_send(14, stat_out.at[0:8], stat_in.at[0:8], hi_pal)
    do_rows(6)
    last_top = jnp.maximum(do_logits(4), do_logits(5))
    ex_wait(14, stat_in.at[0:8])
    other_top, other_mass = stat_in[0:1, :], stat_in[1:2, :]
    first = y_hi == 0
    top_a, top_b = jnp.where(first, top, other_top), jnp.where(first, other_top, top)
    mass_a, mass_b = jnp.where(first, mass, other_mass), jnp.where(first, other_mass, mass)
    last_top = jnp.maximum(last_top, do_logits(6))
    best = jnp.maximum(jnp.maximum(top_a, top_b), last_top)
    evidence = best + jnp.log(
        mass_a * jnp.exp(top_a - best) + mass_b * jnp.exp(top_b - best) + mass_of(pl.ds(3 * SIDE, 2 * SIDE), best)
    )
    for n in range(SHARED, len(BATCHES)):
        p = jnp.exp(total[sum_rows(n)] - evidence).astype(BF16)
        for t in range(2):
            for k, (g, b, yr) in enumerate(BATCHES[n]):
                o = (t * len(BATCHES[n]) + k) * PIECE
                rows = pl.ds(t * SIDE + b * 32 + yr * PIECE, PIECE)
                post[g, rows, mine] = p[o : o + PIECE, :]
    ex_send(22, post.at[2, :, mine], post.at[2, :, mine], core_pal)
    stat_out[8:16, :] = jnp.broadcast_to(evidence, (8, HALF))
    for n in (1, 2, 3, 0):
        p = jnp.exp(total[sum_rows(n)] - evidence).astype(BF16)
        for k, (g, b, yr) in enumerate(BATCHES[n]):
            first_row = pl.multiple_of(y_hi * SIDE + b * 32 + yr * PIECE, PIECE)
            post[g, pl.ds(first_row, PIECE), mine] = p[k * PIECE : (k + 1) * PIECE, :]
        for g in {3: (1, 3), 0: (0,)}.get(n, ()):
            ex_send(16 + g, post.at[g, keep, mine], post.at[g, keep, mine], hi_pal)
            ex_send(20 + g, post.at[g, keep, mine], post.at[g, keep, mine], core_pal)
    ex_send(15, stat_out.at[8:16], stat_in.at[8:16], core_pal)

    def do_relay(g):
        ex_wait(16 + g, post.at[g, give, mine])
        ex_send(24 + g, post.at[g, give, mine], post.at[g, give, mine], core_pal)

    def do_posterior(g):
        ex_wait(20 + g, post.at[g, keep, theirs])
        ex_wait(24 + g, post.at[g, give, theirs])

    def product(g, j):
        cols = pl.ds(pl.multiple_of(j * TILE, TILE), TILE)
        return jnp.dot(post[g], im[:, cols], preferred_element_type=F32)

    def a_rows(j, t):
        return pl.ds(t * SIDE, 64 if isinstance(j, int) and j % 4 == 3 else SIDE)

    def a_copy(kind, j, t, src, dst, peer):
        rows = a_rows(j, t)
        return remote(
            src.at[j, rows], dst.at[j, rows], a_s.at[kind, j, t], a_r.at[kind, j, t], peer
        )

    def a_landed(kind, j, t, dst):
        landed(dst.at[j, a_rows(j, t)], a_s.at[kind, j, t], a_r.at[kind, j, t])

    def f_copy(g, n):
        return remote(f_out.at[n, g], f_in.at[n, g], f_s.at[n, g], f_r.at[n, g], y_pal)

    def first_product(g, n):
        p = product(g, 3 + 4 * n).reshape(8, 2, PIECE, TILE)
        f_out[n, g] = p[:, 1].reshape(SIDE, TILE).astype(BF16)
        f_copy(g, n).start()
        kept[n, g] = p[:, 0].reshape(SIDE, TILE)

    def first_sum(g, n):
        f_copy(g, n).wait_recv()
        return kept[n, g] + f_in[n, g].astype(F32)

    def put(dst, j, rows):
        for t in range(2):
            dst[j, a_rows(j, t)] = rows[t * 64 : t * 64 + 64, :].astype(BF16)

    def get(src, j):
        return jnp.concatenate([src[j, a_rows(j, t)] for t in range(2)], axis=0).astype(F32)

    ex_wait(22, post.at[2, :, theirs])

    @pl.loop(0, 3)
    def _(k):
        s2[k] = product(2, k).astype(BF16)
        for t in range(2):
            a_copy(0, k, t, s2, r_opp, a_plus[t]).start()
        s2[k + 4] = product(2, k + 4).astype(BF16)
        for t in range(2):
            a_copy(0, k + 4, t, s2, r_opp, a_minus[t]).start()

    for n in range(2):
        first_product(2, n)
    def free(k):
        s1[k + 4] = product(1, k + 4).astype(BF16)
        for t in range(2):
            a_copy(1, k + 4, t, s1, r_minus, a_plus[t]).start()
        s3[k] = product(3, k).astype(BF16)
        for t in range(2):
            a_copy(2, k, t, s3, r_plus, a_minus[t]).start()

    def bound(k):
        p1 = product(1, k)
        for t in range(2):
            a_landed(0, k, t, r_opp)
        s1[k] = (p1 + r_opp[k].astype(F32)).astype(BF16)
        for t in range(2):
            a_copy(1, k, t, s1, r_minus, a_plus[t]).start()
        p3 = product(3, k + 4)
        for t in range(2):
            a_landed(0, k + 4, t, r_opp)
        s3[k + 4] = (p3 + r_opp[k + 4].astype(F32)).astype(BF16)
        for t in range(2):
            a_copy(2, k + 4, t, s3, r_plus, a_minus[t]).start()

    do_relay(1)
    do_relay(3)
    do_posterior(1)
    do_posterior(3)
    first_product(1, 1)
    first_product(3, 0)
    first_product(1, 0)
    first_product(3, 1)
    free(0)

    @pl.loop(0, 2)
    def _(k):
        bound(k)

    do_relay(0)
    do_posterior(0)
    for n in range(2):
        first_product(0, n)

    ex_wait(15, stat_in.at[8:16])
    evid[:, mine] = stat_out[8:9, :]
    evid[:, theirs] = stat_in[8:9, :]
    for n in range(NIM // 128):
        evidence_ref[n : n + 1, :] = evid[:, n * 128 : n * 128 + 128]

    def b_copy(kind, j, t, src, dst, peer):
        rows = pl.ds(0, PIECE if j % 4 == 3 else 32)
        return remote(
            src.at[j, t, rows], dst.at[j, t, rows], b_s.at[kind, j, t], b_r.at[kind, j, t], peer
        )

    def b_landed(kind, j, t, dst):
        b_copy(kind, j, t, dst, dst, core_pal).wait_recv()

    def y_copy(j, t):
        return remote(y_out.at[j, t], y_in.at[j, t], yy_s.at[j, t], yy_r.at[j, t], y_pal)

    def first_opposite():
        for n, j in enumerate((3, 7)):
            put(s2, j, first_sum(2, n))
            for t in range(2):
                a_copy(0, j, t, s2, r_opp, (a_plus, a_minus)[n][t]).start()

    def first_free():
        put(s1, 7, first_sum(1, 1))
        for t in range(2):
            a_copy(1, 7, t, s1, r_minus, a_plus[t]).start()
        put(s3, 3, first_sum(3, 0))
        for t in range(2):
            a_copy(2, 3, t, s3, r_plus, a_minus[t]).start()

    def first_bound():
        for t in range(2):
            a_landed(0, 3, t, r_opp)
        put(s1, 3, first_sum(1, 0) + get(r_opp, 3))
        for t in range(2):
            a_copy(1, 3, t, s1, r_minus, a_plus[t]).start()
        for t in range(2):
            a_landed(0, 7, t, r_opp)
        put(s3, 7, first_sum(3, 1) + get(r_opp, 7))
        for t in range(2):
            a_copy(2, 7, t, s3, r_plus, a_minus[t]).start()

    def rows_of(j, t, b):
        n = PIECE if j % 4 == 3 else 32
        return pl.ds(t * SIDE + b * n, n)

    def step_a(k):
        for j, low in ((k, True), (k + 4, False)):
            p = None if k == 3 else product(0, j)
            for t in range(2):
                a_landed(1, j, t, r_minus)
                a_landed(2, j, t, r_plus)
            if k == 3:
                total_j = first_sum(0, j // 4) + get(r_plus, j) + get(r_minus, j)
                for t in range(2):
                    acc[j, a_rows(j, t)] = total_j[t * 64 : t * 64 + 64, :]
            else:
                acc[j] = p + r_plus[j].astype(F32) + r_minus[j].astype(F32)
            n = PIECE if k == 3 else 32
            for t in range(2):
                z2[j, t, 0:n] = acc[j, rows_of(j, t, 2), :].astype(BF16)
                b_copy(0, j, t, z2, zr_opp, b_plus[t] if low else b_minus[t]).start()
                if low:
                    z3[j, t, 0:n] = acc[j, rows_of(j, t, 3), :].astype(BF16)
                    b_copy(2, j, t, z3, zr_plus, b_minus[t]).start()
                else:
                    z1[j, t, 0:n] = acc[j, rows_of(j, t, 1), :].astype(BF16)
                    b_copy(1, j, t, z1, zr_minus, b_plus[t]).start()

    def step_b(k):
        n = PIECE if k == 3 else 32
        for t in range(2):
            b_landed(0, k, t, zr_opp)
            v = acc[k, rows_of(k, t, 1), :] + zr_opp[k, t, 0:n].astype(F32)
            z1[k, t, 0:n] = v.astype(BF16)
            b_copy(1, k, t, z1, zr_minus, b_plus[t]).start()
            j = k + 4
            b_landed(0, j, t, zr_opp)
            v = acc[j, rows_of(j, t, 3), :] + zr_opp[j, t, 0:n].astype(F32)
            z3[j, t, 0:n] = v.astype(BF16)
            b_copy(2, j, t, z3, zr_plus, b_minus[t]).start()

    def step_c(k):
        n = PIECE if k == 3 else 32
        for j in (k, k + 4):
            cols = pl.ds(j * TILE, TILE)
            for t in range(2):
                b_landed(1, j, t, zr_minus)
                b_landed(2, j, t, zr_plus)
                v = acc[j, rows_of(j, t, 0), :] + zr_plus[j, t, 0:n].astype(F32)
                v = v + zr_minus[j, t, 0:n].astype(F32)
                out_ref[t * PIECE : (t + 1) * PIECE, cols] = v[:PIECE, :]
                if k < 3:
                    y_out[j, t] = v[PIECE:, :].astype(BF16)
                    y_copy(j, t).start()

    def step_d(k):
        for j in (k, k + 4):
            cols = pl.ds(j * TILE, TILE)
            for t in range(2):
                y_copy(j, t).wait_recv()
                rows = slice(t * PIECE, (t + 1) * PIECE)
                out_ref[rows, cols] = out_ref[rows, cols] + y_in[j, t].astype(F32)

    step_a(0)
    first_opposite()

    @pl.loop(1, 3)
    def _(k):
        free(k)

    bound(2)
    first_free()
    step_a(1)
    step_b(0)
    step_a(2)
    first_bound()
    step_c(0)
    step_b(1)
    step_b(2)
    step_a(3)
    step_c(1)
    step_c(2)
    step_b(3)
    step_d(0)
    step_d(1)
    step_c(3)
    step_d(2)

    for c in ag_sends:
        c.wait_send()
    for c in ex_sends:
        c.wait_send()

    for j in range(NT):
        for t in range(2):
            a_copy(0, j, t, s2, r_opp, core_pal).wait_send()
            a_copy(1, j, t, s1, r_minus, core_pal).wait_send()
            a_copy(2, j, t, s3, r_plus, core_pal).wait_send()
            b_copy(0, j, t, z2, zr_opp, core_pal).wait_send()
            b_copy(1, j, t, z1, zr_minus, core_pal).wait_send()
            b_copy(2, j, t, z3, zr_plus, core_pal).wait_send()
            if j % 4 < 3:
                y_copy(j, t).wait_send()
    for n in range(2):
        for g in range(4):
            f_copy(g, n).wait_send()


def hand_over(sums_hbm, evidence_hbm, sums_out, evidence_out, sums, evidence, sems):
    sources, held = (sums_hbm, evidence_hbm), (sums, evidence)
    for n, out in enumerate((sums_out, evidence_out)):
        pltpu.make_async_copy(sources[n], held[n], sems.at[0, n]).start()
    for n, out in enumerate((sums_out, evidence_out)):
        pltpu.make_async_copy(sources[n], held[n], sems.at[0, n]).wait()
        pltpu.make_async_copy(held[n], out, sems.at[1, n]).start()
    for n, out in enumerate((sums_out, evidence_out)):
        pltpu.make_async_copy(held[n], out, sems.at[1, n]).wait()


def shards(
    images, references, shell_of_pixel, noise_power, ref_class, ref_orient, class_logw, orient_logw
):
    vmem = pl.BlockSpec(memory_space=pltpu.VMEM)
    hbm = pl.BlockSpec(memory_space=pl.ANY)
    smem = pl.BlockSpec(memory_space=pltpu.SMEM)
    dma = pltpu.SemaphoreType.DMA
    accumulators, evidence = pl.pallas_call(
        kernel,
        out_shape=(
            jax.ShapeDtypeStruct((ROWS, PIX), F32),
            jax.ShapeDtypeStruct((NIM // 128, 128), F32),
        ),
        in_specs=[hbm, hbm, vmem, vmem, vmem, vmem, vmem, smem],
        out_specs=(vmem, vmem),
        scratch_shapes=[
            pltpu.VMEM((NIM, PIX), BF16),
            pltpu.VMEM((PIX, NIM), BF16),
            pltpu.VMEM((4, GROUP, PIX), BF16),
            pltpu.VMEM((NREF, NIM), F32),
            pltpu.VMEM((NREF, HALF), F32),
            pltpu.VMEM((5 * SIDE, HALF), F32),
            pltpu.VMEM((5 * SIDE, HALF), F32),
            pltpu.VMEM((5 * SIDE, HALF), F32),
            pltpu.VMEM((1, PIX), F32),
            pltpu.VMEM((128, 128), F32),
            pltpu.VMEM((2, 128, 128), F32),
            pltpu.VMEM((2, 5 * SIDE, 1), F32),
            pltpu.VMEM((1, NIM), F32),
            pltpu.VMEM((16, HALF), F32),
            pltpu.VMEM((16, HALF), F32),
            pltpu.VMEM((4, GROUP, NIM), BF16),
            pltpu.VMEM((NT, GROUP, TILE), BF16),
            pltpu.VMEM((NT, GROUP, TILE), BF16),
            pltpu.VMEM((NT, GROUP, TILE), BF16),
            pltpu.VMEM((NT, GROUP, TILE), BF16),
            pltpu.VMEM((NT, GROUP, TILE), BF16),
            pltpu.VMEM((NT, GROUP, TILE), BF16),
            pltpu.VMEM((NT, GROUP, TILE), F32),
            pltpu.VMEM((NT, 2, 32, TILE), BF16),
            pltpu.VMEM((NT, 2, 32, TILE), BF16),
            pltpu.VMEM((NT, 2, 32, TILE), BF16),
            pltpu.VMEM((NT, 2, 32, TILE), BF16),
            pltpu.VMEM((NT, 2, 32, TILE), BF16),
            pltpu.VMEM((NT, 2, 32, TILE), BF16),
            pltpu.VMEM((NT, 2, PIECE, TILE), BF16),
            pltpu.VMEM((NT, 2, PIECE, TILE), BF16),
            pltpu.VMEM((2, 4, SIDE, TILE), F32),
            pltpu.VMEM((2, 4, SIDE, TILE), BF16),
            pltpu.VMEM((2, 4, SIDE, TILE), BF16),
            dma((5,)),
            dma((84,)),
            dma((84,)),
            dma((28,)),
            dma((28,)),
            dma((3, NT, 2)),
            dma((3, NT, 2)),
            dma((3, NT, 2)),
            dma((3, NT, 2)),
            dma((NT, 2)),
            dma((NT, 2)),
            dma((2, 4)),
            dma((2, 4)),
        ],
        compiler_params=pltpu.CompilerParams(
            collective_id=0, has_side_effects=True, vmem_limit_bytes=58 << 20
        ),
    )(
        images,
        references,
        shell_of_pixel.reshape(1, PIX),
        noise_power.reshape(1, 64),
        ref_class.reshape(NREF // 128, 128),
        ref_orient.reshape(NREF // 128, 128),
        orient_logw.reshape(1, NORIENT),
        class_logw,
    )
    accumulators, evidence = pl.pallas_call(
        hand_over,
        out_shape=(
            jax.ShapeDtypeStruct((ROWS, PIX), F32),
            jax.ShapeDtypeStruct((NIM // 128, 128), F32),
        ),
        in_specs=[pl.BlockSpec(memory_space=pltpu.HBM)] * 2,
        out_specs=(pl.BlockSpec(memory_space=pltpu.HBM),) * 2,
        scratch_shapes=[
            pltpu.VMEM((ROWS, PIX), F32),
            pltpu.VMEM((NIM // 128, 128), F32),
            dma((2, 2)),
        ],
    )(accumulators, evidence)
    return accumulators, evidence.reshape(NIM)


def solution(mesh):
    placed = (P("img", "shell"), P("img", "shell"), P("shell"), P(), P(), P(), P(), P())
    return jax.shard_map(
        shards, mesh=mesh, in_specs=placed, out_specs=(P("img", "shell"), P("img")), check_vma=False
    )
```

```python
import jax
import jax.numpy as jnp
from jax import lax
from jax.experimental import pallas as pl
from jax.experimental.pallas import tpu as pltpu
from jax.sharding import PartitionSpec as P

INVERSE_HEAT = 0.5
MESH = pl.DeviceIdType.MESH
F32 = jnp.float32
BF16 = jnp.bfloat16

NZ, NY, NX = 4, 2, 4
ROWS = 32
PIECE = 16
PIX = 4096
NIM = 768
HALF = NIM // 2
GROUP = 256
SIDE = GROUP // 2
NREF = 1024
TILE = 512
NT = PIX // TILE
PH = PIX // 2
NORIENT = 6144

FORWARD = [(0, 0), (0, 1), (3, 0), (1, 0), (3, 1), (1, 1), (2, 0), (2, 1)]
BATCHES = [
    [(0, b, yr) for b, yr in FORWARD],
    [(g, b, yr) for g in (1, 3) for b, yr in FORWARD[:4]],
    [(g, b, yr) for g in (1, 3) for b, yr in FORWARD[4:6]],
    [(g, b, yr) for g in (1, 3) for b, yr in FORWARD[6:]],
    [(2, b, yr) for b, yr in FORWARD[:4]],
    [(2, b, yr) for b, yr in FORWARD[4:6]],
    [(2, b, yr) for b, yr in FORWARD[6:]],
]
SHARED = 4
SCORE_ROW = [0, 256, 512, 640, 768, 896, 960]
SUM_ROW = [0, 128, 256, 320, 384, 512, 576]


def kernel(
    images_hbm,
    references_hbm,
    shell_ref,
    noise_ref,
    class_id_ref,
    orient_id_ref,
    orient_ref,
    class_ref,
    out_ref,
    evidence_ref,
    im,
    wim,
    refs,
    score,
    core_in,
    row_out,
    row_in,
    total,
    weight,
    square,
    columns,
    prior,
    evid,
    stat_out,
    stat_in,
    post,
    s1,
    s2,
    s3,
    r_opp,
    r_plus,
    r_minus,
    acc,
    z1,
    z2,
    z3,
    zr_opp,
    zr_plus,
    zr_minus,
    y_out,
    y_in,
    kept,
    f_out,
    f_in,
    load_sem,
    ag_s,
    ag_r,
    ex_s,
    ex_r,
    a_s,
    a_r,
    b_s,
    b_r,
    yy_s,
    yy_r,
    f_s,
    f_r,
):
    s = lax.axis_index("shell")
    i = lax.axis_index("img")
    core = lax.rem(s, 2)
    y_hi = s // 2
    z = i // (NY * NX)
    y = lax.rem(i // NX, NY)
    x = lax.rem(i, NX)

    def at(zz, yv, xx):
        return (zz * NY + yv) * NX + xx

    x_plus = (s, at(z, y, lax.rem(x + 1, NX)))
    x_minus = (s, at(z, y, lax.rem(x + NX - 1, NX)))
    z_plus = (s, at(lax.rem(z + 1, NZ), y, x))
    z_minus = (s, at(lax.rem(z + NZ - 1, NZ), y, x))
    y_pal = (s, at(z, 1 - y, x))
    core_pal = (y_hi * 2 + 1 - core, i)
    hi_pal = ((1 - y_hi) * 2 + core, i)
    a_plus, a_minus = (x_plus, z_plus), (x_minus, z_minus)
    b_plus, b_minus = (z_plus, x_plus), (z_minus, x_minus)

    def remote(src, dst, send_sem, recv_sem, peer):
        return pltpu.make_async_remote_copy(
            src_ref=src,
            dst_ref=dst,
            send_sem=send_sem,
            recv_sem=recv_sem,
            device_id=peer,
            device_id_type=MESH,
        )

    def landed(dst, send_sem, recv_sem):
        remote(dst, dst, send_sem, recv_sem, core_pal).wait_recv()

    own = []
    for t in range(2):
        c = pltpu.make_async_copy(
            references_hbm.at[pl.ds(t * PIECE, PIECE), :],
            refs.at[0, pl.ds(t * SIDE, PIECE), :],
            load_sem.at[t],
        )
        c.start()
        own.append(c)
    image_loads = []
    for n in range(3):
        c = pltpu.make_async_copy(
            images_hbm.at[pl.ds(n * 256, 256), :], im.at[pl.ds(n * 256, 256), :], load_sem.at[2 + n]
        )
        c.start()
        image_loads.append(c)

    barrier = pltpu.get_barrier_semaphore()
    for peer in (x_plus, x_minus, z_plus, z_minus, y_pal, core_pal, hi_pal):
        pl.semaphore_signal(barrier, inc=1, device_id=peer, device_id_type=MESH)
    pl.semaphore_wait(barrier, 7)

    index = {}
    ag_sends = []

    def slot(name):
        if name not in index:
            index[name] = len(index)
        return index[name]

    def piece(t, a, b, yr, part=None):
        rows = pl.ds(t * SIDE + b * 32 + yr * PIECE, PIECE)
        if part is None:
            return refs.at[a, rows, :]
        return refs.at[a, rows, pl.ds(part * PH, PH)]

    def ag_send(name, src, dst, peer):
        n = slot(name)
        c = remote(src, dst, ag_s.at[n], ag_r.at[n], peer)
        c.start()
        ag_sends.append(c)

    def ag_wait(name, dst):
        n = slot(name)
        landed(dst, ag_s.at[n], ag_r.at[n])

    def send_b(t, yr):
        ag_send(("b+", t, yr), piece(t, 0, 0, yr), piece(t, 0, 3, yr), b_plus[t])
        ag_send(("b-", t, yr), piece(t, 0, 0, yr), piece(t, 0, 1, yr), b_minus[t])

    def send_a(t, b, yr):
        ag_send(("a+", t, b, yr), piece(t, 0, b, yr), piece(t, 3, b, yr), a_plus[t])
        ag_send(("a-", t, b, yr), piece(t, 0, b, yr), piece(t, 1, b, yr), a_minus[t])

    def log_prior():
        square[...] = jnp.zeros((128, 128), F32)
        for n, ids in enumerate((class_id_ref, orient_id_ref)):
            square[0:8, :] = ids[...].astype(F32)
            columns[n] = square[...].T

        def place(row, a, b, yr, kind):
            za = lax.rem(z + jnp.where(kind == 0, b, a), NZ)
            xa = lax.rem(x + jnp.where(kind == 0, a, b), NX)
            ya = y if yr == 0 else 1 - y
            first = at(za, ya, xa) * ROWS + kind * PIECE
            rows = pl.ds(pl.multiple_of(lax.rem(first, 128), PIECE), PIECE)
            pick = lax.broadcasted_iota(jnp.int32, (PIECE, 128), 1) == first // 128
            for n in range(2):
                found = jnp.sum(jnp.where(pick, columns[n, rows, :], 0.0), axis=1, keepdims=True)
                prior[n, pl.ds(row, PIECE), :] = found

        for n, batch in enumerate(BATCHES):
            for k, (g, b, yr) in enumerate(batch):
                if n < SHARED:
                    place(SUM_ROW[n] + k * PIECE, g, b, yr, y_hi)
                else:
                    for t in range(2):
                        place(SUM_ROW[n] + (t * len(batch) + k) * PIECE, g, b, yr, t)

        @pl.loop(0, 5)
        def _(block):
            rows = pl.ds(pl.multiple_of(block * SIDE, SIDE), SIDE)
            kind = prior[0, rows, :]
            orient = jnp.broadcast_to(prior[1, rows, :], (SIDE, 128)).astype(jnp.int32)

            def add(n, sums):
                cols = pl.ds(pl.multiple_of(n * 128, 128), 128)
                ids = lax.broadcasted_iota(jnp.int32, (SIDE, 128), 1) + n * 128
                logw = jnp.broadcast_to(orient_ref[:, cols], (SIDE, 128))
                return sums + jnp.where(orient == ids, logw, 0.0)

            sums = lax.fori_loop(0, NORIENT // 128, add, jnp.zeros((SIDE, 128), F32))
            found = jnp.zeros((SIDE, 1), F32)
            for n in range(4):
                found = found + jnp.where(kind == float(n), class_ref[n], 0.0)
            prior[0, rows, :] = found + jnp.sum(sums, axis=1, keepdims=True)

    for t in range(2):
        own[t].wait()
    for t in range(2):
        ag_send(("y", t), piece(t, 0, 0, 0), piece(t, 0, 0, 1), y_pal)
    for t in range(2):
        send_b(t, 0)
    for t in range(2):
        send_a(t, 0, 0)

    noise_row = 1.0 / noise_ref[...]
    r64 = lax.broadcasted_iota(jnp.int32, (64, 64), 0)
    c64 = lax.broadcasted_iota(jnp.int32, (64, 64), 1)
    noise_col = jnp.sum(
        jnp.where(r64 == c64, jnp.broadcast_to(noise_row, (64, 64)), 0.0), axis=1, keepdims=True
    )

    @pl.loop(0, PIX // 512)
    def _(n):
        cols = pl.ds(pl.multiple_of(n * 512, 512), 512)
        shell = jnp.broadcast_to(shell_ref[:, cols], (64, 512))
        hit = shell == lax.broadcasted_iota(jnp.int32, (64, 512), 0)
        weight[:, cols] = jnp.sum(
            jnp.where(hit, jnp.broadcast_to(noise_col, (64, 512)), 0.0), axis=0, keepdims=True
        )

    for t in range(2):
        ag_wait(("y", t), piece(t, 0, 0, 1))
        send_b(t, 1)
        send_a(t, 0, 1)

    def pass_b(yr):
        for t in range(2):
            ag_wait(("b+", t, yr), piece(t, 0, 3, yr))
            ag_send(("bf+", t, yr), piece(t, 0, 3, yr, 0), piece(t, 0, 2, yr, 0), b_plus[t])
            ag_wait(("b-", t, yr), piece(t, 0, 1, yr))
            ag_send(("bf-", t, yr), piece(t, 0, 1, yr, 1), piece(t, 0, 2, yr, 1), b_minus[t])
        for t in range(2):
            send_a(t, 3, yr)
            send_a(t, 1, yr)

    def pass_a(b, yr):
        for t in range(2):
            ag_wait(("a+", t, b, yr), piece(t, 3, b, yr))
            ag_send(("af+", t, b, yr), piece(t, 3, b, yr, 0), piece(t, 2, b, yr, 0), a_plus[t])
            ag_wait(("a-", t, b, yr), piece(t, 1, b, yr))
            ag_send(("af-", t, b, yr), piece(t, 1, b, yr, 1), piece(t, 2, b, yr, 1), a_minus[t])

    def opposite_landed(pieces):
        for b, yr in pieces:
            for t in range(2):
                ag_wait(("af+", t, b, yr), piece(t, 2, b, yr, 0))
                ag_wait(("af-", t, b, yr), piece(t, 2, b, yr, 1))

    pass_b(0)
    pass_a(0, 0)

    for n in range(3):
        image_loads[n].wait()

        @pl.loop(0, PIX // 256)
        def _(k):
            cols = pl.ds(pl.multiple_of(k * 256, 256), 256)
            rows = pl.ds(n * 256, 256)
            wim[cols, rows] = (im[rows, cols].astype(F32) * weight[:, cols]).astype(BF16).T

    pass_a(0, 1)
    pass_b(1)
    log_prior()
    pass_a(3, 0)
    pass_a(1, 0)
    for yr in range(2):
        for t in range(2):
            ag_wait(("bf+", t, yr), piece(t, 0, 2, yr, 0))
            ag_wait(("bf-", t, yr), piece(t, 0, 2, yr, 1))
            send_a(t, 2, yr)

    mine = pl.ds(pl.multiple_of(core * HALF, 128), HALF)
    theirs = pl.ds(pl.multiple_of((1 - core) * HALF, 128), HALF)
    keep = pl.ds(pl.multiple_of(y_hi * SIDE, SIDE), SIDE)
    give = pl.ds(pl.multiple_of((1 - y_hi) * SIDE, SIDE), SIDE)
    ex_sends = []

    def ex_send(n, src, dst, peer):
        c = remote(src, dst, ex_s.at[n], ex_r.at[n], peer)
        c.start()
        ex_sends.append(c)

    def ex_wait(n, dst):
        landed(dst, ex_s.at[n], ex_r.at[n])

    def size(n):
        return 2 * PIECE * len(BATCHES[n])

    def score_rows(n):
        return pl.ds(SCORE_ROW[n], size(n))

    def sum_rows(n):
        return pl.ds(SUM_ROW[n], size(n) // 2 if n < SHARED else size(n))

    def kind_rows(n, kind):
        return pl.ds(pl.multiple_of(SCORE_ROW[n] + kind * (size(n) // 2), 16), size(n) // 2)

    def do_scores(n):
        batch = BATCHES[n]
        n_rows = size(n)
        rows = score_rows(n)

        def of(cols):
            return jnp.concatenate(
                [
                    refs[g, t * SIDE + b * 32 + yr * PIECE : t * SIDE + b * 32 + (yr + 1) * PIECE, cols]
                    for t in range(2)
                    for g, b, yr in batch
                ],
                axis=0,
            )

        def add(k, sums, chunks):
            for u in range(chunks):
                cols = pl.ds(pl.multiple_of((k * chunks + u) * 128, 128), 128)
                part = of(cols).astype(F32)
                sums = sums + part * part * weight[:, cols]
            return sums

        zero = jnp.zeros((n_rows, 128), F32)
        if n_rows > 128:
            sums = lax.fori_loop(0, PIX // 512, lambda k, v: add(k, v, 4), zero)
        else:
            sums = add(0, zero, PIX // 256) + add(1, zero, PIX // 256)
        norm = 0.5 * jnp.sum(sums, axis=1, keepdims=True)
        part = jnp.dot(of(slice(None)), wim[...], preferred_element_type=F32)
        score[rows, :] = part - norm
        ex_send(n, score.at[rows, theirs], core_in.at[rows], core_pal)

    def do_rows(n):
        rows, sums = score_rows(n), sum_rows(n)
        ex_wait(n, core_in.at[rows])
        if n < SHARED:
            away, home = kind_rows(n, 1 - y_hi), kind_rows(n, y_hi)
            row_out[sums] = score[away, mine] + core_in[away, :]
            ex_send(7 + n, row_out.at[sums], row_in.at[sums], hi_pal)
            total[sums] = score[home, mine] + core_in[home, :]
        else:
            row_out[sums] = score[rows, mine] + core_in[rows, :]
            ex_send(7 + n, row_out.at[sums], row_in.at[sums], hi_pal)

    def do_logits(n):
        sums = sum_rows(n)
        ex_wait(7 + n, row_in.at[sums])
        near = total if n < SHARED else row_out
        logits = INVERSE_HEAT * (near[sums] + row_in[sums]) + prior[0, sums, :]
        total[sums] = logits
        return jnp.max(logits, axis=0, keepdims=True)

    def mass_of(rows, top):
        return jnp.sum(jnp.exp(total[rows] - top), axis=0, keepdims=True)

    shared_rows = pl.ds(0, 3 * SIDE)
    do_scores(0)
    do_scores(1)
    do_rows(0)
    do_rows(1)
    pass_a(3, 1)
    pass_a(1, 1)
    do_scores(2)
    opposite_landed(FORWARD[:4])
    do_scores(4)
    do_rows(2)
    do_rows(4)
    pass_a(2, 0)
    pass_a(2, 1)
    do_scores(3)
    opposite_landed(FORWARD[4:6])
    do_rows(3)
    do_scores(5)
    top = jnp.maximum(do_logits(0), do_logits(1))
    opposite_landed(FORWARD[6:])
    do_rows(5)
    do_scores(6)
    top = jnp.maximum(top, do_logits(2))
    top = jnp.maximum(top, do_logits(3))
    mass = mass_of(shared_rows, top)
    stat_out[0:1, :] = top
    stat_out[1:2, :] = mass
    ex_send(14, stat_out.at[0:8], stat_in.at[0:8], hi_pal)
    do_rows(6)
    last_top = jnp.maximum(do_logits(4), do_logits(5))
    ex_wait(14, stat_in.at[0:8])
    other_top, other_mass = stat_in[0:1, :], stat_in[1:2, :]
    first = y_hi == 0
    top_a, top_b = jnp.where(first, top, other_top), jnp.where(first, other_top, top)
    mass_a, mass_b = jnp.where(first, mass, other_mass), jnp.where(first, other_mass, mass)
    last_top = jnp.maximum(last_top, do_logits(6))
    best = jnp.maximum(jnp.maximum(top_a, top_b), last_top)
    evidence = best + jnp.log(
        mass_a * jnp.exp(top_a - best) + mass_b * jnp.exp(top_b - best) + mass_of(pl.ds(3 * SIDE, 2 * SIDE), best)
    )
    for n in range(SHARED, len(BATCHES)):
        p = jnp.exp(total[sum_rows(n)] - evidence).astype(BF16)
        for t in range(2):
            for k, (g, b, yr) in enumerate(BATCHES[n]):
                o = (t * len(BATCHES[n]) + k) * PIECE
                rows = pl.ds(t * SIDE + b * 32 + yr * PIECE, PIECE)
                post[g, rows, mine] = p[o : o + PIECE, :]
    ex_send(22, post.at[2, :, mine], post.at[2, :, mine], core_pal)
    stat_out[8:16, :] = jnp.broadcast_to(evidence, (8, HALF))
    for n in (1, 2, 3, 0):
        p = jnp.exp(total[sum_rows(n)] - evidence).astype(BF16)
        for k, (g, b, yr) in enumerate(BATCHES[n]):
            first_row = pl.multiple_of(y_hi * SIDE + b * 32 + yr * PIECE, PIECE)
            post[g, pl.ds(first_row, PIECE), mine] = p[k * PIECE : (k + 1) * PIECE, :]
        for g in {3: (1, 3), 0: (0,)}.get(n, ()):
            ex_send(16 + g, post.at[g, keep, mine], post.at[g, keep, mine], hi_pal)
            ex_send(20 + g, post.at[g, keep, mine], post.at[g, keep, mine], core_pal)
    ex_send(15, stat_out.at[8:16], stat_in.at[8:16], core_pal)

    def do_relay(g):
        ex_wait(16 + g, post.at[g, give, mine])
        ex_send(24 + g, post.at[g, give, mine], post.at[g, give, mine], core_pal)

    def do_posterior(g):
        ex_wait(20 + g, post.at[g, keep, theirs])
        ex_wait(24 + g, post.at[g, give, theirs])

    def product(g, j):
        cols = pl.ds(pl.multiple_of(j * TILE, TILE), TILE)
        return jnp.dot(post[g], im[:, cols], preferred_element_type=F32)

    def a_rows(j, t):
        return pl.ds(t * SIDE, 64 if isinstance(j, int) and j % 4 == 3 else SIDE)

    def a_copy(kind, j, t, src, dst, peer):
        rows = a_rows(j, t)
        return remote(
            src.at[j, rows], dst.at[j, rows], a_s.at[kind, j, t], a_r.at[kind, j, t], peer
        )

    def a_landed(kind, j, t, dst):
        landed(dst.at[j, a_rows(j, t)], a_s.at[kind, j, t], a_r.at[kind, j, t])

    def f_copy(g, n):
        return remote(f_out.at[n, g], f_in.at[n, g], f_s.at[n, g], f_r.at[n, g], y_pal)

    def first_product(g, n):
        p = product(g, 3 + 4 * n).reshape(8, 2, PIECE, TILE)
        f_out[n, g] = p[:, 1].reshape(SIDE, TILE).astype(BF16)
        f_copy(g, n).start()
        kept[n, g] = p[:, 0].reshape(SIDE, TILE)

    def first_sum(g, n):
        f_copy(g, n).wait_recv()
        return kept[n, g] + f_in[n, g].astype(F32)

    def put(dst, j, rows):
        for t in range(2):
            dst[j, a_rows(j, t)] = rows[t * 64 : t * 64 + 64, :].astype(BF16)

    def get(src, j):
        return jnp.concatenate([src[j, a_rows(j, t)] for t in range(2)], axis=0).astype(F32)

    ex_wait(22, post.at[2, :, theirs])

    @pl.loop(0, 3)
    def _(k):
        s2[k] = product(2, k).astype(BF16)
        for t in range(2):
            a_copy(0, k, t, s2, r_opp, a_plus[t]).start()
        s2[k + 4] = product(2, k + 4).astype(BF16)
        for t in range(2):
            a_copy(0, k + 4, t, s2, r_opp, a_minus[t]).start()

    for n in range(2):
        first_product(2, n)
    def free(k):
        s1[k + 4] = product(1, k + 4).astype(BF16)
        for t in range(2):
            a_copy(1, k + 4, t, s1, r_minus, a_plus[t]).start()
        s3[k] = product(3, k).astype(BF16)
        for t in range(2):
            a_copy(2, k, t, s3, r_plus, a_minus[t]).start()

    def bound(k):
        p1 = product(1, k)
        for t in range(2):
            a_landed(0, k, t, r_opp)
        s1[k] = (p1 + r_opp[k].astype(F32)).astype(BF16)
        for t in range(2):
            a_copy(1, k, t, s1, r_minus, a_plus[t]).start()
        p3 = product(3, k + 4)
        for t in range(2):
            a_landed(0, k + 4, t, r_opp)
        s3[k + 4] = (p3 + r_opp[k + 4].astype(F32)).astype(BF16)
        for t in range(2):
            a_copy(2, k + 4, t, s3, r_plus, a_minus[t]).start()

    do_relay(1)
    do_relay(3)
    do_posterior(1)
    do_posterior(3)
    first_product(1, 1)
    first_product(3, 0)
    first_product(1, 0)
    first_product(3, 1)
    free(0)

    @pl.loop(0, 2)
    def _(k):
        bound(k)

    do_relay(0)
    do_posterior(0)
    for n in range(2):
        first_product(0, n)

    ex_wait(15, stat_in.at[8:16])
    evid[:, mine] = stat_out[8:9, :]
    evid[:, theirs] = stat_in[8:9, :]
    for n in range(NIM // 128):
        evidence_ref[n : n + 1, :] = evid[:, n * 128 : n * 128 + 128]

    def b_copy(kind, j, t, src, dst, peer):
        rows = pl.ds(0, PIECE if j % 4 == 3 else 32)
        return remote(
            src.at[j, t, rows], dst.at[j, t, rows], b_s.at[kind, j, t], b_r.at[kind, j, t], peer
        )

    def b_landed(kind, j, t, dst):
        b_copy(kind, j, t, dst, dst, core_pal).wait_recv()

    def y_copy(j, t):
        return remote(y_out.at[j, t], y_in.at[j, t], yy_s.at[j, t], yy_r.at[j, t], y_pal)

    def first_opposite():
        for n, j in enumerate((3, 7)):
            put(s2, j, first_sum(2, n))
            for t in range(2):
                a_copy(0, j, t, s2, r_opp, (a_plus, a_minus)[n][t]).start()

    def first_free():
        put(s1, 7, first_sum(1, 1))
        for t in range(2):
            a_copy(1, 7, t, s1, r_minus, a_plus[t]).start()
        put(s3, 3, first_sum(3, 0))
        for t in range(2):
            a_copy(2, 3, t, s3, r_plus, a_minus[t]).start()

    def first_bound():
        for t in range(2):
            a_landed(0, 3, t, r_opp)
        put(s1, 3, first_sum(1, 0) + get(r_opp, 3))
        for t in range(2):
            a_copy(1, 3, t, s1, r_minus, a_plus[t]).start()
        for t in range(2):
            a_landed(0, 7, t, r_opp)
        put(s3, 7, first_sum(3, 1) + get(r_opp, 7))
        for t in range(2):
            a_copy(2, 7, t, s3, r_plus, a_minus[t]).start()

    def rows_of(j, t, b):
        n = PIECE if j % 4 == 3 else 32
        return pl.ds(t * SIDE + b * n, n)

    def step_a(k):
        for j, low in ((k, True), (k + 4, False)):
            p = None if k == 3 else product(0, j)
            for t in range(2):
                a_landed(1, j, t, r_minus)
                a_landed(2, j, t, r_plus)
            if k == 3:
                total_j = first_sum(0, j // 4) + get(r_plus, j) + get(r_minus, j)
                for t in range(2):
                    acc[j, a_rows(j, t)] = total_j[t * 64 : t * 64 + 64, :]
            else:
                acc[j] = p + r_plus[j].astype(F32) + r_minus[j].astype(F32)
            n = PIECE if k == 3 else 32
            for t in range(2):
                z2[j, t, 0:n] = acc[j, rows_of(j, t, 2), :].astype(BF16)
                b_copy(0, j, t, z2, zr_opp, b_plus[t] if low else b_minus[t]).start()
                if low:
                    z3[j, t, 0:n] = acc[j, rows_of(j, t, 3), :].astype(BF16)
                    b_copy(2, j, t, z3, zr_plus, b_minus[t]).start()
                else:
                    z1[j, t, 0:n] = acc[j, rows_of(j, t, 1), :].astype(BF16)
                    b_copy(1, j, t, z1, zr_minus, b_plus[t]).start()

    def step_b(k):
        n = PIECE if k == 3 else 32
        for t in range(2):
            b_landed(0, k, t, zr_opp)
            v = acc[k, rows_of(k, t, 1), :] + zr_opp[k, t, 0:n].astype(F32)
            z1[k, t, 0:n] = v.astype(BF16)
            b_copy(1, k, t, z1, zr_minus, b_plus[t]).start()
            j = k + 4
            b_landed(0, j, t, zr_opp)
            v = acc[j, rows_of(j, t, 3), :] + zr_opp[j, t, 0:n].astype(F32)
            z3[j, t, 0:n] = v.astype(BF16)
            b_copy(2, j, t, z3, zr_plus, b_minus[t]).start()

    def step_c(k):
        n = PIECE if k == 3 else 32
        for j in (k, k + 4):
            cols = pl.ds(j * TILE, TILE)
            for t in range(2):
                b_landed(1, j, t, zr_minus)
                b_landed(2, j, t, zr_plus)
                v = acc[j, rows_of(j, t, 0), :] + zr_plus[j, t, 0:n].astype(F32)
                v = v + zr_minus[j, t, 0:n].astype(F32)
                out_ref[t * PIECE : (t + 1) * PIECE, cols] = v[:PIECE, :]
                if k < 3:
                    y_out[j, t] = v[PIECE:, :].astype(BF16)
                    y_copy(j, t).start()

    def step_d(k):
        for j in (k, k + 4):
            cols = pl.ds(j * TILE, TILE)
            for t in range(2):
                y_copy(j, t).wait_recv()
                rows = slice(t * PIECE, (t + 1) * PIECE)
                out_ref[rows, cols] = out_ref[rows, cols] + y_in[j, t].astype(F32)

    step_a(0)
    first_opposite()

    @pl.loop(1, 3)
    def _(k):
        free(k)

    bound(2)
    first_free()
    step_a(1)
    step_b(0)
    step_a(2)
    first_bound()
    step_c(0)
    step_b(1)
    step_b(2)
    step_a(3)
    step_c(1)
    step_c(2)
    step_b(3)
    step_d(0)
    step_d(1)
    step_c(3)
    step_d(2)

    for c in ag_sends:
        c.wait_send()
    for c in ex_sends:
        c.wait_send()

    for j in range(NT):
        for t in range(2):
            a_copy(0, j, t, s2, r_opp, core_pal).wait_send()
            a_copy(1, j, t, s1, r_minus, core_pal).wait_send()
            a_copy(2, j, t, s3, r_plus, core_pal).wait_send()
            b_copy(0, j, t, z2, zr_opp, core_pal).wait_send()
            b_copy(1, j, t, z1, zr_minus, core_pal).wait_send()
            b_copy(2, j, t, z3, zr_plus, core_pal).wait_send()
            if j % 4 < 3:
                y_copy(j, t).wait_send()
    for n in range(2):
        for g in range(4):
            f_copy(g, n).wait_send()


def hand_over(sums_hbm, evidence_hbm, sums_out, evidence_out, sums, evidence, sems):
    sources, held = (sums_hbm, evidence_hbm), (sums, evidence)
    for n, out in enumerate((sums_out, evidence_out)):
        pltpu.make_async_copy(sources[n], held[n], sems.at[0, n]).start()
    for n, out in enumerate((sums_out, evidence_out)):
        pltpu.make_async_copy(sources[n], held[n], sems.at[0, n]).wait()
        pltpu.make_async_copy(held[n], out, sems.at[1, n]).start()
    for n, out in enumerate((sums_out, evidence_out)):
        pltpu.make_async_copy(held[n], out, sems.at[1, n]).wait()


def shards(
    images, references, shell_of_pixel, noise_power, ref_class, ref_orient, class_logw, orient_logw
):
    vmem = pl.BlockSpec(memory_space=pltpu.VMEM)
    hbm = pl.BlockSpec(memory_space=pl.ANY)
    smem = pl.BlockSpec(memory_space=pltpu.SMEM)
    dma = pltpu.SemaphoreType.DMA
    accumulators, evidence = pl.pallas_call(
        kernel,
        out_shape=(
            jax.ShapeDtypeStruct((ROWS, PIX), F32),
            jax.ShapeDtypeStruct((NIM // 128, 128), F32),
        ),
        in_specs=[hbm, hbm, vmem, vmem, vmem, vmem, vmem, smem],
        out_specs=(vmem, vmem),
        scratch_shapes=[
            pltpu.VMEM((NIM, PIX), BF16),
            pltpu.VMEM((PIX, NIM), BF16),
            pltpu.VMEM((4, GROUP, PIX), BF16),
            pltpu.VMEM((NREF, NIM), F32),
            pltpu.VMEM((NREF, HALF), F32),
            pltpu.VMEM((5 * SIDE, HALF), F32),
            pltpu.VMEM((5 * SIDE, HALF), F32),
            pltpu.VMEM((5 * SIDE, HALF), F32),
            pltpu.VMEM((1, PIX), F32),
            pltpu.VMEM((128, 128), F32),
            pltpu.VMEM((2, 128, 128), F32),
            pltpu.VMEM((2, 5 * SIDE, 1), F32),
            pltpu.VMEM((1, NIM), F32),
            pltpu.VMEM((16, HALF), F32),
            pltpu.VMEM((16, HALF), F32),
            pltpu.VMEM((4, GROUP, NIM), BF16),
            pltpu.VMEM((NT, GROUP, TILE), BF16),
            pltpu.VMEM((NT, GROUP, TILE), BF16),
            pltpu.VMEM((NT, GROUP, TILE), BF16),
            pltpu.VMEM((NT, GROUP, TILE), BF16),
            pltpu.VMEM((NT, GROUP, TILE), BF16),
            pltpu.VMEM((NT, GROUP, TILE), BF16),
            pltpu.VMEM((NT, GROUP, TILE), F32),
            pltpu.VMEM((NT, 2, 32, TILE), BF16),
            pltpu.VMEM((NT, 2, 32, TILE), BF16),
            pltpu.VMEM((NT, 2, 32, TILE), BF16),
            pltpu.VMEM((NT, 2, 32, TILE), BF16),
            pltpu.VMEM((NT, 2, 32, TILE), BF16),
            pltpu.VMEM((NT, 2, 32, TILE), BF16),
            pltpu.VMEM((NT, 2, PIECE, TILE), BF16),
            pltpu.VMEM((NT, 2, PIECE, TILE), BF16),
            pltpu.VMEM((2, 4, SIDE, TILE), F32),
            pltpu.VMEM((2, 4, SIDE, TILE), BF16),
            pltpu.VMEM((2, 4, SIDE, TILE), BF16),
            dma((5,)),
            dma((84,)),
            dma((84,)),
            dma((28,)),
            dma((28,)),
            dma((3, NT, 2)),
            dma((3, NT, 2)),
            dma((3, NT, 2)),
            dma((3, NT, 2)),
            dma((NT, 2)),
            dma((NT, 2)),
            dma((2, 4)),
            dma((2, 4)),
        ],
        compiler_params=pltpu.CompilerParams(
            collective_id=0, has_side_effects=True, vmem_limit_bytes=58 << 20
        ),
    )(
        images,
        references,
        shell_of_pixel.reshape(1, PIX),
        noise_power.reshape(1, 64),
        ref_class.reshape(NREF // 128, 128),
        ref_orient.reshape(NREF // 128, 128),
        orient_logw.reshape(1, NORIENT),
        class_logw,
    )
    accumulators, evidence = pl.pallas_call(
        hand_over,
        out_shape=(
            jax.ShapeDtypeStruct((ROWS, PIX), F32),
            jax.ShapeDtypeStruct((NIM // 128, 128), F32),
        ),
        in_specs=[pl.BlockSpec(memory_space=pltpu.HBM)] * 2,
        out_specs=(pl.BlockSpec(memory_space=pltpu.HBM),) * 2,
        scratch_shapes=[
            pltpu.VMEM((ROWS, PIX), F32),
            pltpu.VMEM((NIM // 128, 128), F32),
            dma((2, 2)),
        ],
    )(accumulators, evidence)
    return accumulators, evidence.reshape(NIM)


def solution(mesh):
    placed = (P("img", "shell"), P("img", "shell"), P("shell"), P(), P(), P(), P(), P())
    return jax.shard_map(
        shards, mesh=mesh, in_specs=placed, out_specs=(P("img", "shell"), P("img")), check_vma=False
    )
```
